32 devices in a mesh: dp: 8 (over y, x, core), tensor: 4 (over z).
Axes of the slice: x: 2, y: 2, z: 4, core: 2. Of those that a mesh axis runs over, the one named last changes fastest.
Arguments:
- gradient: float32 [5120, 27648], P('dp', 'tensor'), may hold values from -6 to 6
- momentum: float32 [5120, 27648], P('dp', 'tensor'), may hold values from -6 to 6
- right_factor: float32 [27648, 256], P('tensor'), may hold values from -6 to 6
Outputs:
- update: float32 [5120, 27648], P('dp', 'tensor')
- new_momentum: float32 [5120, 27648], P('dp', 'tensor')
- new_right: float32 [27648, 256], P('tensor')
The draws below stay inside these ranges and needn't reach their ends.
All inputs are finite; a program needn't handle non-finite values.
Results may differ from the reference program's by a relative error of at most 0.000098.
Values sent between devices are 32-bit elements; how exact they have to be, the bound alone decides.
No kernel may reach another device: no remote copies, remote signals or barrier semaphores. Data moves between devices by JAX's collectives and lax.ppermute only.
A program may use at most 192 MiB of HBM per device.

```python
import jax
import jax.numpy as jnp
from jax import lax

ROWS = 5120
COLS = 27648
RANK = 256


def shard_levels(key, dims, cuts, least, largest):
    def one(axis_at, shards_of):
        heights = jax.random.uniform(jax.random.fold_in(jax.random.fold_in(key, 6), axis_at), (shards_of,), jnp.float32, least / len(cuts), largest / len(cuts))
        return jnp.repeat(jnp.exp(heights), dims[axis_at] // shards_of).reshape((-1,) + (1,) * (len(dims) - axis_at - 1))

    loudness = one(*cuts[0])
    for cut in cuts[1:]:
        loudness = loudness * one(*cut)
    return loudness


def centred(rng, shape, scale, limit, split=(), dtype=jnp.bfloat16):
    array = jax.random.normal(rng, shape, jnp.float32) * scale
    if len(split) > 0:
        array = shard_levels(rng, shape, split, -0.22, 0.18) * array
    return jnp.clip(array, min=-limit, max=limit).astype(dtype)


def setup_inputs(seed: int = 0) -> dict:
    seeds = jax.random.split(jax.random.key(seed), 4)
    return {
        "gradient": centred(seeds[0], (ROWS, COLS), 1.0, 6.0, ((0, 8), (1, 4)), jnp.float32),
        "momentum": centred(seeds[1], (ROWS, COLS), 1.0, 6.0, ((0, 8), (1, 4)), jnp.float32),
        "right_factor": centred(seeds[2], (COLS, RANK), 1.0, 6.0, ((0, 4),), jnp.float32),
    }


def reference(gradient, momentum, right_factor):
    high = lax.Precision.HIGHEST
    buffer = momentum + gradient
    left = jnp.dot(buffer.astype(jnp.float32), right_factor.astype(jnp.float32), precision=high, preferred_element_type=jnp.float32)
    gram = jnp.dot(left.T.astype(jnp.float32), left.astype(jnp.float32), precision=high, preferred_element_type=jnp.float32)
    chol = jnp.linalg.cholesky(gram)
    ortho = jax.scipy.linalg.solve_triangular(chol, left.T, lower=True).T
    right = jnp.dot(buffer.T.astype(jnp.float32), ortho.astype(jnp.float32), precision=high, preferred_element_type=jnp.float32)
    scale_col = jnp.sqrt(lax.optimization_barrier(jnp.sum(right * right, axis=0)) / COLS + 1e-06)
    new_right = right / scale_col
    new_momentum = buffer - 0.05 * jnp.dot(ortho.astype(jnp.float32), right.T.astype(jnp.float32), precision=high, preferred_element_type=jnp.float32)
    factor = (ROWS / RANK) ** 0.5
    update = factor * jnp.dot(ortho.astype(jnp.float32), new_right.T.astype(jnp.float32), precision=high, preferred_element_type=jnp.float32)
    return (update, new_momentum, new_right)
```

```python
import functools

import jax
import jax.numpy as jnp
from jax import lax
from jax.experimental import pallas as pl
from jax.experimental.pallas import tpu as pltpu
from jax.sharding import PartitionSpec as P

F32 = jnp.float32
BF16 = jnp.bfloat16
HIGH = lax.Precision.HIGHEST
LANES = 128
VMEM_LIMIT = 60 * 1024 * 1024

NN = (((1,), (0,)), ((), ()))
NT = (((1,), (1,)), ((), ()))
TN = (((0,), (0,)), ((), ()))


def params(**kw):
    return pltpu.CompilerParams(vmem_limit_bytes=VMEM_LIMIT, **kw)


def cost(flops, moved):
    return pl.CostEstimate(flops=int(flops), bytes_accessed=int(moved), transcendentals=0)


def split(x):
    hi = x.astype(BF16)
    lo = (x - hi.astype(F32)).astype(BF16)
    return hi, lo


def dot3(ah, al, bh, bl, dims):
    d = functools.partial(lax.dot_general, dimension_numbers=dims, preferred_element_type=F32)
    return d(ah, bh) + (d(ah, bl) + d(al, bh))


def dot_high(a, b, dims):
    return lax.dot_general(a, b, dims, precision=HIGH, preferred_element_type=F32)


def scalars(*values):
    return jnp.stack([jnp.asarray(v, jnp.int32) for v in values])


def column_block(cols):
    blocks = cols // LANES
    return LANES * max(k for k in range(1, 9) if blocks % k == 0)


def left_kernel(at, g, m, r, *rest):
    buffer, out = rest[-2:]
    step = pl.program_id(0)
    b = g[...] + m[...]
    buffer[...] = b
    bh, bl = split(b)
    rh, rl = split(r[...])
    term = dot3(bh, bl, rh, rl, NN)

    @pl.when(step == 0)
    def _():
        out[...] = term

    @pl.when(step > 0)
    def _():
        out[...] += term


def left_half(at, gradient, momentum, right_factor, buffer):
    rows, cols = gradient.shape
    rank = right_factor.shape[1]
    half, wide = rows // 2, column_block(cols)
    block = pl.BlockSpec((half, wide), lambda j, at: (at[0], j))
    first = buffer is None
    return pl.pallas_call(
        left_kernel,
        grid_spec=pltpu.PrefetchScalarGridSpec(
            num_scalar_prefetch=1,
            grid=(cols // wide,),
            in_specs=[block, block, pl.BlockSpec((wide, rank), lambda j, at: (j, 0))]
            + ([] if first else [pl.BlockSpec(memory_space=pl.ANY)]),
            out_specs=[block, pl.BlockSpec((half, rank), lambda j, at: (0, 0))],
        ),
        out_shape=[
            jax.ShapeDtypeStruct((rows, cols), F32),
            jax.ShapeDtypeStruct((half, rank), F32),
        ],
        input_output_aliases={} if first else {4: 0},
        compiler_params=params(),
        cost_estimate=cost(6 * half * cols * rank, 4 * (3 * half * cols + cols * rank)),
        name="left_half",
    )(scalars(at), gradient, momentum, right_factor, *([] if first else [buffer]))


def gram_kernel(*refs):
    pieces, (left, lh, ll, gram) = refs[:-4], refs[-4:]
    n = pieces[0].shape[0]
    for i, piece in enumerate(pieces):
        x = piece[...]
        at = pl.ds(i * n, n)
        left[at, :] = x
        h, l = split(x)
        lh[at, :] = h
        ll[at, :] = l
    half = left.shape[0] // 2
    own, other = left[:half, :], left[half:, :]
    gram[...] = dot_high(own, own, TN) + dot_high(other, other, TN)


def gram_of(pieces):
    rank = pieces[0].shape[1]
    rows = sum(p.shape[0] for p in pieces)
    return pl.pallas_call(
        gram_kernel,
        out_shape=[
            jax.ShapeDtypeStruct((rows, rank), F32),
            jax.ShapeDtypeStruct((rows, rank), BF16),
            jax.ShapeDtypeStruct((rows, rank), BF16),
            jax.ShapeDtypeStruct((rank, rank), F32),
        ],
        compiler_params=params(),
        cost_estimate=cost(12 * rows * rank * rank, 12 * rows * rank),
        name="gram_of",
    )(*pieces)


def w_term(own, other, lh, ll):
    half = own.shape[0]
    total = None
    for ref, at in ((own, 0), (other, half)):
        bh, bl = split(ref[...])
        term = dot3(bh, bl, lh[at : at + half, :], ll[at : at + half, :], TN)
        total = term if total is None else total + term
    return total


def w_send_kernel(at, own, other, lh, ll, out):
    out[...] = w_term(own, other, lh, ll)


def w_keep_kernel(at, own, other, lh, ll, got, send, keep):
    total = w_term(own, other, lh, ll) + got[...]

    @pl.when(pl.program_id(0) == 0)
    def _():
        send[...] = total

    @pl.when(pl.program_id(0) == 1)
    def _():
        keep[...] = total


def w_specs(buffer, rank, unit):
    half = buffer.shape[0] // 2
    whole = pl.BlockSpec((2 * half, rank), lambda i, at: (0, 0))
    return [
        pl.BlockSpec((half, unit), lambda i, at: (at[0], at[2 + i])),
        pl.BlockSpec((half, unit), lambda i, at: (at[1], at[2 + i])),
        whole,
        whole,
    ]


def w_cost(buffer, rank, unit):
    rows = buffer.shape[0]
    return cost(2 * 6 * rows * unit * rank, 2 * 4 * (rows * unit + unit * rank))


def w_send(s, units, buffer, lh, ll, unit):
    rank = lh.shape[1]
    return pl.pallas_call(
        w_send_kernel,
        grid_spec=pltpu.PrefetchScalarGridSpec(
            num_scalar_prefetch=1,
            grid=(2,),
            in_specs=w_specs(buffer, rank, unit),
            out_specs=pl.BlockSpec((unit, rank), lambda i, at: (i, 0)),
        ),
        out_shape=jax.ShapeDtypeStruct((2 * unit, rank), F32),
        compiler_params=params(),
        cost_estimate=w_cost(buffer, rank, unit),
        name="w_send",
    )(scalars(s, 1 - s, *units), buffer, buffer, lh, ll)


def w_keep(s, units, order, buffer, lh, ll, got, unit):
    rank = lh.shape[1]
    one = pl.BlockSpec((unit, rank), lambda i, at: (0, 0))
    return pl.pallas_call(
        w_keep_kernel,
        grid_spec=pltpu.PrefetchScalarGridSpec(
            num_scalar_prefetch=1,
            grid=(2,),
            in_specs=w_specs(buffer, rank, unit)
            + [pl.BlockSpec((unit, rank), lambda i, at: (at[4 + i], 0))],
            out_specs=[one, one],
        ),
        out_shape=[jax.ShapeDtypeStruct((unit, rank), F32)] * 2,
        compiler_params=params(),
        cost_estimate=w_cost(buffer, rank, unit),
        name="w_keep",
    )(scalars(s, 1 - s, *units, *order), buffer, buffer, lh, ll, got)


GROUP = 8


def factor_group(rows, at):
    full = (GROUP, LANES)
    columns = [jnp.broadcast_to(rows[:, at + j : at + j + 1], full) for j in range(GROUP)]
    a = {
        (i, j): jnp.broadcast_to(columns[j][i : i + 1, :], full)
        for j in range(GROUP)
        for i in range(j, GROUP)
    }
    low, c = {}, {}
    for k in range(GROUP):
        c[k, k] = lax.rsqrt(a[k, k])
        for i in range(k + 1, GROUP):
            low[i, k] = a[i, k] * c[k, k]
        for j in range(k + 1, GROUP):
            for i in range(j, GROUP):
                a[i, j] = a[i, j] - low[i, k] * low[j, k]
        for j in range(k):
            total = low[k, j] * c[j, j]
            for i in range(j + 1, k):
                total = total + low[k, i] * c[i, j]
            c[k, j] = -c[k, k] * total
    return c


def spread(x, width):
    return jnp.concatenate([x] * (width // LANES), axis=1)


def eliminate(block):
    size, width = block.shape
    sub = lax.broadcasted_iota(jnp.int32, (GROUP, LANES), 0)
    groups = [block[i : i + GROUP, :] for i in range(0, size, GROUP)]
    for p in range(len(groups)):
        at = p * GROUP
        rows = groups[p]
        c = factor_group(rows, at)
        done = None
        for j in range(GROUP):
            col = jnp.zeros((GROUP, LANES), F32)
            for i in range(j, GROUP):
                col = jnp.where(sub == i, c[i, j], col)
            term = spread(col, width) * jnp.broadcast_to(rows[j : j + 1, :], (GROUP, width))
            done = term if done is None else done + term
        groups[p] = done
        if p + 1 == len(groups):
            break
        solved = None
        for k in range(GROUP):
            col = jnp.zeros((GROUP, LANES), F32)
            for j in range(k + 1):
                col = jnp.where(sub == j, c[k, j], col)
            term = spread(col, width) * jnp.broadcast_to(done[k : k + 1, :], (GROUP, width))
            solved = term if solved is None else solved + term
        for q in range(p + 1, len(groups)):
            x = groups[q]
            total = None
            for j in range(GROUP):
                term = jnp.broadcast_to(x[:, at + j : at + j + 1], (GROUP, width)) * jnp.broadcast_to(
                    solved[j : j + 1, :], (GROUP, width)
                )
                total = term if total is None else total + term
            groups[q] = x - total
    return jnp.concatenate(groups, axis=0)


def chol_kernel(gram, left, x_out, oh, ol, work):
    rank = gram.shape[0]
    size = min(64, rank)
    work[:, :rank] = gram[...]
    r = lax.broadcasted_iota(jnp.int32, (rank, rank), 0)
    c = lax.broadcasted_iota(jnp.int32, (rank, rank), 1)
    work[:, rank:] = jnp.where(r == c, 1.0, 0.0).astype(F32)

    def step(b, _):
        at = pl.multiple_of(b * size, size)
        rows = pl.ds(at, size)
        width = 2 * rank
        block = pltpu.roll(work[rows, :], lax.rem(width - at, width), 1)
        block = pltpu.roll(eliminate(block), at, 1)
        x_out[rows, :] = block[:, rank:]

        @pl.when(b + 1 < rank // size)
        def _():
            work[...] -= dot_high(block[:, :rank], block, TN)

        return 0

    lax.fori_loop(0, rank // size, step, 0)
    h, l = split(dot_high(left[...], x_out[...], NT))
    oh[...] = h
    ol[...] = l


def chol_inverse(gram, left):
    rows, rank = left.shape
    return pl.pallas_call(
        chol_kernel,
        out_shape=[
            jax.ShapeDtypeStruct((rank, rank), F32),
            jax.ShapeDtypeStruct((rows, rank), BF16),
            jax.ShapeDtypeStruct((rows, rank), BF16),
        ],
        scratch_shapes=[pltpu.VMEM((rank, 2 * rank), F32)],
        compiler_params=params(),
        cost_estimate=cost(4e9, 4 * rows * rank),
        name="chol_inverse",
    )(gram, left)


def right_kernel(at, ka, ga, kb, gb, x, ra, rb, squares):
    rows, rank = ka.shape
    total = jnp.zeros((1, rank), F32)
    for i, (k, g, out) in enumerate(((ka, ga, ra), (kb, gb, rb))):
        value = dot_high(k[...] + g[...], x[...], NT)
        out[...] = value
        row = lax.broadcasted_iota(jnp.int32, (rows, rank), 0) + at[i]
        value = jnp.where(row < at[2], value, 0.0)
        total = total + jnp.sum(value * value, axis=0, keepdims=True)
    squares[...] = jnp.broadcast_to(total, squares.shape)


def right_rows(at_a, at_b, cols, ka, ga, kb, gb, x):
    rows, rank = ka.shape
    vm = pl.BlockSpec(memory_space=pltpu.VMEM)
    return pl.pallas_call(
        right_kernel,
        in_specs=[pl.BlockSpec(memory_space=pltpu.SMEM)] + [vm] * 5,
        out_specs=[vm] * 3,
        out_shape=[jax.ShapeDtypeStruct((rows, rank), F32)] * 2
        + [jax.ShapeDtypeStruct((GROUP, rank), F32)],
        compiler_params=params(),
        cost_estimate=cost(24 * rows * rank * rank, 24 * rows * rank),
        name="right_rows",
    )(scalars(at_a, at_b, cols), ka, ga, kb, gb, x)


def final_kernel(count, total_cols, factor, at, *refs):
    pieces = refs[:count]
    squares, oh, ol, buffer = refs[count : count + 4]
    update, momentum, new_right, rh, rl, nh, nl = refs[-7:]
    u, h = pl.program_id(0), pl.program_id(1)
    half = buffer.shape[0]
    for k in range(count):

        @pl.when((u == k) & (h == 0))
        def _(k=k):
            right = pieces[k][...]
            scale = jnp.sqrt(squares[0:1, :] / total_cols + 1e-06)
            scaled = right / scale
            new_right[...] = scaled
            rh[...], rl[...] = split(right)
            nh[...], nl[...] = split(scaled)

    rows = pl.ds(pl.multiple_of(h * half, half), half)
    a, b = oh[rows, :], ol[rows, :]
    momentum[...] = buffer[...] - 0.05 * dot3(a, b, rh[...], rl[...], NT)
    update[...] = factor * dot3(a, b, nh[...], nl[...], NT)


def final(s, units, pieces, squares, oh, ol, buffer, total_rows, total_cols, before):
    rows, cols = buffer.shape
    unit, rank = pieces[0].shape
    half, count = rows // 2, len(pieces)
    wide = pl.BlockSpec((half, unit), lambda u, h, at: (at[h], at[2 + u]))
    whole = lambda shape: pl.BlockSpec(shape, lambda u, h, at: (0, 0))
    n_in = count + 5
    factor = (total_rows / rank) ** 0.5
    return pl.pallas_call(
        functools.partial(final_kernel, count, total_cols, factor),
        grid_spec=pltpu.PrefetchScalarGridSpec(
            num_scalar_prefetch=1,
            grid=(count, 2),
            in_specs=[whole((unit, rank))] * count
            + [whole((GROUP, rank)), whole((rows, rank)), whole((rows, rank)), wide]
            + [pl.BlockSpec(memory_space=pl.ANY)] * len(before),
            out_specs=[wide, wide, pl.BlockSpec((unit, rank), lambda u, h, at: (at[2 + u], 0))],
            scratch_shapes=[pltpu.VMEM((unit, rank), BF16)] * 4,
        ),
        out_shape=[
            jax.ShapeDtypeStruct((rows, cols), F32),
            jax.ShapeDtypeStruct((rows, cols), F32),
            jax.ShapeDtypeStruct((cols, rank), F32),
        ],
        input_output_aliases={n_in + i: i for i in range(len(before))},
        compiler_params=params(),
        cost_estimate=cost(12 * count * rows * unit * rank, 4 * count * unit * (3 * rows + 2 * rank)),
        name="final",
    )(scalars(s, 1 - s, *units), *pieces, squares, oh, ol, buffer, *before)


def power_of_two(n):
    return n & (n - 1) == 0


def bits_of(n):
    return list(range(n.bit_length() - 1))


def swap(x, axis, bit):
    n = lax.axis_size(axis)
    return lax.ppermute(x, axis, [(i, i ^ (1 << bit)) for i in range(n)])


def sum_over(x, axis):
    n = lax.axis_size(axis)
    if not power_of_two(n):
        return lax.psum(x, axis)
    for bit in bits_of(n):
        x = x + swap(x, axis, bit)
    return x


def on_device(gradient, momentum, right_factor):
    rows, cols = gradient.shape
    rank = right_factor.shape[1]
    n_dp, n_tp = lax.axis_size("dp"), lax.axis_size("tensor")
    d, z = lax.axis_index("dp"), lax.axis_index("tensor")
    half = rows // 2

    s = lax.rem(z, 2)
    buffer, away = left_half(1 - s, gradient, momentum, right_factor, None)
    if power_of_two(n_tp) and n_tp > 1:
        got = swap(away, "tensor", 0)
        buffer, mine = left_half(s, gradient, momentum, right_factor, buffer)
        mine = mine + got
        own = [mine[: half // 2], mine[half // 2 :]]
        for bit in bits_of(n_tp)[1:]:
            own = [x + swap(x, "tensor", bit) for x in own]
        pieces = own + [swap(x, "tensor", 0) for x in own]
    else:
        buffer, mine = left_half(s, gradient, momentum, right_factor, buffer)
        both = lax.psum(jnp.where(s == 0, jnp.stack([mine, away]), jnp.stack([away, mine])), "tensor")
        pieces = [lax.dynamic_index_in_dim(both, i, 0, False) for i in (s, 1 - s)]

    left, lh, ll, gram = gram_of(pieces)
    gram = sum_over(gram, "dp")

    unit = LANES * (-(-cols // (8 * LANES)))
    bits = bits_of(n_dp)
    core = lax.rem(d, 2)
    orders = [bits[1:], bits[1:][::-1]]
    bit_of = lambda b: lax.rem(d // (1 << b), 2)
    sent = [
        w_send(s, [4 * h + 2 * (1 - core), 4 * h + 2 * (1 - core) + 1], buffer, lh, ll, unit)
        for h in range(2)
    ]
    got = [swap(x, "dp", 0) for x in sent]
    x_inv, oh, ol = chol_inverse(gram, left)
    kept, here = [], []
    for h, order in enumerate(orders):
        t = bit_of(order[0])
        base = 4 * h + 2 * core
        send, keep = w_keep(s, [base + 1 - t, base + t], [1 - t, t], buffer, lh, ll, got[h], unit)
        at = (base + t) * unit
        recv = swap(send, "dp", order[0])
        for b in order[1:]:
            x = keep + recv
            n = x.shape[0] // 2
            t = bit_of(b)
            recv = swap(lax.dynamic_slice_in_dim(x, (1 - t) * n, n, 0), "dp", b)
            keep = lax.dynamic_slice_in_dim(x, t * n, n, 0)
            at = at + t * n
        kept.append((keep, recv))
        here.append(at)

    ra, rb, squares = right_rows(here[0], here[1], cols, *kept[0], *kept[1], x_inv)

    near, far = [], []
    for h, (order, x) in enumerate(zip(orders, (ra, rb))):
        for b in order[:0:-1]:
            y = swap(x, "dp", b)
            x = jnp.where(bit_of(b) == 0, jnp.concatenate([x, y]), jnp.concatenate([y, x]))
        t = bit_of(order[0])
        y = swap(x, "dp", order[0])
        base, beside = 4 * h + 2 * core, 4 * h + 2 * (1 - core)
        near.append(((base + t, x), (beside + t, swap(x, "dp", 0))))
        far.append(((base + 1 - t, y), (beside + 1 - t, swap(y, "dp", 0))))

    squares = sum_over(sum_over(squares, "dp"), "tensor")
    outs = ()
    for group in (near, far):
        units = [u for part in group for u, _ in part]
        data = [x for part in group for _, x in part]
        outs = final(s, units, data, squares, oh, ol, buffer, rows * n_dp, cols * n_tp, outs)
    return tuple(outs)


def solution(mesh):
    return jax.shard_map(
        on_device,
        mesh=mesh,
        in_specs=(P("dp", "tensor"), P("dp", "tensor"), P("tensor", None)),
        out_specs=(P("dp", "tensor"), P("dp", "tensor"), P("tensor", None)),
        check_vma=False,
    )
```

```python
import functools

import jax
import jax.numpy as jnp
from jax import lax
from jax.experimental import pallas as pl
from jax.experimental.pallas import tpu as pltpu
from jax.sharding import PartitionSpec as P


F32 = jnp.float32
BF16 = jnp.bfloat16
HIGH = lax.Precision.HIGHEST
LANES = 128
VMEM_LIMIT = 60 * 1024 * 1024

NN = (((1,), (0,)), ((), ()))
NT = (((1,), (1,)), ((), ()))
TN = (((0,), (0,)), ((), ()))


ANY = pl.BlockSpec(memory_space=pl.ANY)


def params(**kw):
    return pltpu.CompilerParams(vmem_limit_bytes=VMEM_LIMIT, **kw)


def cost(flops, moved):
    return pl.CostEstimate(flops=int(flops), bytes_accessed=int(moved), transcendentals=0)


def split(x):
    hi = x.astype(BF16)
    lo = (x - hi.astype(F32)).astype(BF16)
    return hi, lo


def dot3(ah, al, bh, bl, dims):
    d = functools.partial(lax.dot_general, dimension_numbers=dims, preferred_element_type=F32)
    return d(ah, bh) + (d(ah, bl) + d(al, bh))


def dot_high(a, b, dims):
    return lax.dot_general(a, b, dims, precision=HIGH, preferred_element_type=F32)


def scalars(*values):
    return jnp.stack([jnp.asarray(v, jnp.int32) for v in values])


def column_block(cols):
    blocks = cols // LANES
    return LANES * max(k for k in range(1, 9) if blocks % k == 0)


def left_kernel(at, g, m, r, *rest):
    buffer, out = rest[-2:]
    step = pl.program_id(0)
    b = g[...] + m[...]
    buffer[...] = b
    bh, bl = split(b)
    rh, rl = split(r[...])
    term = dot3(bh, bl, rh, rl, NN)

    @pl.when(step == 0)
    def _():
        out[...] = term

    @pl.when(step > 0)
    def _():
        out[...] += term


def left_half(at, gradient, momentum, right_factor, buffer):
    rows, cols = gradient.shape
    rank = right_factor.shape[1]
    half, wide = rows // 2, column_block(cols)
    block = pl.BlockSpec((half, wide), lambda j, at: (at[0], j))
    first = buffer is None
    return pl.pallas_call(
        left_kernel,
        grid_spec=pltpu.PrefetchScalarGridSpec(
            num_scalar_prefetch=1,
            grid=(cols // wide,),
            in_specs=[block, block, pl.BlockSpec((wide, rank), lambda j, at: (j, 0))]
            + ([] if first else [ANY]),
            out_specs=[block, pl.BlockSpec((half, rank), lambda j, at: (0, 0))],
        ),
        out_shape=[
            jax.ShapeDtypeStruct((rows, cols), F32),
            jax.ShapeDtypeStruct((half, rank), F32),
        ],
        input_output_aliases={} if first else {4: 0},
        compiler_params=params(),
        cost_estimate=cost(6 * half * cols * rank, 4 * (3 * half * cols + cols * rank)),
        name="left_half",
    )(scalars(at), gradient, momentum, right_factor, *([] if first else [buffer]))


def gram_kernel(*refs):
    pieces, (left, lh, ll, gram) = refs[:-4], refs[-4:]
    n = pieces[0].shape[0]
    for i, piece in enumerate(pieces):
        x = piece[...]
        at = pl.ds(i * n, n)
        left[at, :] = x
        h, l = split(x)
        lh[at, :] = h
        ll[at, :] = l
    half = left.shape[0] // 2
    own, other = left[:half, :], left[half:, :]
    gram[...] = dot_high(own, own, TN) + dot_high(other, other, TN)


def gram_of(pieces):
    rank = pieces[0].shape[1]
    rows = sum(p.shape[0] for p in pieces)
    return pl.pallas_call(
        gram_kernel,
        out_shape=[
            jax.ShapeDtypeStruct((rows, rank), F32),
            jax.ShapeDtypeStruct((rows, rank), BF16),
            jax.ShapeDtypeStruct((rows, rank), BF16),
            jax.ShapeDtypeStruct((rank, rank), F32),
        ],
        compiler_params=params(),
        cost_estimate=cost(12 * rows * rank * rank, 12 * rows * rank),
        name="gram_of",
    )(*pieces)


def w_term(own, other, lh, ll):
    half = own.shape[0]
    total = None
    for ref, at in ((own, 0), (other, half)):
        bh, bl = split(ref[...])
        term = dot3(bh, bl, lh[at : at + half, :], ll[at : at + half, :], TN)
        total = term if total is None else total + term
    return total


def w_send_kernel(at, own, other, lh, ll, out):
    out[...] = w_term(own, other, lh, ll)


def w_keep_kernel(at, own, other, lh, ll, got, send, keep):
    total = w_term(own, other, lh, ll) + got[...]

    @pl.when(pl.program_id(0) == 0)
    def _():
        send[...] = total

    @pl.when(pl.program_id(0) == 1)
    def _():
        keep[...] = total


def w_specs(buffer, rank, unit):
    half = buffer.shape[0] // 2
    whole = pl.BlockSpec((2 * half, rank), lambda i, at: (0, 0))
    return [
        pl.BlockSpec((half, unit), lambda i, at: (at[0], at[2 + i])),
        pl.BlockSpec((half, unit), lambda i, at: (at[1], at[2 + i])),
        whole,
        whole,
    ]


def w_cost(buffer, rank, unit):
    rows = buffer.shape[0]
    return cost(2 * 6 * rows * unit * rank, 2 * 4 * (rows * unit + unit * rank))


def w_send(s, units, buffer, lh, ll, unit):
    rank = lh.shape[1]
    return pl.pallas_call(
        w_send_kernel,
        grid_spec=pltpu.PrefetchScalarGridSpec(
            num_scalar_prefetch=1,
            grid=(2,),
            in_specs=w_specs(buffer, rank, unit),
            out_specs=pl.BlockSpec((unit, rank), lambda i, at: (i, 0)),
        ),
        out_shape=jax.ShapeDtypeStruct((2 * unit, rank), F32),
        compiler_params=params(),
        cost_estimate=w_cost(buffer, rank, unit),
        name="w_send",
    )(scalars(s, 1 - s, *units), buffer, buffer, lh, ll)


def w_keep(s, units, order, buffer, lh, ll, got, unit):
    rank = lh.shape[1]
    one = pl.BlockSpec((unit, rank), lambda i, at: (0, 0))
    return pl.pallas_call(
        w_keep_kernel,
        grid_spec=pltpu.PrefetchScalarGridSpec(
            num_scalar_prefetch=1,
            grid=(2,),
            in_specs=w_specs(buffer, rank, unit)
            + [pl.BlockSpec((unit, rank), lambda i, at: (at[4 + i], 0))],
            out_specs=[one, one],
        ),
        out_shape=[jax.ShapeDtypeStruct((unit, rank), F32)] * 2,
        compiler_params=params(),
        cost_estimate=w_cost(buffer, rank, unit),
        name="w_keep",
    )(scalars(s, 1 - s, *units, *order), buffer, buffer, lh, ll, got)


GROUP = 8


def factor_group(rows, at):
    full = (GROUP, LANES)
    columns = [jnp.broadcast_to(rows[:, at + j : at + j + 1], full) for j in range(GROUP)]
    a = {
        (i, j): jnp.broadcast_to(columns[j][i : i + 1, :], full)
        for j in range(GROUP)
        for i in range(j, GROUP)
    }
    low, c = {}, {}
    for k in range(GROUP):
        c[k, k] = lax.rsqrt(a[k, k])
        for i in range(k + 1, GROUP):
            low[i, k] = a[i, k] * c[k, k]
        for j in range(k + 1, GROUP):
            for i in range(j, GROUP):
                a[i, j] = a[i, j] - low[i, k] * low[j, k]
        for j in range(k):
            total = low[k, j] * c[j, j]
            for i in range(j + 1, k):
                total = total + low[k, i] * c[i, j]
            c[k, j] = -c[k, k] * total
    return c


def spread(x, width):
    return jnp.concatenate([x] * (width // LANES), axis=1)


def eliminate(block):
    size, width = block.shape
    sub = lax.broadcasted_iota(jnp.int32, (GROUP, LANES), 0)
    groups = [block[i : i + GROUP, :] for i in range(0, size, GROUP)]
    for p in range(len(groups)):
        at = p * GROUP
        rows = groups[p]
        c = factor_group(rows, at)
        done = None
        for j in range(GROUP):
            col = jnp.zeros((GROUP, LANES), F32)
            for i in range(j, GROUP):
                col = jnp.where(sub == i, c[i, j], col)
            term = spread(col, width) * jnp.broadcast_to(rows[j : j + 1, :], (GROUP, width))
            done = term if done is None else done + term
        groups[p] = done
        if p + 1 == len(groups):
            break
        solved = None
        for k in range(GROUP):
            col = jnp.zeros((GROUP, LANES), F32)
            for j in range(k + 1):
                col = jnp.where(sub == j, c[k, j], col)
            term = spread(col, width) * jnp.broadcast_to(done[k : k + 1, :], (GROUP, width))
            solved = term if solved is None else solved + term
        for q in range(p + 1, len(groups)):
            x = groups[q]
            total = None
            for j in range(GROUP):
                term = jnp.broadcast_to(x[:, at + j : at + j + 1], (GROUP, width)) * jnp.broadcast_to(
                    solved[j : j + 1, :], (GROUP, width)
                )
                total = term if total is None else total + term
            groups[q] = x - total
    return jnp.concatenate(groups, axis=0)


def chol_kernel(gram, left, x_out, oh, ol, work):
    rank = gram.shape[0]
    size = min(64, rank)
    work[:, :rank] = gram[...]
    r = lax.broadcasted_iota(jnp.int32, (rank, rank), 0)
    c = lax.broadcasted_iota(jnp.int32, (rank, rank), 1)
    work[:, rank:] = jnp.where(r == c, 1.0, 0.0).astype(F32)

    def step(b, _):
        at = pl.multiple_of(b * size, size)
        rows = pl.ds(at, size)
        width = 2 * rank
        block = pltpu.roll(work[rows, :], lax.rem(width - at, width), 1)
        block = pltpu.roll(eliminate(block), at, 1)
        x_out[rows, :] = block[:, rank:]

        @pl.when(b + 1 < rank // size)
        def _():
            work[...] -= dot_high(block[:, :rank], block, TN)

        return 0

    lax.fori_loop(0, rank // size, step, 0)
    h, l = split(dot_high(left[...], x_out[...], NT))
    oh[...] = h
    ol[...] = l


def chol_inverse(gram, left):
    rows, rank = left.shape
    vm = pl.BlockSpec(memory_space=pltpu.VMEM)
    return pl.pallas_call(
        chol_kernel,
        in_specs=[vm, vm],
        out_specs=[vm] * 3,
        out_shape=[
            jax.ShapeDtypeStruct((rank, rank), F32),
            jax.ShapeDtypeStruct((rows, rank), BF16),
            jax.ShapeDtypeStruct((rows, rank), BF16),
        ],
        scratch_shapes=[pltpu.VMEM((rank, 2 * rank), F32)],
        compiler_params=params(),
        cost_estimate=cost(4e9, 4 * rows * rank),
        name="chol_inverse",
    )(gram, left)


def right_kernel(at, ka, ga, kb, gb, x, ra, rb, squares):
    rows, rank = ka.shape
    total = jnp.zeros((1, rank), F32)
    for i, (k, g, out) in enumerate(((ka, ga, ra), (kb, gb, rb))):
        value = dot_high(k[...] + g[...], x[...], NT)
        out[...] = value
        row = lax.broadcasted_iota(jnp.int32, (rows, rank), 0) + at[i]
        value = jnp.where(row < at[2], value, 0.0)
        total = total + jnp.sum(value * value, axis=0, keepdims=True)
    squares[...] = jnp.broadcast_to(total, squares.shape)


def right_rows(at_a, at_b, cols, ka, ga, kb, gb, x):
    rows, rank = ka.shape
    vm = pl.BlockSpec(memory_space=pltpu.VMEM)
    return pl.pallas_call(
        right_kernel,
        in_specs=[pl.BlockSpec(memory_space=pltpu.SMEM)] + [vm] * 5,
        out_specs=[vm] * 3,
        out_shape=[jax.ShapeDtypeStruct((rows, rank), F32)] * 2
        + [jax.ShapeDtypeStruct((GROUP, rank), F32)],
        compiler_params=params(),
        cost_estimate=cost(24 * rows * rank * rank, 24 * rows * rank),
        name="right_rows",
    )(scalars(at_a, at_b, cols), ka, ga, kb, gb, x)


def join_kernel(at, x, y, out):
    n = x.shape[0]
    out[pl.ds(pl.multiple_of(at[0] * n, GROUP), n), :] = x[...]
    out[pl.ds(pl.multiple_of((1 - at[0]) * n, GROUP), n), :] = y[...]


def join(t, x, y):
    rows, rank = x.shape
    vm = pl.BlockSpec(memory_space=pltpu.VMEM)
    return pl.pallas_call(
        join_kernel,
        in_specs=[pl.BlockSpec(memory_space=pltpu.SMEM), vm, vm],
        out_specs=vm,
        out_shape=jax.ShapeDtypeStruct((2 * rows, rank), F32),
        compiler_params=params(),
        cost_estimate=cost(rows * rank, 16 * rows * rank),
        name="join",
    )(scalars(t), x, y)


def final_kernel(count, total_cols, factor, at, *refs):
    pieces = refs[:count]
    squares, oh, ol, buffer = refs[count : count + 4]
    update, momentum, new_right, rh, rl, nh, nl = refs[-7:]
    u, h = pl.program_id(0), pl.program_id(1)
    half = buffer.shape[0]
    for k in range(count):

        @pl.when((u == k) & (h == 0))
        def _(k=k):
            right = pieces[k][...]
            scale = jnp.sqrt(squares[0:1, :] / total_cols + 1e-06)
            scaled = right / scale
            new_right[...] = scaled
            rh[...], rl[...] = split(right)
            nh[...], nl[...] = split(scaled)

    rows = pl.ds(pl.multiple_of(h * half, half), half)
    a, b = oh[rows, :], ol[rows, :]
    momentum[...] = buffer[...] - 0.05 * dot3(a, b, rh[...], rl[...], NT)
    update[...] = factor * dot3(a, b, nh[...], nl[...], NT)


def final(s, units, pieces, squares, oh, ol, buffer, total_rows, total_cols, before):
    rows, cols = buffer.shape
    unit, rank = pieces[0].shape
    half, count = rows // 2, len(pieces)
    wide = pl.BlockSpec((half, unit), lambda u, h, at: (at[h], at[2 + u]))
    whole = lambda shape: pl.BlockSpec(shape, lambda u, h, at: (0, 0))
    n_in = count + 5
    factor = (total_rows / rank) ** 0.5
    return pl.pallas_call(
        functools.partial(final_kernel, count, total_cols, factor),
        grid_spec=pltpu.PrefetchScalarGridSpec(
            num_scalar_prefetch=1,
            grid=(count, 2),
            in_specs=[whole((unit, rank))] * count
            + [whole((GROUP, rank)), whole((rows, rank)), whole((rows, rank)), wide]
            + [ANY] * len(before),
            out_specs=[wide, wide, pl.BlockSpec((unit, rank), lambda u, h, at: (at[2 + u], 0))],
            scratch_shapes=[pltpu.VMEM((unit, rank), BF16)] * 4,
        ),
        out_shape=[
            jax.ShapeDtypeStruct((rows, cols), F32),
            jax.ShapeDtypeStruct((rows, cols), F32),
            jax.ShapeDtypeStruct((cols, rank), F32),
        ],
        input_output_aliases={n_in + i: i for i in range(len(before))},
        compiler_params=params(),
        cost_estimate=cost(12 * count * rows * unit * rank, 4 * count * unit * (3 * rows + 2 * rank)),
        name="final",
    )(scalars(s, 1 - s, *units), *pieces, squares, oh, ol, buffer, *before)


def power_of_two(n):
    return n & (n - 1) == 0


def bits_of(n):
    return list(range(n.bit_length() - 1))


def swap(x, axis, bit):
    n = lax.axis_size(axis)
    return lax.ppermute(x, axis, [(i, i ^ (1 << bit)) for i in range(n)])


def sum_over(x, axis):
    n = lax.axis_size(axis)
    if not power_of_two(n):
        return lax.psum(x, axis)
    for bit in bits_of(n):
        y = swap(x, axis, bit)
        x = x + y
    return x


def on_device(gradient, momentum, right_factor):
    rows, cols = gradient.shape
    n_dp, n_tp = lax.axis_size("dp"), lax.axis_size("tensor")
    d, z = lax.axis_index("dp"), lax.axis_index("tensor")
    half = rows // 2

    s = lax.rem(z, 2)
    buffer, away = left_half(1 - s, gradient, momentum, right_factor, None)
    if power_of_two(n_tp) and n_tp > 1:
        got = swap(away, "tensor", 0)
        buffer, mine = left_half(s, gradient, momentum, right_factor, buffer)
        mine = mine + got
        own = [mine[: half // 2], mine[half // 2 :]]
        for bit in bits_of(n_tp)[1:]:
            own = [x + swap(x, "tensor", bit) for x in own]
        pieces = own + [swap(x, "tensor", 0) for x in own]
    else:
        buffer, mine = left_half(s, gradient, momentum, right_factor, buffer)
        both = lax.psum(jnp.where(s == 0, jnp.stack([mine, away]), jnp.stack([away, mine])), "tensor")
        pieces = [lax.dynamic_index_in_dim(both, i, 0, False) for i in (s, 1 - s)]

    left, lh, ll, gram = gram_of(pieces)
    gram = sum_over(gram, "dp")

    unit = LANES * (-(-cols // (8 * LANES)))
    bits = bits_of(n_dp)
    core = lax.rem(d, 2)
    orders = [bits[1:], bits[1:][::-1]]
    bit_of = lambda b: lax.rem(d // (1 << b), 2)
    got = []
    for h in range(2):
        units = [4 * h + 2 * (1 - core), 4 * h + 2 * (1 - core) + 1]
        sent = w_send(s, units, buffer, lh, ll, unit)
        got.append(swap(sent, "dp", 0))
    kept, here = [], []
    for h, order in enumerate(orders):
        t = bit_of(order[0])
        base = 4 * h + 2 * core
        send, keep = w_keep(s, [base + 1 - t, base + t], [1 - t, t], buffer, lh, ll, got[h], unit)
        at = (base + t) * unit
        recv = swap(send, "dp", order[0])
        for b in order[1:]:
            x = keep + recv
            n = x.shape[0] // 2
            t = bit_of(b)
            recv = swap(lax.dynamic_slice_in_dim(x, (1 - t) * n, n, 0), "dp", b)
            keep = lax.dynamic_slice_in_dim(x, t * n, n, 0)
            at = at + t * n
        kept.append((keep, recv))
        here.append(at)

    x_inv, oh, ol = chol_inverse(gram, left)
    ra, rb, squares = right_rows(here[0], here[1], cols, *kept[0], *kept[1], x_inv)
    squares = sum_over(sum_over(squares, "dp"), "tensor")

    near, far = [], []
    for h, (order, x) in enumerate(zip(orders, (ra, rb))):
        for b in order[:0:-1]:
            y = swap(x, "dp", b)
            x = join(bit_of(b), x, y)
        t = bit_of(order[0])
        y = swap(x, "dp", order[0])
        base, beside = 4 * h + 2 * core, 4 * h + 2 * (1 - core)
        near.append(((base + t, x), (beside + t, swap(x, "dp", 0))))
        far.append(((base + 1 - t, y), (beside + 1 - t, swap(y, "dp", 0))))

    outs = ()
    for group in (near, far):
        units = [u for part in group for u, _ in part]
        data = [x for part in group for _, x in part]
        outs = final(s, units, data, squares, oh, ol, buffer, rows * n_dp, cols * n_tp, outs)
    return tuple(outs)


def solution(mesh):
    return jax.shard_map(
        on_device,
        mesh=mesh,
        in_specs=(P("dp", "tensor"), P("dp", "tensor"), P("tensor", None)),
        out_specs=(P("dp", "tensor"), P("dp", "tensor"), P("tensor", None)),
        check_vma=False,
    )
```

```python
import functools

import jax
import jax.numpy as jnp
from jax import lax
from jax.experimental import pallas as pl
from jax.experimental.pallas import tpu as pltpu
from jax.sharding import PartitionSpec as P


F32 = jnp.float32
BF16 = jnp.bfloat16
HIGH = lax.Precision.HIGHEST
LANES = 128
VMEM_LIMIT = 40 * 1024 * 1024

NN = (((1,), (0,)), ((), ()))
NT = (((1,), (1,)), ((), ()))
TN = (((0,), (0,)), ((), ()))


ANY = pl.BlockSpec(memory_space=pl.ANY)
VMEM = pl.BlockSpec(memory_space=pltpu.VMEM)
SMEM = pl.BlockSpec(memory_space=pltpu.SMEM)


def params(**kw):
    return pltpu.CompilerParams(vmem_limit_bytes=VMEM_LIMIT, **kw)


def cost(flops, moved):
    return pl.CostEstimate(flops=int(flops), bytes_accessed=int(moved), transcendentals=0)


def split(x):
    hi = x.astype(BF16)
    lo = (x - hi.astype(F32)).astype(BF16)
    return hi, lo


def dot3(ah, al, bh, bl, dims):
    d = functools.partial(lax.dot_general, dimension_numbers=dims, preferred_element_type=F32)
    return d(ah, bh) + (d(ah, bl) + d(al, bh))


def dot_high(a, b, dims):
    return lax.dot_general(a, b, dims, precision=HIGH, preferred_element_type=F32)


def scalars(*values):
    return jnp.stack([jnp.asarray(v, jnp.int32) for v in values])


def column_block(cols):
    blocks = cols // LANES
    return LANES * max(k for k in range(1, 9) if blocks % k == 0)


def left_kernel(at, g, m, r, buffer, out, gs, ms, rs, sems):
    depth, half, wide = gs.shape
    steps = g.shape[1] // wide
    rows = pl.ds(pl.multiple_of(at[0] * half, GROUP), half)

    def copies(j, slot):
        part = pl.ds(pl.multiple_of(j * wide, LANES), wide)
        return (
            pltpu.make_async_copy(g.at[rows, part], gs.at[slot], sems.at[0, slot]),
            pltpu.make_async_copy(m.at[rows, part], ms.at[slot], sems.at[1, slot]),
            pltpu.make_async_copy(r.at[part, :], rs.at[slot], sems.at[2, slot]),
        )

    for j in range(min(depth, steps)):
        for copy in copies(j, j):
            copy.start()
    out[...] = jnp.zeros_like(out)

    def body(j, _):
        slot = lax.rem(j, depth)
        for copy in copies(j, slot):
            copy.wait()
        b = gs[slot] + ms[slot]
        buffer[:, pl.ds(pl.multiple_of(j * wide, LANES), wide)] = b
        bh, bl = split(b)
        rh, rl = split(rs[slot])
        out[...] += dot3(bh, bl, rh, rl, NN)

        @pl.when(j + depth < steps)
        def _():
            for copy in copies(j + depth, slot):
                copy.start()

        return 0

    lax.fori_loop(0, steps, body, 0)


def left_half(at, gradient, momentum, right_factor, padded):
    rows, cols = gradient.shape
    rank = right_factor.shape[1]
    half, wide, depth = rows // 2, column_block(cols), 4
    return pl.pallas_call(
        left_kernel,
        in_specs=[SMEM, ANY, ANY, ANY],
        out_specs=[VMEM, VMEM],
        out_shape=[pltpu.VMEM((half, padded), F32), jax.ShapeDtypeStruct((half, rank), F32)],
        scratch_shapes=[
            pltpu.VMEM((depth, half, wide), F32),
            pltpu.VMEM((depth, half, wide), F32),
            pltpu.VMEM((depth, wide, rank), F32),
            pltpu.SemaphoreType.DMA((3, depth)),
        ],
        compiler_params=params(),
        cost_estimate=cost(6 * half * cols * rank, 4 * (2 * half * cols + cols * rank)),
        name="left_half",
    )(scalars(at), gradient, momentum, right_factor)


def gram_kernel(*refs):
    pieces, (left, lh, ll, gram) = refs[:-4], refs[-4:]
    n = pieces[0].shape[0]
    for i, piece in enumerate(pieces):
        x = piece[...]
        at = pl.ds(i * n, n)
        left[at, :] = x
        h, l = split(x)
        lh[at, :] = h
        ll[at, :] = l
    half = left.shape[0] // 2
    own, other = left[:half, :], left[half:, :]
    gram[...] = dot_high(own, own, TN) + dot_high(other, other, TN)


def gram_of(pieces):
    rank = pieces[0].shape[1]
    rows = sum(p.shape[0] for p in pieces)
    return pl.pallas_call(
        gram_kernel,
        out_shape=[
            jax.ShapeDtypeStruct((rows, rank), F32),
            jax.ShapeDtypeStruct((rows, rank), BF16),
            jax.ShapeDtypeStruct((rows, rank), BF16),
            jax.ShapeDtypeStruct((rank, rank), F32),
        ],
        compiler_params=params(),
        cost_estimate=cost(12 * rows * rank * rank, 12 * rows * rank),
        name="gram_of",
    )(*pieces)


def w_term(unit, width, own, other, lh, ll):
    half = own.shape[0]
    part = pl.ds(pl.multiple_of(unit * width, LANES), width)
    total = None
    for ref, at in ((own, 0), (other, half)):
        bh, bl = split(ref[:, part])
        term = dot3(bh, bl, lh[at : at + half, :], ll[at : at + half, :], TN)
        total = term if total is None else total + term
    return total


def w_send_kernel(at, own, other, lh, ll, out):
    out[...] = w_term(at[pl.program_id(0)], out.shape[0], own, other, lh, ll)


def w_keep_kernel(at, own, other, lh, ll, got, send, keep):
    i, width = pl.program_id(0), send.shape[0]
    total = w_term(at[i], width, own, other, lh, ll) + got[...]

    @pl.when(i == 0)
    def _():
        send[...] = total

    @pl.when(i == 1)
    def _():
        keep[...] = total


def w_cost(rows, rank, unit):
    return cost(2 * 6 * rows * unit * rank, 2 * 4 * unit * rank)


def w_send(units, own, other, lh, ll, unit):
    rows, rank = lh.shape
    return pl.pallas_call(
        w_send_kernel,
        grid_spec=pltpu.PrefetchScalarGridSpec(
            num_scalar_prefetch=1,
            grid=(2,),
            in_specs=[VMEM] * 4,
            out_specs=pl.BlockSpec((unit, rank), lambda i, at: (i, 0)),
        ),
        out_shape=jax.ShapeDtypeStruct((2 * unit, rank), F32),
        compiler_params=params(),
        cost_estimate=w_cost(rows, rank, unit),
        name="w_send",
    )(scalars(*units), own, other, lh, ll)


def w_keep(units, order, own, other, lh, ll, got, unit):
    rows, rank = lh.shape
    one = pl.BlockSpec((unit, rank), lambda i, at: (0, 0))
    return pl.pallas_call(
        w_keep_kernel,
        grid_spec=pltpu.PrefetchScalarGridSpec(
            num_scalar_prefetch=1,
            grid=(2,),
            in_specs=[VMEM] * 4 + [pl.BlockSpec((unit, rank), lambda i, at: (at[2 + i], 0))],
            out_specs=[one, one],
        ),
        out_shape=[jax.ShapeDtypeStruct((unit, rank), F32)] * 2,
        compiler_params=params(),
        cost_estimate=w_cost(rows, rank, unit),
        name="w_keep",
    )(scalars(*units, *order), own, other, lh, ll, got)


GROUP = 8


def factor_group(rows, at):
    full = (GROUP, LANES)
    columns = [jnp.broadcast_to(rows[:, at + j : at + j + 1], full) for j in range(GROUP)]
    a = {
        (i, j): jnp.broadcast_to(columns[j][i : i + 1, :], full)
        for j in range(GROUP)
        for i in range(j, GROUP)
    }
    low, c = {}, {}
    for k in range(GROUP):
        c[k, k] = lax.rsqrt(a[k, k])
        for i in range(k + 1, GROUP):
            low[i, k] = a[i, k] * c[k, k]
        for j in range(k + 1, GROUP):
            for i in range(j, GROUP):
                a[i, j] = a[i, j] - low[i, k] * low[j, k]
        for j in range(k):
            total = low[k, j] * c[j, j]
            for i in range(j + 1, k):
                total = total + low[k, i] * c[i, j]
            c[k, j] = -c[k, k] * total
    return c


def spread(x, width):
    return jnp.concatenate([x] * (width // LANES), axis=1)


def eliminate(block):
    size, width = block.shape
    sub = lax.broadcasted_iota(jnp.int32, (GROUP, LANES), 0)
    groups = [block[i : i + GROUP, :] for i in range(0, size, GROUP)]
    for p in range(len(groups)):
        at = p * GROUP
        rows = groups[p]
        c = factor_group(rows, at)
        done = None
        for j in range(GROUP):
            col = jnp.zeros((GROUP, LANES), F32)
            for i in range(j, GROUP):
                col = jnp.where(sub == i, c[i, j], col)
            term = spread(col, width) * jnp.broadcast_to(rows[j : j + 1, :], (GROUP, width))
            done = term if done is None else done + term
        groups[p] = done
        if p + 1 == len(groups):
            break
        solved = None
        for k in range(GROUP):
            col = jnp.zeros((GROUP, LANES), F32)
            for j in range(k + 1):
                col = jnp.where(sub == j, c[k, j], col)
            term = spread(col, width) * jnp.broadcast_to(done[k : k + 1, :], (GROUP, width))
            solved = term if solved is None else solved + term
        for q in range(p + 1, len(groups)):
            x = groups[q]
            total = None
            for j in range(GROUP):
                term = jnp.broadcast_to(x[:, at + j : at + j + 1], (GROUP, width)) * jnp.broadcast_to(
                    solved[j : j + 1, :], (GROUP, width)
                )
                total = term if total is None else total + term
            groups[q] = x - total
    return jnp.concatenate(groups, axis=0)


def chol_kernel(gram, left, x_out, oh, ol, work):
    rank = gram.shape[0]
    size = min(64, rank)
    work[:, :rank] = gram[...]
    r = lax.broadcasted_iota(jnp.int32, (rank, rank), 0)
    c = lax.broadcasted_iota(jnp.int32, (rank, rank), 1)
    work[:, rank:] = jnp.where(r == c, 1.0, 0.0).astype(F32)

    def step(b, _):
        at = pl.multiple_of(b * size, size)
        rows = pl.ds(at, size)
        width = 2 * rank
        block = pltpu.roll(work[rows, :], lax.rem(width - at, width), 1)
        block = pltpu.roll(eliminate(block), at, 1)
        x_out[rows, :] = block[:, rank:]

        @pl.when(b + 1 < rank // size)
        def _():
            work[...] -= dot_high(block[:, :rank], block, TN)

        return 0

    lax.fori_loop(0, rank // size, step, 0)
    h, l = split(dot_high(left[...], x_out[...], NT))
    oh[...] = h
    ol[...] = l


def chol_inverse(gram, left):
    rows, rank = left.shape
    vm = pl.BlockSpec(memory_space=pltpu.VMEM)
    return pl.pallas_call(
        chol_kernel,
        in_specs=[vm, vm],
        out_specs=[vm] * 3,
        out_shape=[
            jax.ShapeDtypeStruct((rank, rank), F32),
            jax.ShapeDtypeStruct((rows, rank), BF16),
            jax.ShapeDtypeStruct((rows, rank), BF16),
        ],
        scratch_shapes=[pltpu.VMEM((rank, 2 * rank), F32)],
        compiler_params=params(),
        cost_estimate=cost(4e9, 4 * rows * rank),
        name="chol_inverse",
    )(gram, left)


def right_kernel(at, ka, ga, kb, gb, x, ra, rb, squares):
    rows, rank = ka.shape
    total = jnp.zeros((1, rank), F32)
    for i, (k, g, out) in enumerate(((ka, ga, ra), (kb, gb, rb))):
        value = dot_high(k[...] + g[...], x[...], NT)
        out[...] = value
        row = lax.broadcasted_iota(jnp.int32, (rows, rank), 0) + at[i]
        value = jnp.where(row < at[2], value, 0.0)
        total = total + jnp.sum(value * value, axis=0, keepdims=True)
    squares[...] = jnp.broadcast_to(total, squares.shape)


def right_rows(at_a, at_b, cols, ka, ga, kb, gb, x):
    rows, rank = ka.shape
    vm = pl.BlockSpec(memory_space=pltpu.VMEM)
    return pl.pallas_call(
        right_kernel,
        in_specs=[pl.BlockSpec(memory_space=pltpu.SMEM)] + [vm] * 5,
        out_specs=[vm] * 3,
        out_shape=[jax.ShapeDtypeStruct((rows, rank), F32)] * 2
        + [jax.ShapeDtypeStruct((GROUP, rank), F32)],
        compiler_params=params(),
        cost_estimate=cost(24 * rows * rank * rank, 24 * rows * rank),
        name="right_rows",
    )(scalars(at_a, at_b, cols), ka, ga, kb, gb, x)


def join_kernel(at, x, y, out):
    n = x.shape[0]
    out[pl.ds(pl.multiple_of(at[0] * n, GROUP), n), :] = x[...]
    out[pl.ds(pl.multiple_of((1 - at[0]) * n, GROUP), n), :] = y[...]


def join(t, x, y):
    rows, rank = x.shape
    vm = pl.BlockSpec(memory_space=pltpu.VMEM)
    return pl.pallas_call(
        join_kernel,
        in_specs=[pl.BlockSpec(memory_space=pltpu.SMEM), vm, vm],
        out_specs=vm,
        out_shape=jax.ShapeDtypeStruct((2 * rows, rank), F32),
        compiler_params=params(),
        cost_estimate=cost(rows * rank, 16 * rows * rank),
        name="join",
    )(scalars(t), x, y)


def final_kernel(count, total_cols, factor, at, *refs):
    pieces = refs[:count]
    squares, oh, ol, own, other = refs[count : count + 5]
    update, momentum, new_right, rh, rl, nh, nl = refs[-7:]
    u = pl.program_id(0)
    half, width = own.shape[0], new_right.shape[0]
    for k in range(count):

        @pl.when(u == k)
        def _(k=k):
            right = pieces[k][...]
            scale = jnp.sqrt(squares[0:1, :] / total_cols + 1e-06)
            scaled = right / scale
            new_right[...] = scaled
            rh[...], rl[...] = split(right)
            nh[...], nl[...] = split(scaled)

    part = pl.ds(pl.multiple_of(at[2 + u] * width, LANES), width)
    for h, buffer in enumerate((own, other)):
        rows = pl.ds(pl.multiple_of(at[h] * half, GROUP), half)
        a, b = oh[h * half : (h + 1) * half, :], ol[h * half : (h + 1) * half, :]
        momentum[rows, :] = buffer[:, part] - 0.05 * dot3(a, b, rh[...], rl[...], NT)
        update[rows, :] = factor * dot3(a, b, nh[...], nl[...], NT)


def final(s, units, pieces, squares, oh, ol, own, other, cols, total_rows, total_cols, before):
    rows = oh.shape[0]
    unit, rank = pieces[0].shape
    count = len(pieces)
    wide = pl.BlockSpec((rows, unit), lambda u, at: (0, at[2 + u]))
    factor = (total_rows / rank) ** 0.5
    return pl.pallas_call(
        functools.partial(final_kernel, count, total_cols, factor),
        grid_spec=pltpu.PrefetchScalarGridSpec(
            num_scalar_prefetch=1,
            grid=(count,),
            in_specs=[VMEM] * (count + 5) + [ANY] * len(before),
            out_specs=[wide, wide, pl.BlockSpec((unit, rank), lambda u, at: (at[2 + u], 0))],
            scratch_shapes=[pltpu.VMEM((unit, rank), BF16)] * 4,
        ),
        out_shape=[
            jax.ShapeDtypeStruct((rows, cols), F32),
            jax.ShapeDtypeStruct((rows, cols), F32),
            jax.ShapeDtypeStruct((cols, rank), F32),
        ],
        input_output_aliases={count + 6 + i: i for i in range(len(before))},
        compiler_params=params(),
        cost_estimate=cost(12 * count * rows * unit * rank, 4 * count * unit * (2 * rows + 2 * rank)),
        name="final",
    )(scalars(s, 1 - s, *units), *pieces, squares, oh, ol, own, other, *before)


def power_of_two(n):
    return n & (n - 1) == 0


def bits_of(n):
    return list(range(n.bit_length() - 1))


def swap(x, axis, *places):
    n = lax.axis_size(axis)
    mask = sum(1 << bit for bit in places)
    return lax.ppermute(x, axis, [(i, i ^ mask) for i in range(n)])


def sum_over(x, axis):
    n = lax.axis_size(axis)
    if not power_of_two(n):
        return lax.psum(x, axis)
    for bit in bits_of(n):
        y = swap(x, axis, bit)
        x = x + y
    return x


def on_device(gradient, momentum, right_factor):
    rows, cols = gradient.shape
    n_dp, n_tp = lax.axis_size("dp"), lax.axis_size("tensor")
    d, z = lax.axis_index("dp"), lax.axis_index("tensor")

    s = lax.rem(z, 2)
    unit = LANES * (-(-cols // (8 * LANES)))
    buffer_other, away = left_half(1 - s, gradient, momentum, right_factor, 8 * unit)
    if power_of_two(n_tp) and n_tp > 1:
        got = swap(away, "tensor", 0)
        buffer_own, mine = left_half(s, gradient, momentum, right_factor, 8 * unit)
        mine = mine + got
        own = [mine[: rows // 4], mine[rows // 4 :]]
        for bit in bits_of(n_tp)[1:]:
            own = [x + swap(x, "tensor", bit) for x in own]
        pieces = own + [swap(x, "tensor", 0) for x in own]
    else:
        buffer_own, mine = left_half(s, gradient, momentum, right_factor, 8 * unit)
        both = lax.psum(jnp.where(s == 0, jnp.stack([mine, away]), jnp.stack([away, mine])), "tensor")
        pieces = [lax.dynamic_index_in_dim(both, i, 0, False) for i in (s, 1 - s)]

    left, lh, ll, gram = gram_of(pieces)
    gram = sum_over(gram, "dp")

    bits = bits_of(n_dp)
    core = lax.rem(d, 2)
    orders = [bits[1:], bits[1:][::-1]]
    bit_of = lambda b: lax.rem(d // (1 << b), 2)
    got = []
    for h in range(2):
        units = [4 * h + 2 * (1 - core), 4 * h + 2 * (1 - core) + 1]
        sent = w_send(units, buffer_own, buffer_other, lh, ll, unit)
        got.append(swap(sent, "dp", 0))
    kept, here = [], []
    for h, order in enumerate(orders):
        t = bit_of(order[0])
        base = 4 * h + 2 * core
        units, places = [base + 1 - t, base + t], [1 - t, t]
        send, keep = w_keep(units, places, buffer_own, buffer_other, lh, ll, got[h], unit)
        at = (base + t) * unit
        recv = swap(send, "dp", order[0])
        for b in order[1:]:
            x = keep + recv
            n = x.shape[0] // 2
            t = bit_of(b)
            recv = swap(lax.dynamic_slice_in_dim(x, (1 - t) * n, n, 0), "dp", b)
            keep = lax.dynamic_slice_in_dim(x, t * n, n, 0)
            at = at + t * n
        kept.append((keep, recv))
        here.append(at)

    x_inv, oh, ol = chol_inverse(gram, left)
    ra, rb, squares = right_rows(here[0], here[1], cols, *kept[0], *kept[1], x_inv)
    squares = sum_over(squares, "tensor")
    for b in bits[:1] + bits[3:]:
        squares = squares + swap(squares, "dp", b)
    first, second = bits[1:3]
    others = [swap(squares, "dp", *m) for m in ((first,), (second,), (first, second))]
    squares = (squares + others[0]) + (others[1] + others[2])

    near, far = [], []
    for h, (order, x) in enumerate(zip(orders, (ra, rb))):
        for b in order[:0:-1]:
            y = swap(x, "dp", b)
            x = join(bit_of(b), x, y)
        t = bit_of(order[0])
        y = swap(x, "dp", order[0])
        base, beside = 4 * h + 2 * core, 4 * h + 2 * (1 - core)
        near.append(((base + t, x), (beside + t, swap(x, "dp", 0))))
        far.append(((base + 1 - t, y), (beside + 1 - t, swap(y, "dp", 0))))

    outs = ()
    for group in (near, far):
        units = [u for part in group for u, _ in part]
        data = [x for part in group for _, x in part]
        held = (squares, oh, ol, buffer_own, buffer_other)
        outs = final(s, units, data, *held, cols, rows * n_dp, cols * n_tp, outs)
    return tuple(outs)


def solution(mesh):
    return jax.shard_map(
        on_device,
        mesh=mesh,
        in_specs=(P("dp", "tensor"), P("dp", "tensor"), P("tensor", None)),
        out_specs=(P("dp", "tensor"), P("dp", "tensor"), P("tensor", None)),
        check_vma=False,
    )
```

```python
import functools

import jax
import jax.numpy as jnp
from jax import lax
from jax.experimental import pallas as pl
from jax.experimental.pallas import tpu as pltpu
from jax.sharding import PartitionSpec as P


F32 = jnp.float32
BF16 = jnp.bfloat16
HIGH = lax.Precision.HIGHEST
LANES = 128

NN = (((1,), (0,)), ((), ()))
NT = (((1,), (1,)), ((), ()))
TN = (((0,), (0,)), ((), ()))


HBM = pl.BlockSpec(memory_space=pltpu.HBM)
VMEM = pl.BlockSpec(memory_space=pltpu.VMEM)
SMEM = pl.BlockSpec(memory_space=pltpu.SMEM)


def params(mib):
    return pltpu.CompilerParams(vmem_limit_bytes=mib * 1024 * 1024)


def cost(flops, moved):
    return pl.CostEstimate(flops=int(flops), bytes_accessed=int(moved), transcendentals=0)


def split(x):
    hi = x.astype(BF16)
    lo = (x - hi.astype(F32)).astype(BF16)
    return hi, lo


def dot3(ah, al, bh, bl, dims):
    d = functools.partial(lax.dot_general, dimension_numbers=dims, preferred_element_type=F32)
    return d(ah, bh) + (d(ah, bl) + d(al, bh))


def dot_high(a, b, dims):
    return lax.dot_general(a, b, dims, precision=HIGH, preferred_element_type=F32)


def column_block(cols):
    blocks = cols // LANES
    return LANES * max(k for k in range(1, 9) if blocks % k == 0)


def left_kernel(which, at, g, m, r, buffer, out, gs, ms, rs, sems):
    depth, half, wide = gs.shape
    steps = g.shape[1] // wide
    rows = pl.ds(pl.multiple_of(at[which] * half, GROUP), half)

    def copies(j, slot):
        part = pl.ds(pl.multiple_of(j * wide, LANES), wide)
        return (
            pltpu.make_async_copy(g.at[rows, part], gs.at[slot], sems.at[0, slot]),
            pltpu.make_async_copy(m.at[rows, part], ms.at[slot], sems.at[1, slot]),
            pltpu.make_async_copy(r.at[part, :], rs.at[slot], sems.at[2, slot]),
        )

    for j in range(min(depth, steps)):
        for copy in copies(j, j):
            copy.start()
    out[...] = jnp.zeros_like(out)

    def body(j, _):
        slot = lax.rem(j, depth)
        for copy in copies(j, slot):
            copy.wait()
        b = gs[slot] + ms[slot]
        buffer[:, pl.ds(pl.multiple_of(j * wide, LANES), wide)] = b
        bh, bl = split(b)
        rh, rl = split(rs[slot])
        out[...] += dot3(bh, bl, rh, rl, NN)

        @pl.when(j + depth < steps)
        def _():
            for copy in copies(j + depth, slot):
                copy.start()

        return 0

    lax.fori_loop(0, steps, body, 0)


def left_half(at, which, gradient, momentum, right_factor, padded):
    rows, cols = gradient.shape
    rank = right_factor.shape[1]
    half, wide, depth = rows // 2, column_block(cols), 4
    return pl.pallas_call(
        functools.partial(left_kernel, which),
        in_specs=[SMEM, HBM, HBM, HBM],
        out_specs=[VMEM, VMEM],
        out_shape=[pltpu.VMEM((half, padded), F32), jax.ShapeDtypeStruct((half, rank), F32)],
        scratch_shapes=[
            pltpu.VMEM((depth, half, wide), F32),
            pltpu.VMEM((depth, half, wide), F32),
            pltpu.VMEM((depth, wide, rank), F32),
            pltpu.SemaphoreType.DMA((3, depth)),
        ],
        compiler_params=params(40),
        cost_estimate=cost(6 * half * cols * rank, 4 * (2 * half * cols + cols * rank)),
        name="left_half",
    )(at, gradient, momentum, right_factor)


def gram_kernel(*refs):
    pieces, (left, lh, ll, gram) = refs[:-4], refs[-4:]
    n = pieces[0].shape[0]
    for i, piece in enumerate(pieces):
        x = piece[...]
        at = pl.ds(i * n, n)
        left[at, :] = x
        h, l = split(x)
        lh[at, :] = h
        ll[at, :] = l
    half = left.shape[0] // 2
    own, other = left[:half, :], left[half:, :]
    gram[...] = dot_high(own, own, TN) + dot_high(other, other, TN)


def gram_of(pieces):
    rank = pieces[0].shape[1]
    rows = sum(p.shape[0] for p in pieces)
    return pl.pallas_call(
        gram_kernel,
        out_shape=[
            jax.ShapeDtypeStruct((rows, rank), F32),
            jax.ShapeDtypeStruct((rows, rank), BF16),
            jax.ShapeDtypeStruct((rows, rank), BF16),
            jax.ShapeDtypeStruct((rank, rank), F32),
        ],
        compiler_params=params(8),
        cost_estimate=cost(12 * rows * rank * rank, 12 * rows * rank),
        name="gram_of",
    )(*pieces)


def w_term(unit, width, own, other, lh, ll):
    half = own.shape[0]
    part = pl.ds(pl.multiple_of(unit * width, LANES), width)
    total = None
    for ref, at in ((own, 0), (other, half)):
        bh, bl = split(ref[:, part])
        term = dot3(bh, bl, lh[at : at + half, :], ll[at : at + half, :], TN)
        total = term if total is None else total + term
    return total


def w_send_kernel(place, at, own, other, lh, ll, out):
    out[...] = w_term(at[place + pl.program_id(0)], out.shape[0], own, other, lh, ll)


def w_keep_kernel(place, at, own, other, lh, ll, got, send, keep):
    i, width = pl.program_id(0), send.shape[0]
    total = w_term(at[place + i], width, own, other, lh, ll) + got[...]

    @pl.when(i == 0)
    def _():
        send[...] = total

    @pl.when(i == 1)
    def _():
        keep[...] = total


def w_cost(rows, rank, unit):
    return cost(2 * 6 * rows * unit * rank, 2 * 4 * unit * rank)


def w_send(at, place, own, other, lh, ll, unit):
    rows, rank = lh.shape
    return pl.pallas_call(
        functools.partial(w_send_kernel, place),
        grid_spec=pltpu.PrefetchScalarGridSpec(
            num_scalar_prefetch=1,
            grid=(2,),
            in_specs=[VMEM] * 4,
            out_specs=pl.BlockSpec((unit, rank), lambda i, at: (i, 0)),
        ),
        out_shape=jax.ShapeDtypeStruct((2 * unit, rank), F32),
        compiler_params=params(8),
        cost_estimate=w_cost(rows, rank, unit),
        name="w_send",
    )(at, own, other, lh, ll)


def w_keep(at, place, own, other, lh, ll, got, unit):
    rows, rank = lh.shape
    one = pl.BlockSpec((unit, rank), lambda i, at: (0, 0))
    return pl.pallas_call(
        functools.partial(w_keep_kernel, place),
        grid_spec=pltpu.PrefetchScalarGridSpec(
            num_scalar_prefetch=1,
            grid=(2,),
            in_specs=[VMEM] * 4 + [pl.BlockSpec((unit, rank), lambda i, at: (at[place + 2 + i], 0))],
            out_specs=[one, one],
        ),
        out_shape=[jax.ShapeDtypeStruct((unit, rank), F32)] * 2,
        compiler_params=params(10),
        cost_estimate=w_cost(rows, rank, unit),
        name="w_keep",
    )(at, own, other, lh, ll, got)


GROUP = 8


def factor_group(rows, at):
    full = (GROUP, LANES)
    columns = [jnp.broadcast_to(rows[:, at + j : at + j + 1], full) for j in range(GROUP)]
    a = {
        (i, j): jnp.broadcast_to(columns[j][i : i + 1, :], full)
        for j in range(GROUP)
        for i in range(j, GROUP)
    }
    low, c = {}, {}
    for k in range(GROUP):
        c[k, k] = lax.rsqrt(a[k, k])
        for i in range(k + 1, GROUP):
            low[i, k] = a[i, k] * c[k, k]
        for j in range(k + 1, GROUP):
            for i in range(j, GROUP):
                a[i, j] = a[i, j] - low[i, k] * low[j, k]
        for j in range(k):
            total = low[k, j] * c[j, j]
            for i in range(j + 1, k):
                total = total + low[k, i] * c[i, j]
            c[k, j] = -c[k, k] * total
    return c


def spread(x, width):
    return jnp.concatenate([x] * (width // LANES), axis=1)


def eliminate(block):
    size, width = block.shape
    sub = lax.broadcasted_iota(jnp.int32, (GROUP, LANES), 0)
    groups = [block[i : i + GROUP, :] for i in range(0, size, GROUP)]
    for p in range(len(groups)):
        at = p * GROUP
        rows = groups[p]
        c = factor_group(rows, at)
        done = None
        for j in range(GROUP):
            col = jnp.zeros((GROUP, LANES), F32)
            for i in range(j, GROUP):
                col = jnp.where(sub == i, c[i, j], col)
            term = spread(col, width) * jnp.broadcast_to(rows[j : j + 1, :], (GROUP, width))
            done = term if done is None else done + term
        groups[p] = done
        if p + 1 == len(groups):
            break
        solved = None
        for k in range(GROUP):
            col = jnp.zeros((GROUP, LANES), F32)
            for j in range(k + 1):
                col = jnp.where(sub == j, c[k, j], col)
            term = spread(col, width) * jnp.broadcast_to(done[k : k + 1, :], (GROUP, width))
            solved = term if solved is None else solved + term
        for q in range(p + 1, len(groups)):
            x = groups[q]
            total = None
            for j in range(GROUP):
                term = jnp.broadcast_to(x[:, at + j : at + j + 1], (GROUP, width)) * jnp.broadcast_to(
                    solved[j : j + 1, :], (GROUP, width)
                )
                total = term if total is None else total + term
            groups[q] = x - total
    return jnp.concatenate(groups, axis=0)


def chol_kernel(gram, left, x_out, oh, ol, work):
    rank = gram.shape[0]
    size = min(64, rank)
    work[:, :rank] = gram[...]
    r = lax.broadcasted_iota(jnp.int32, (rank, rank), 0)
    c = lax.broadcasted_iota(jnp.int32, (rank, rank), 1)
    work[:, rank:] = jnp.where(r == c, 1.0, 0.0).astype(F32)

    def step(b, _):
        at = pl.multiple_of(b * size, size)
        rows = pl.ds(at, size)
        width = 2 * rank
        block = pltpu.roll(work[rows, :], lax.rem(width - at, width), 1)
        block = pltpu.roll(eliminate(block), at, 1)
        x_out[rows, :] = block[:, rank:]

        @pl.when(b + 1 < rank // size)
        def _():
            work[...] -= dot_high(block[:, :rank], block, TN)

        return 0

    lax.fori_loop(0, rank // size, step, 0)
    h, l = split(dot_high(left[...], x_out[...], NT))
    oh[...] = h
    ol[...] = l


def chol_inverse(gram, left):
    rows, rank = left.shape
    vm = pl.BlockSpec(memory_space=pltpu.VMEM)
    return pl.pallas_call(
        chol_kernel,
        in_specs=[vm, vm],
        out_specs=[vm] * 3,
        out_shape=[
            jax.ShapeDtypeStruct((rank, rank), F32),
            jax.ShapeDtypeStruct((rows, rank), BF16),
            jax.ShapeDtypeStruct((rows, rank), BF16),
        ],
        scratch_shapes=[pltpu.VMEM((rank, 2 * rank), F32)],
        compiler_params=params(8),
        cost_estimate=cost(4e9, 4 * rows * rank),
        name="chol_inverse",
    )(gram, left)


def right_kernel(place, cols, at, ka, ga, kb, gb, x, ra, rb, squares):
    rows, rank = ka.shape
    total = jnp.zeros((1, rank), F32)
    for i, (k, g, out) in enumerate(((ka, ga, ra), (kb, gb, rb))):
        value = dot_high(k[...] + g[...], x[...], NT)
        out[...] = value
        row = lax.broadcasted_iota(jnp.int32, (rows, rank), 0) + at[place + i]
        value = jnp.where(row < cols, value, 0.0)
        total = total + jnp.sum(value * value, axis=0, keepdims=True)
    squares[...] = jnp.broadcast_to(total, squares.shape)


def right_rows(at, place, cols, ka, ga, kb, gb, x):
    rows, rank = ka.shape
    vm = pl.BlockSpec(memory_space=pltpu.VMEM)
    return pl.pallas_call(
        functools.partial(right_kernel, place, cols),
        in_specs=[pl.BlockSpec(memory_space=pltpu.SMEM)] + [vm] * 5,
        out_specs=[vm] * 3,
        out_shape=[jax.ShapeDtypeStruct((rows, rank), F32)] * 2
        + [jax.ShapeDtypeStruct((GROUP, rank), F32)],
        compiler_params=params(8),
        cost_estimate=cost(24 * rows * rank * rank, 24 * rows * rank),
        name="right_rows",
    )(at, ka, ga, kb, gb, x)


def join_kernel(place, at, x, y, out):
    n, t = x.shape[0], at[place]
    out[pl.ds(pl.multiple_of(t * n, GROUP), n), :] = x[...]
    out[pl.ds(pl.multiple_of((1 - t) * n, GROUP), n), :] = y[...]


def join(at, place, x, y):
    rows, rank = x.shape
    return pl.pallas_call(
        functools.partial(join_kernel, place),
        in_specs=[SMEM, VMEM, VMEM],
        out_specs=VMEM,
        out_shape=jax.ShapeDtypeStruct((2 * rows, rank), F32),
        compiler_params=params(6),
        cost_estimate=cost(rows * rank, 16 * rows * rank),
        name="join",
    )(at, x, y)


def halve_kernel(place, at, x, y, send, keep):
    n, t = send.shape[0], at[place]
    for part, out in ((1 - t, send), (t, keep)):
        rows = pl.ds(pl.multiple_of(part * n, GROUP), n)
        out[...] = x[rows, :] + y[rows, :]


def halve(at, place, x, y):
    rows, rank = x.shape
    return pl.pallas_call(
        functools.partial(halve_kernel, place),
        in_specs=[SMEM, VMEM, VMEM],
        out_specs=[VMEM, VMEM],
        out_shape=[jax.ShapeDtypeStruct((rows // 2, rank), F32)] * 2,
        compiler_params=params(6),
        cost_estimate=cost(rows * rank, 12 * rows * rank),
        name="halve",
    )(at, x, y)


def final_kernel(place, count, total_cols, factor, at, *refs):
    pieces = refs[:count]
    squares, oh, ol, own, other = refs[count : count + 5]
    update, momentum, new_right, rh, rl, nh, nl = refs[-7:]
    u = pl.program_id(0)
    half, width = own.shape[0], new_right.shape[0]
    for k in range(count):

        @pl.when(u == k)
        def _(k=k):
            right = pieces[k][...]
            scale = jnp.sqrt(squares[0:1, :] / total_cols + 1e-06)
            scaled = right / scale
            new_right[...] = scaled
            rh[...], rl[...] = split(right)
            nh[...], nl[...] = split(scaled)

    part = pl.ds(pl.multiple_of(at[place + u] * width, LANES), width)
    for h, buffer in enumerate((own, other)):
        rows = pl.ds(pl.multiple_of(at[h] * half, GROUP), half)
        a, b = oh[h * half : (h + 1) * half, :], ol[h * half : (h + 1) * half, :]
        momentum[rows, :] = buffer[:, part] - 0.05 * dot3(a, b, rh[...], rl[...], NT)
        update[rows, :] = factor * dot3(a, b, nh[...], nl[...], NT)


def final(at, place, pieces, squares, oh, ol, own, other, cols, total_rows, total_cols, before):
    rows = oh.shape[0]
    unit, rank = pieces[0].shape
    count = len(pieces)
    wide = pl.BlockSpec((rows, unit), lambda u, at: (0, at[place + u]))
    factor = (total_rows / rank) ** 0.5
    return pl.pallas_call(
        functools.partial(final_kernel, place, count, total_cols, factor),
        grid_spec=pltpu.PrefetchScalarGridSpec(
            num_scalar_prefetch=1,
            grid=(count,),
            in_specs=[VMEM] * (count + 5) + [HBM] * len(before),
            out_specs=[wide, wide, pl.BlockSpec((unit, rank), lambda u, at: (at[place + u], 0))],
            scratch_shapes=[pltpu.VMEM((unit, rank), BF16)] * 4,
        ),
        out_shape=[
            jax.ShapeDtypeStruct((rows, cols), F32),
            jax.ShapeDtypeStruct((rows, cols), F32),
            jax.ShapeDtypeStruct((cols, rank), F32),
        ],
        input_output_aliases={count + 6 + i: i for i in range(len(before))},
        compiler_params=params(20),
        cost_estimate=cost(12 * count * rows * unit * rank, 4 * count * unit * (2 * rows + 2 * rank)),
        name="final",
    )(at, *pieces, squares, oh, ol, own, other, *before)


def power_of_two(n):
    return n & (n - 1) == 0


def bits_of(n):
    return list(range(n.bit_length() - 1))


def swap(x, axis, *places):
    n = lax.axis_size(axis)
    mask = sum(1 << bit for bit in places)
    return lax.ppermute(x, axis, [(i, i ^ mask) for i in range(n)])


def sum_over(x, axis):
    n = lax.axis_size(axis)
    if not power_of_two(n):
        return lax.psum(x, axis)
    for bit in bits_of(n):
        y = swap(x, axis, bit)
        x = x + y
    return x


def on_device(gradient, momentum, right_factor):
    rows, cols = gradient.shape
    n_dp, n_tp = lax.axis_size("dp"), lax.axis_size("tensor")
    d, z = lax.axis_index("dp"), lax.axis_index("tensor")
    bits = bits_of(n_dp)

    unit = LANES * (-(-cols // (8 * LANES)))
    orders = [bits[1:], bits[1:][::-1]]
    table = []

    def put(*values):
        table.extend(values)
        return len(table) - len(values)

    bit_of = lambda b: (d >> b) & 1
    s, core = z & 1, d & 1
    put(s, 1 - s)
    send_at, keep_at, bit_at, near, far, first = [], [], [], [], [], []
    for h, order in enumerate(orders):
        t = bit_of(order[0])
        base, beside = 4 * h + 2 * core, 4 * h + 2 * (1 - core)
        send_at.append(put(beside, beside + 1))
        keep_at.append(put(base + 1 - t, base + t, 1 - t, t))
        bit_at.append({b: put(bit_of(b)) for b in order[1:]})
        near += [base + t, beside + t]
        far += [base + 1 - t, beside + 1 - t]
        at, n = (base + t) * unit, unit
        for b in order[1:]:
            n = n // 2
            at = at + bit_of(b) * n
        first.append(at)
    near_at, far_at, first_at = put(*near), put(*far), put(*first)
    at = jnp.stack([jnp.asarray(v, jnp.int32) for v in table])

    inputs = (gradient, momentum, right_factor, 8 * unit)
    buffer_other, away = left_half(at, 1, *inputs)
    if power_of_two(n_tp) and n_tp > 1:
        got = swap(away, "tensor", 0)
        buffer_own, mine = left_half(at, 0, *inputs)
        mine = mine + got
        own = [mine[: rows // 4], mine[rows // 4 :]]
        for bit in bits_of(n_tp)[1:]:
            own = [x + swap(x, "tensor", bit) for x in own]
        pieces = own + [swap(x, "tensor", 0) for x in own]
    else:
        buffer_own, mine = left_half(at, 0, *inputs)
        both = lax.psum(jnp.where(s == 0, jnp.stack([mine, away]), jnp.stack([away, mine])), "tensor")
        pieces = [lax.dynamic_index_in_dim(both, i, 0, False) for i in (s, 1 - s)]

    left, lh, ll, gram = gram_of(pieces)
    gram = sum_over(gram, "dp")

    held = (buffer_own, buffer_other)
    got = []
    for h in range(2):
        sent = w_send(at, send_at[h], *held, lh, ll, unit)
        got.append(swap(sent, "dp", 0))
    kept = []
    for h, order in enumerate(orders):
        send, keep = w_keep(at, keep_at[h], *held, lh, ll, got[h], unit)
        recv = swap(send, "dp", order[0])
        for b in order[1:]:
            send, keep = halve(at, bit_at[h][b], keep, recv)
            recv = swap(send, "dp", b)
        kept += [keep, recv]

    x_inv, oh, ol = chol_inverse(gram, left)
    *right, squares = right_rows(at, first_at, cols, *kept, x_inv)
    squares = sum_over(squares, "tensor")
    for b in bits[:1] + bits[3:]:
        squares = squares + swap(squares, "dp", b)
    b, c = bits[1:3]
    others = [swap(squares, "dp", *m) for m in ((b,), (c,), (b, c))]
    squares = (squares + others[0]) + (others[1] + others[2])

    near, far = [], []
    for h, (order, x) in enumerate(zip(orders, right)):
        for b in order[:0:-1]:
            x = join(at, bit_at[h][b], x, swap(x, "dp", b))
        y = swap(x, "dp", order[0])
        near += [x, swap(x, "dp", 0)]
        far += [y, swap(y, "dp", 0)]

    outs = ()
    for place, data in ((near_at, near), (far_at, far)):
        sizes = (cols, rows * n_dp, cols * n_tp)
        outs = final(at, place, data, squares, oh, ol, *held, *sizes, outs)
    return tuple(outs)


def solution(mesh):
    return jax.shard_map(
        on_device,
        mesh=mesh,
        in_specs=(P("dp", "tensor"), P("dp", "tensor"), P("tensor", None)),
        out_specs=(P("dp", "tensor"), P("dp", "tensor"), P("tensor", None)),
        check_vma=False,
    )
```

```python
import functools

import jax
import jax.numpy as jnp
from jax import lax
from jax.experimental import pallas as pl
from jax.experimental.pallas import tpu as pltpu
from jax.sharding import PartitionSpec as P


F32 = jnp.float32
BF16 = jnp.bfloat16
HIGH = lax.Precision.HIGHEST
LANES = 128

NN = (((1,), (0,)), ((), ()))
NT = (((1,), (1,)), ((), ()))
TN = (((0,), (0,)), ((), ()))


HBM = pl.BlockSpec(memory_space=pltpu.HBM)
VMEM = pl.BlockSpec(memory_space=pltpu.VMEM)
SMEM = pl.BlockSpec(memory_space=pltpu.SMEM)


def params(mib):
    return pltpu.CompilerParams(vmem_limit_bytes=mib * 1024 * 1024)


def cost(flops, moved):
    return pl.CostEstimate(flops=int(flops), bytes_accessed=int(moved), transcendentals=0)


def split(x):
    hi = x.astype(BF16)
    lo = (x - hi.astype(F32)).astype(BF16)
    return hi, lo


def dot3(ah, al, bh, bl, dims):
    d = functools.partial(lax.dot_general, dimension_numbers=dims, preferred_element_type=F32)
    return d(ah, bh) + (d(ah, bl) + d(al, bh))


def dot_high(a, b, dims):
    return lax.dot_general(a, b, dims, precision=HIGH, preferred_element_type=F32)


def column_block(cols):
    blocks = cols // LANES
    return LANES * max(k for k in range(1, 9) if blocks % k == 0)


def left_kernel(which, at, g, m, r, buffer, out, gs, ms, rs, sems):
    depth, half, wide = gs.shape
    steps = g.shape[1] // wide
    rows = pl.ds(pl.multiple_of(at[which] * half, GROUP), half)

    def copies(j, slot):
        part = pl.ds(pl.multiple_of(j * wide, LANES), wide)
        return (
            pltpu.make_async_copy(g.at[rows, part], gs.at[slot], sems.at[0, slot]),
            pltpu.make_async_copy(m.at[rows, part], ms.at[slot], sems.at[1, slot]),
            pltpu.make_async_copy(r.at[part, :], rs.at[slot], sems.at[2, slot]),
        )

    for j in range(min(depth, steps)):
        for copy in copies(j, j):
            copy.start()
    out[...] = jnp.zeros_like(out)

    def body(j, _):
        slot = lax.rem(j, depth)
        for copy in copies(j, slot):
            copy.wait()
        b = gs[slot] + ms[slot]
        buffer[:, pl.ds(pl.multiple_of(j * wide, LANES), wide)] = b
        bh, bl = split(b)
        rh, rl = split(rs[slot])
        out[...] += dot3(bh, bl, rh, rl, NN)

        @pl.when(j + depth < steps)
        def _():
            for copy in copies(j + depth, slot):
                copy.start()

        return 0

    lax.fori_loop(0, steps, body, 0)


def left_half(at, which, gradient, momentum, right_factor, padded):
    rows, cols = gradient.shape
    rank = right_factor.shape[1]
    half, wide, depth = rows // 2, column_block(cols), 4
    return pl.pallas_call(
        functools.partial(left_kernel, which),
        in_specs=[SMEM, HBM, HBM, HBM],
        out_specs=[VMEM, VMEM],
        out_shape=[pltpu.VMEM((half, padded), F32), jax.ShapeDtypeStruct((half, rank), F32)],
        scratch_shapes=[
            pltpu.VMEM((depth, half, wide), F32),
            pltpu.VMEM((depth, half, wide), F32),
            pltpu.VMEM((depth, wide, rank), F32),
            pltpu.SemaphoreType.DMA((3, depth)),
        ],
        compiler_params=params(40),
        cost_estimate=cost(6 * half * cols * rank, 4 * (2 * half * cols + cols * rank)),
        name="left_half",
    )(at, gradient, momentum, right_factor)


def total_kernel(count, *refs):
    ins, outs = refs[:count], refs[count:]
    n = outs[0].shape[0]
    for i, out in enumerate(outs):
        terms = [x[i * n : (i + 1) * n, :] for x in ins]
        while len(terms) > 1:
            terms = [terms[k] + terms[k + 1] for k in range(0, len(terms), 2)]
        out[...] = terms[0]


def total(*blocks, parts=1):
    rows, rank = blocks[0].shape
    outs = pl.pallas_call(
        functools.partial(total_kernel, len(blocks)),
        in_specs=[VMEM] * len(blocks),
        out_specs=[VMEM] * parts,
        out_shape=[jax.ShapeDtypeStruct((rows // parts, rank), F32)] * parts,
        compiler_params=params(6),
        cost_estimate=cost(rows * rank, 4 * (len(blocks) + 1) * rows * rank),
        name="total",
    )(*blocks)
    return outs[0] if parts == 1 else outs


def gram_kernel(place, at, *refs):
    pieces, (left, lh, ll, send, keep, gram) = refs[:-6], refs[-6:]
    n = pieces[0].shape[0]
    for i, piece in enumerate(pieces):
        x = piece[...]
        rows = pl.ds(i * n, n)
        left[rows, :] = x
        lh[rows, :], ll[rows, :] = split(x)
    half = left.shape[0] // 2
    own, other = left[:half, :], left[half:, :]
    gram[...] = dot_high(own, own, TN) + dot_high(other, other, TN)
    n, core = send.shape[0], at[place]
    send[...] = gram[pl.ds(pl.multiple_of((1 - core) * n, GROUP), n), :]
    keep[...] = gram[pl.ds(pl.multiple_of(core * n, GROUP), n), :]


def gram_of(at, place, pieces):
    rank = pieces[0].shape[1]
    rows = sum(p.shape[0] for p in pieces)
    return pl.pallas_call(
        functools.partial(gram_kernel, place),
        in_specs=[SMEM] + [VMEM] * len(pieces),
        out_specs=[VMEM] * 5,
        out_shape=[
            jax.ShapeDtypeStruct((rows, rank), F32),
            jax.ShapeDtypeStruct((rows, rank), BF16),
            jax.ShapeDtypeStruct((rows, rank), BF16),
            jax.ShapeDtypeStruct((rank // 2, rank), F32),
            jax.ShapeDtypeStruct((rank // 2, rank), F32),
        ],
        scratch_shapes=[pltpu.VMEM((rank, rank), F32)],
        compiler_params=params(8),
        cost_estimate=cost(12 * rows * rank * rank, 12 * rows * rank),
        name="gram_of",
    )(at, *pieces)


def w_term(unit, width, own, other, lh, ll):
    part = pl.ds(pl.multiple_of(unit * width, LANES), width)
    bh, bl = split(jnp.concatenate([own[:, part], other[:, part]], axis=0))
    return dot3(bh, bl, lh[...], ll[...], TN)


def w_send_kernel(place, at, own, other, lh, ll, out):
    out[...] = w_term(at[place + pl.program_id(0)], out.shape[0], own, other, lh, ll)


def w_keep_kernel(place, at, own, other, lh, ll, got, send, keep):
    i, width = pl.program_id(0), send.shape[0]
    total = w_term(at[place + i], width, own, other, lh, ll) + got[...]

    @pl.when(i == 0)
    def _():
        send[...] = total

    @pl.when(i == 1)
    def _():
        keep[...] = total


def w_cost(rows, rank, unit):
    return cost(2 * 6 * rows * unit * rank, 2 * 4 * unit * rank)


def w_send(at, place, own, other, lh, ll, unit):
    rows, rank = lh.shape
    return pl.pallas_call(
        functools.partial(w_send_kernel, place),
        grid_spec=pltpu.PrefetchScalarGridSpec(
            num_scalar_prefetch=1,
            grid=(2,),
            in_specs=[VMEM] * 4,
            out_specs=pl.BlockSpec((unit, rank), lambda i, at: (i, 0)),
        ),
        out_shape=jax.ShapeDtypeStruct((2 * unit, rank), F32),
        compiler_params=params(12),
        cost_estimate=w_cost(rows, rank, unit),
        name="w_send",
    )(at, own, other, lh, ll)


def w_keep(at, place, own, other, lh, ll, got, unit):
    rows, rank = lh.shape
    one = pl.BlockSpec((unit, rank), lambda i, at: (0, 0))
    return pl.pallas_call(
        functools.partial(w_keep_kernel, place),
        grid_spec=pltpu.PrefetchScalarGridSpec(
            num_scalar_prefetch=1,
            grid=(2,),
            in_specs=[VMEM] * 4 + [pl.BlockSpec((unit, rank), lambda i, at: (at[place + 2 + i], 0))],
            out_specs=[one, one],
        ),
        out_shape=[jax.ShapeDtypeStruct((unit, rank), F32)] * 2,
        compiler_params=params(14),
        cost_estimate=w_cost(rows, rank, unit),
        name="w_keep",
    )(at, own, other, lh, ll, got)


GROUP = 8


def factor_group(rows, at):
    full = (GROUP, LANES)
    columns = [jnp.broadcast_to(rows[:, at + j : at + j + 1], full) for j in range(GROUP)]
    a = {
        (i, j): jnp.broadcast_to(columns[j][i : i + 1, :], full)
        for j in range(GROUP)
        for i in range(j, GROUP)
    }
    low, c = {}, {}
    for k in range(GROUP):
        c[k, k] = lax.rsqrt(a[k, k])
        for i in range(k + 1, GROUP):
            low[i, k] = a[i, k] * c[k, k]
        for j in range(k + 1, GROUP):
            for i in range(j, GROUP):
                a[i, j] = a[i, j] - low[i, k] * low[j, k]
        for j in range(k):
            total = low[k, j] * c[j, j]
            for i in range(j + 1, k):
                total = total + low[k, i] * c[i, j]
            c[k, j] = -c[k, k] * total
    return c


def spread(x, width):
    return jnp.concatenate([x] * (width // LANES), axis=1)


def eliminate(block):
    size, width = block.shape
    sub = lax.broadcasted_iota(jnp.int32, (GROUP, LANES), 0)
    groups = [block[i : i + GROUP, :] for i in range(0, size, GROUP)]
    for p in range(len(groups)):
        at = p * GROUP
        rows = groups[p]
        c = factor_group(rows, at)
        done = None
        for j in range(GROUP):
            col = jnp.zeros((GROUP, LANES), F32)
            for i in range(j, GROUP):
                col = jnp.where(sub == i, c[i, j], col)
            term = spread(col, width) * jnp.broadcast_to(rows[j : j + 1, :], (GROUP, width))
            done = term if done is None else done + term
        groups[p] = done
        if p + 1 == len(groups):
            break
        solved = None
        for k in range(GROUP):
            col = jnp.zeros((GROUP, LANES), F32)
            for j in range(k + 1):
                col = jnp.where(sub == j, c[k, j], col)
            term = spread(col, width) * jnp.broadcast_to(done[k : k + 1, :], (GROUP, width))
            solved = term if solved is None else solved + term
        for q in range(p + 1, len(groups)):
            x = groups[q]
            total = None
            for j in range(GROUP):
                term = jnp.broadcast_to(x[:, at + j : at + j + 1], (GROUP, width)) * jnp.broadcast_to(
                    solved[j : j + 1, :], (GROUP, width)
                )
                total = term if total is None else total + term
            groups[q] = x - total
    return jnp.concatenate(groups, axis=0)


def chol_kernel(place, at, mine, beside, left, x_out, oh, ol, work):
    n, rank = mine.shape
    size = min(64, rank)
    core = at[place]
    work[pl.ds(pl.multiple_of(core * n, GROUP), n), :rank] = mine[...]
    work[pl.ds(pl.multiple_of((1 - core) * n, GROUP), n), :rank] = beside[...]
    r = lax.broadcasted_iota(jnp.int32, (rank, rank), 0)
    c = lax.broadcasted_iota(jnp.int32, (rank, rank), 1)
    work[:, rank:] = jnp.where(r == c, 1.0, 0.0).astype(F32)

    def step(b, _):
        top = pl.multiple_of(b * size, size)
        rows = pl.ds(top, size)
        width = 2 * rank
        block = pltpu.roll(work[rows, :], lax.rem(width - top, width), 1)
        block = pltpu.roll(eliminate(block), top, 1)
        x_out[rows, :] = block[:, rank:]

        @pl.when(b + 1 < rank // size)
        def _():
            work[...] -= dot_high(block[:, :rank], block, TN)

        return 0

    lax.fori_loop(0, rank // size, step, 0)
    h, l = split(dot_high(left[...], x_out[...], NT))
    oh[...] = h
    ol[...] = l


def chol_inverse(at, place, mine, beside, left):
    rows, rank = left.shape
    return pl.pallas_call(
        functools.partial(chol_kernel, place),
        in_specs=[SMEM] + [VMEM] * 3,
        out_specs=[VMEM] * 3,
        out_shape=[
            jax.ShapeDtypeStruct((rank, rank), F32),
            jax.ShapeDtypeStruct((rows, rank), BF16),
            jax.ShapeDtypeStruct((rows, rank), BF16),
        ],
        scratch_shapes=[pltpu.VMEM((rank, 2 * rank), F32)],
        compiler_params=params(8),
        cost_estimate=cost(4e9, 4 * rows * rank),
        name="chol_inverse",
    )(at, mine, beside, left)


def right_kernel(place, cols, at, ka, ga, kb, gb, x, ra, rb, squares):
    rows, rank = ka.shape
    total = jnp.zeros((1, rank), F32)
    for i, (k, g, out) in enumerate(((ka, ga, ra), (kb, gb, rb))):
        value = dot_high(k[...] + g[...], x[...], NT)
        out[...] = value
        row = lax.broadcasted_iota(jnp.int32, (rows, rank), 0) + at[place + i]
        value = jnp.where(row < cols, value, 0.0)
        total = total + jnp.sum(value * value, axis=0, keepdims=True)
    squares[...] = jnp.broadcast_to(total, squares.shape)


def right_rows(at, place, cols, ka, ga, kb, gb, x):
    rows, rank = ka.shape
    vm = pl.BlockSpec(memory_space=pltpu.VMEM)
    return pl.pallas_call(
        functools.partial(right_kernel, place, cols),
        in_specs=[pl.BlockSpec(memory_space=pltpu.SMEM)] + [vm] * 5,
        out_specs=[vm] * 3,
        out_shape=[jax.ShapeDtypeStruct((rows, rank), F32)] * 2
        + [jax.ShapeDtypeStruct((GROUP, rank), F32)],
        compiler_params=params(8),
        cost_estimate=cost(24 * rows * rank * rank, 24 * rows * rank),
        name="right_rows",
    )(at, ka, ga, kb, gb, x)


def join_kernel(place, at, x, y, out):
    n, t = x.shape[0], at[place]
    out[pl.ds(pl.multiple_of(t * n, GROUP), n), :] = x[...]
    out[pl.ds(pl.multiple_of((1 - t) * n, GROUP), n), :] = y[...]


def join(at, place, x, y):
    rows, rank = x.shape
    return pl.pallas_call(
        functools.partial(join_kernel, place),
        in_specs=[SMEM, VMEM, VMEM],
        out_specs=VMEM,
        out_shape=jax.ShapeDtypeStruct((2 * rows, rank), F32),
        compiler_params=params(6),
        cost_estimate=cost(rows * rank, 16 * rows * rank),
        name="join",
    )(at, x, y)


def halve_kernel(place, at, x, y, send, keep):
    n, t = send.shape[0], at[place]
    for part, out in ((1 - t, send), (t, keep)):
        rows = pl.ds(pl.multiple_of(part * n, GROUP), n)
        out[...] = x[rows, :] + y[rows, :]


def halve(at, place, x, y):
    rows, rank = x.shape
    return pl.pallas_call(
        functools.partial(halve_kernel, place),
        in_specs=[SMEM, VMEM, VMEM],
        out_specs=[VMEM, VMEM],
        out_shape=[jax.ShapeDtypeStruct((rows // 2, rank), F32)] * 2,
        compiler_params=params(6),
        cost_estimate=cost(rows * rank, 12 * rows * rank),
        name="halve",
    )(at, x, y)


def final_kernel(place, count, total_cols, factor, at, *refs):
    pieces = refs[:count]
    squares, oh, ol, own, other = refs[count : count + 5]
    update, momentum, new_right, rh, rl, nh, nl = refs[-7:]
    u = pl.program_id(0)
    half, width = own.shape[0], new_right.shape[0]
    for k in range(count):

        @pl.when(u == k)
        def _(k=k):
            right = pieces[k][...]
            scale = jnp.sqrt(squares[0:1, :] / total_cols + 1e-06)
            scaled = right / scale
            new_right[...] = scaled
            rh[...], rl[...] = split(right)
            nh[...], nl[...] = split(scaled)

    part = pl.ds(pl.multiple_of(at[place + u] * width, LANES), width)
    for h, buffer in enumerate((own, other)):
        rows = pl.ds(pl.multiple_of(at[h] * half, GROUP), half)
        a, b = oh[h * half : (h + 1) * half, :], ol[h * half : (h + 1) * half, :]
        momentum[rows, :] = buffer[:, part] - 0.05 * dot3(a, b, rh[...], rl[...], NT)
        update[rows, :] = factor * dot3(a, b, nh[...], nl[...], NT)


def final(at, place, pieces, squares, oh, ol, own, other, cols, total_rows, total_cols, before):
    rows = oh.shape[0]
    unit, rank = pieces[0].shape
    count = len(pieces)
    wide = pl.BlockSpec((rows, unit), lambda u, at: (0, at[place + u]))
    factor = (total_rows / rank) ** 0.5
    return pl.pallas_call(
        functools.partial(final_kernel, place, count, total_cols, factor),
        grid_spec=pltpu.PrefetchScalarGridSpec(
            num_scalar_prefetch=1,
            grid=(count,),
            in_specs=[VMEM] * (count + 5) + [HBM] * len(before),
            out_specs=[wide, wide, pl.BlockSpec((unit, rank), lambda u, at: (at[place + u], 0))],
            scratch_shapes=[pltpu.VMEM((unit, rank), BF16)] * 4,
        ),
        out_shape=[
            jax.ShapeDtypeStruct((rows, cols), F32),
            jax.ShapeDtypeStruct((rows, cols), F32),
            jax.ShapeDtypeStruct((cols, rank), F32),
        ],
        input_output_aliases={count + 6 + i: i for i in range(len(before))},
        compiler_params=params(20),
        cost_estimate=cost(12 * count * rows * unit * rank, 4 * count * unit * (2 * rows + 2 * rank)),
        name="final",
    )(at, *pieces, squares, oh, ol, own, other, *before)


def power_of_two(n):
    return n & (n - 1) == 0


def bits_of(n):
    return list(range(n.bit_length() - 1))


def swap(x, axis, *places):
    n = lax.axis_size(axis)
    mask = sum(1 << bit for bit in places)
    return lax.ppermute(x, axis, [(i, i ^ mask) for i in range(n)])


def spread_sum(x, bits):
    for b in bits[3:]:
        x = total(x, swap(x, "dp", b))
    b, c = bits[1:3]
    others = [swap(x, "dp", *m) for m in ((b,), (c,), (b, c))]
    return total(x, *others)


def on_device(gradient, momentum, right_factor):
    rows, cols = gradient.shape
    n_dp, n_tp = lax.axis_size("dp"), lax.axis_size("tensor")
    d, z = lax.axis_index("dp"), lax.axis_index("tensor")
    bits = bits_of(n_dp)

    unit = LANES * (-(-cols // (8 * LANES)))
    orders = [bits[1:], bits[1:][::-1]]
    table = []

    def put(*values):
        table.extend(values)
        return len(table) - len(values)

    bit_of = lambda b: (d >> b) & 1
    s, core = z & 1, d & 1
    put(s, 1 - s)
    core_at = put(core)
    send_at, keep_at, bit_at, near, far, first = [], [], [], [], [], []
    for h, order in enumerate(orders):
        t = bit_of(order[0])
        base, beside = 4 * h + 2 * core, 4 * h + 2 * (1 - core)
        send_at.append(put(beside, beside + 1))
        keep_at.append(put(base + 1 - t, base + t, 1 - t, t))
        bit_at.append({b: put(bit_of(b)) for b in order[1:]})
        near += [base + t, beside + t]
        far += [base + 1 - t, beside + 1 - t]
        at, n = (base + t) * unit, unit
        for b in order[1:]:
            n = n // 2
            at = at + bit_of(b) * n
        first.append(at)
    near_at, far_at, first_at = put(*near), put(*far), put(*first)
    at = jnp.stack([jnp.asarray(v, jnp.int32) for v in table])

    inputs = (gradient, momentum, right_factor, 8 * unit)
    buffer_other, away = left_half(at, 1, *inputs)
    if power_of_two(n_tp) and n_tp > 1:
        got = swap(away, "tensor", 0)
        buffer_own, mine = left_half(at, 0, *inputs)
        own = list(total(mine, got, parts=2))
        for bit in bits_of(n_tp)[1:]:
            for i in range(2):
                got = swap(own[i], "tensor", bit)
                own[i] = total(own[i], got)
        pieces = own[:]
        for i in range(2):
            pieces.append(swap(own[i], "tensor", 0))
    else:
        buffer_own, mine = left_half(at, 0, *inputs)
        both = lax.psum(jnp.where(s == 0, jnp.stack([mine, away]), jnp.stack([away, mine])), "tensor")
        pieces = [lax.dynamic_index_in_dim(both, i, 0, False) for i in (s, 1 - s)]

    left, lh, ll, send, gram = gram_of(at, core_at, pieces)
    got = swap(send, "dp", 0)
    gram = spread_sum(total(gram, got), bits)
    gram_beside = swap(gram, "dp", 0)

    held = (buffer_own, buffer_other)
    got = []
    for h in range(2):
        sent = w_send(at, send_at[h], *held, lh, ll, unit)
        got.append(swap(sent, "dp", 0))
    kept = []
    for h, order in enumerate(orders):
        send, keep = w_keep(at, keep_at[h], *held, lh, ll, got[h], unit)
        recv = swap(send, "dp", order[0])
        for b in order[1:]:
            send, keep = halve(at, bit_at[h][b], keep, recv)
            recv = swap(send, "dp", b)
        kept += [keep, recv]

    x_inv, oh, ol = chol_inverse(at, core_at, gram, gram_beside, left)
    *right, squares = right_rows(at, first_at, cols, *kept, x_inv)
    if power_of_two(n_tp):
        for b in bits_of(n_tp):
            squares = total(squares, swap(squares, "tensor", b))
    else:
        squares = lax.psum(squares, "tensor")
    got = swap(squares, "dp", 0)
    squares = total(squares, got)
    squares = spread_sum(squares, bits)

    near, far = [], []
    for h, (order, x) in enumerate(zip(orders, right)):
        for b in order[:0:-1]:
            y = swap(x, "dp", b)
            x = join(at, bit_at[h][b], x, y)
        y = swap(x, "dp", order[0])
        near += [x, swap(x, "dp", 0)]
        far += [y, swap(y, "dp", 0)]

    outs = ()
    for place, data in ((near_at, near), (far_at, far)):
        sizes = (cols, rows * n_dp, cols * n_tp)
        outs = final(at, place, data, squares, oh, ol, *held, *sizes, outs)
    return tuple(outs)


def solution(mesh):
    return jax.shard_map(
        on_device,
        mesh=mesh,
        in_specs=(P("dp", "tensor"), P("dp", "tensor"), P("tensor", None)),
        out_specs=(P("dp", "tensor"), P("dp", "tensor"), P("tensor", None)),
        check_vma=False,
    )
```

```python
import functools

import jax
import jax.numpy as jnp
from jax import lax
from jax.experimental import pallas as pl
from jax.experimental.pallas import tpu as pltpu
from jax.sharding import PartitionSpec as P


F32 = jnp.float32
BF16 = jnp.bfloat16
HIGH = lax.Precision.HIGHEST
LANES = 128

NN = (((1,), (0,)), ((), ()))
NT = (((1,), (1,)), ((), ()))
TN = (((0,), (0,)), ((), ()))


HBM = pl.BlockSpec(memory_space=pltpu.HBM)
VMEM = pl.BlockSpec(memory_space=pltpu.VMEM)
SMEM = pl.BlockSpec(memory_space=pltpu.SMEM)


def params(mib):
    return pltpu.CompilerParams(vmem_limit_bytes=mib * 1024 * 1024)


def cost(flops, moved):
    return pl.CostEstimate(flops=int(flops), bytes_accessed=int(moved), transcendentals=0)


def split(x):
    hi = x.astype(BF16)
    lo = (x - hi.astype(F32)).astype(BF16)
    return hi, lo


def dot3(ah, al, bh, bl, dims):
    d = functools.partial(lax.dot_general, dimension_numbers=dims, preferred_element_type=F32)
    return d(ah, bh) + (d(ah, bl) + d(al, bh))


def dot_high(a, b, dims):
    return lax.dot_general(a, b, dims, precision=HIGH, preferred_element_type=F32)


def column_block(cols):
    blocks = cols // LANES
    return LANES * max(k for k in range(1, 9) if blocks % k == 0)


def left_kernel(which, at, g, m, r, buffer, out, gs, ms, rs, sems):
    depth, half, wide = gs.shape
    steps = g.shape[1] // wide
    rows = pl.ds(pl.multiple_of(at[which] * half, GROUP), half)

    def copies(j, slot):
        part = pl.ds(pl.multiple_of(j * wide, LANES), wide)
        return (
            pltpu.make_async_copy(g.at[rows, part], gs.at[slot], sems.at[0, slot]),
            pltpu.make_async_copy(m.at[rows, part], ms.at[slot], sems.at[1, slot]),
            pltpu.make_async_copy(r.at[part, :], rs.at[slot], sems.at[2, slot]),
        )

    for j in range(min(depth, steps)):
        for copy in copies(j, j):
            copy.start()
    out[...] = jnp.zeros_like(out)

    def body(j, _):
        slot = lax.rem(j, depth)
        for copy in copies(j, slot):
            copy.wait()
        b = gs[slot] + ms[slot]
        buffer[:, pl.ds(pl.multiple_of(j * wide, LANES), wide)] = b
        bh, bl = split(b)
        rh, rl = split(rs[slot])
        out[...] += dot3(bh, bl, rh, rl, NN)

        @pl.when(j + depth < steps)
        def _():
            for copy in copies(j + depth, slot):
                copy.start()

        return 0

    lax.fori_loop(0, steps, body, 0)


def left_half(at, which, gradient, momentum, right_factor, padded):
    rows, cols = gradient.shape
    rank = right_factor.shape[1]
    half, wide, depth = rows // 2, column_block(cols), 4
    return pl.pallas_call(
        functools.partial(left_kernel, which),
        in_specs=[SMEM, HBM, HBM, HBM],
        out_specs=[VMEM, VMEM],
        out_shape=[pltpu.VMEM((half, padded), F32), jax.ShapeDtypeStruct((half, rank), F32)],
        scratch_shapes=[
            pltpu.VMEM((depth, half, wide), F32),
            pltpu.VMEM((depth, half, wide), F32),
            pltpu.VMEM((depth, wide, rank), F32),
            pltpu.SemaphoreType.DMA((3, depth)),
        ],
        compiler_params=params(40),
        cost_estimate=cost(6 * half * cols * rank, 4 * (2 * half * cols + cols * rank)),
        name="left_half",
    )(at, gradient, momentum, right_factor)


def total_kernel(count, *refs):
    ins, outs = refs[:count], refs[count:]
    n = outs[0].shape[0]
    for i, out in enumerate(outs):
        terms = [x[i * n : (i + 1) * n, :] for x in ins]
        while len(terms) > 1:
            terms = [terms[k] + terms[k + 1] for k in range(0, len(terms), 2)]
        out[...] = terms[0]


def total(*blocks, parts=1):
    rows, rank = blocks[0].shape
    outs = pl.pallas_call(
        functools.partial(total_kernel, len(blocks)),
        in_specs=[VMEM] * len(blocks),
        out_specs=[VMEM] * parts,
        out_shape=[jax.ShapeDtypeStruct((rows // parts, rank), F32)] * parts,
        compiler_params=params(6),
        cost_estimate=cost(rows * rank, 4 * (len(blocks) + 1) * rows * rank),
        name="total",
    )(*blocks)
    return outs[0] if parts == 1 else outs


def gram_kernel(place, at, *refs):
    pieces, (left, lh, ll, send, keep, gram) = refs[:-6], refs[-6:]
    n = pieces[0].shape[0]
    for i, piece in enumerate(pieces):
        x = piece[...]
        rows = pl.ds(i * n, n)
        left[rows, :] = x
        lh[rows, :], ll[rows, :] = split(x)
    half = left.shape[0] // 2
    own, other = left[:half, :], left[half:, :]
    gram[...] = dot_high(own, own, TN) + dot_high(other, other, TN)
    n, core = send.shape[0], at[place]
    send[...] = gram[pl.ds(pl.multiple_of((1 - core) * n, GROUP), n), :]
    keep[...] = gram[pl.ds(pl.multiple_of(core * n, GROUP), n), :]


def gram_of(at, place, pieces):
    rank = pieces[0].shape[1]
    rows = sum(p.shape[0] for p in pieces)
    return pl.pallas_call(
        functools.partial(gram_kernel, place),
        in_specs=[SMEM] + [VMEM] * len(pieces),
        out_specs=[VMEM] * 5,
        out_shape=[
            jax.ShapeDtypeStruct((rows, rank), F32),
            jax.ShapeDtypeStruct((rows, rank), BF16),
            jax.ShapeDtypeStruct((rows, rank), BF16),
            jax.ShapeDtypeStruct((rank // 2, rank), F32),
            jax.ShapeDtypeStruct((rank // 2, rank), F32),
        ],
        scratch_shapes=[pltpu.VMEM((rank, rank), F32)],
        compiler_params=params(8),
        cost_estimate=cost(12 * rows * rank * rank, 12 * rows * rank),
        name="gram_of",
    )(at, *pieces)


def w_term(unit, width, own, other, lh, ll):
    part = pl.ds(pl.multiple_of(unit * width, LANES), width)
    bh, bl = split(jnp.concatenate([own[:, part], other[:, part]], axis=0))
    return dot3(bh, bl, lh[...], ll[...], TN)


def w_send_kernel(place, at, own, other, lh, ll, out):
    out[...] = w_term(at[place + pl.program_id(0)], out.shape[0], own, other, lh, ll)


def w_keep_kernel(place, at, own, other, lh, ll, got, send, keep):
    i, width = pl.program_id(0), send.shape[0]
    total = w_term(at[place + i], width, own, other, lh, ll) + got[...]

    @pl.when(i == 0)
    def _():
        send[...] = total

    @pl.when(i == 1)
    def _():
        keep[...] = total


def w_cost(rows, rank, unit):
    return cost(2 * 6 * rows * unit * rank, 2 * 4 * unit * rank)


def w_send(at, place, own, other, lh, ll, unit):
    rows, rank = lh.shape
    return pl.pallas_call(
        functools.partial(w_send_kernel, place),
        grid_spec=pltpu.PrefetchScalarGridSpec(
            num_scalar_prefetch=1,
            grid=(2,),
            in_specs=[VMEM] * 4,
            out_specs=pl.BlockSpec((unit, rank), lambda i, at: (i, 0)),
        ),
        out_shape=jax.ShapeDtypeStruct((2 * unit, rank), F32),
        compiler_params=params(12),
        cost_estimate=w_cost(rows, rank, unit),
        name="w_send",
    )(at, own, other, lh, ll)


def w_keep(at, place, own, other, lh, ll, got, unit):
    rows, rank = lh.shape
    one = pl.BlockSpec((unit, rank), lambda i, at: (0, 0))
    return pl.pallas_call(
        functools.partial(w_keep_kernel, place),
        grid_spec=pltpu.PrefetchScalarGridSpec(
            num_scalar_prefetch=1,
            grid=(2,),
            in_specs=[VMEM] * 4 + [pl.BlockSpec((unit, rank), lambda i, at: (at[place + 2 + i], 0))],
            out_specs=[one, one],
        ),
        out_shape=[jax.ShapeDtypeStruct((unit, rank), F32)] * 2,
        compiler_params=params(14),
        cost_estimate=w_cost(rows, rank, unit),
        name="w_keep",
    )(at, own, other, lh, ll, got)


GROUP = 8


def factor_group(rows, at):
    full = (GROUP, LANES)
    columns = [jnp.broadcast_to(rows[:, at + j : at + j + 1], full) for j in range(GROUP)]
    a = {
        (i, j): jnp.broadcast_to(columns[j][i : i + 1, :], full)
        for j in range(GROUP)
        for i in range(j, GROUP)
    }
    low, c = {}, {}
    for k in range(GROUP):
        c[k, k] = lax.rsqrt(a[k, k])
        for i in range(k + 1, GROUP):
            low[i, k] = a[i, k] * c[k, k]
        for j in range(k + 1, GROUP):
            for i in range(j, GROUP):
                a[i, j] = a[i, j] - low[i, k] * low[j, k]
        for j in range(k):
            total = low[k, j] * c[j, j]
            for i in range(j + 1, k):
                total = total + low[k, i] * c[i, j]
            c[k, j] = -c[k, k] * total
    return c


def spread(x, width):
    return jnp.concatenate([x] * (width // LANES), axis=1)


def eliminate(block):
    size, width = block.shape
    sub = lax.broadcasted_iota(jnp.int32, (GROUP, LANES), 0)
    groups = [block[i : i + GROUP, :] for i in range(0, size, GROUP)]
    for p in range(len(groups)):
        at = p * GROUP
        rows = groups[p]
        c = factor_group(rows, at)
        done = None
        for j in range(GROUP):
            col = jnp.zeros((GROUP, LANES), F32)
            for i in range(j, GROUP):
                col = jnp.where(sub == i, c[i, j], col)
            term = spread(col, width) * jnp.broadcast_to(rows[j : j + 1, :], (GROUP, width))
            done = term if done is None else done + term
        groups[p] = done
        if p + 1 == len(groups):
            break
        solved = None
        for k in range(GROUP):
            col = jnp.zeros((GROUP, LANES), F32)
            for j in range(k + 1):
                col = jnp.where(sub == j, c[k, j], col)
            term = spread(col, width) * jnp.broadcast_to(done[k : k + 1, :], (GROUP, width))
            solved = term if solved is None else solved + term
        for q in range(p + 1, len(groups)):
            x = groups[q]
            total = None
            for j in range(GROUP):
                term = jnp.broadcast_to(x[:, at + j : at + j + 1], (GROUP, width)) * jnp.broadcast_to(
                    solved[j : j + 1, :], (GROUP, width)
                )
                total = term if total is None else total + term
            groups[q] = x - total
    return jnp.concatenate(groups, axis=0)


def chol_kernel(place, at, mine, beside, left, x_out, oh, ol, work):
    n, rank = mine.shape
    size = min(64, rank)
    core = at[place]
    work[pl.ds(pl.multiple_of(core * n, GROUP), n), :rank] = mine[...]
    work[pl.ds(pl.multiple_of((1 - core) * n, GROUP), n), :rank] = beside[...]
    r = lax.broadcasted_iota(jnp.int32, (rank, rank), 0)
    c = lax.broadcasted_iota(jnp.int32, (rank, rank), 1)
    work[:, rank:] = jnp.where(r == c, 1.0, 0.0).astype(F32)

    def step(b, _):
        top = pl.multiple_of(b * size, size)
        rows = pl.ds(top, size)
        width = 2 * rank
        block = pltpu.roll(work[rows, :], lax.rem(width - top, width), 1)
        block = pltpu.roll(eliminate(block), top, 1)
        x_out[rows, :] = block[:, rank:]

        @pl.when(b + 1 < rank // size)
        def _():
            work[...] -= dot_high(block[:, :rank], block, TN)

        return 0

    lax.fori_loop(0, rank // size, step, 0)
    h, l = split(dot_high(left[...], x_out[...], NT))
    oh[...] = h
    ol[...] = l


def chol_inverse(at, place, mine, beside, left):
    rows, rank = left.shape
    return pl.pallas_call(
        functools.partial(chol_kernel, place),
        in_specs=[SMEM] + [VMEM] * 3,
        out_specs=[VMEM] * 3,
        out_shape=[
            jax.ShapeDtypeStruct((rank, rank), F32),
            jax.ShapeDtypeStruct((rows, rank), BF16),
            jax.ShapeDtypeStruct((rows, rank), BF16),
        ],
        scratch_shapes=[pltpu.VMEM((rank, 2 * rank), F32)],
        compiler_params=params(8),
        cost_estimate=cost(4e9, 4 * rows * rank),
        name="chol_inverse",
    )(at, mine, beside, left)


def right_kernel(place, cols, at, ka, ga, kb, gb, x, ra, rb, squares):
    rows, rank = ka.shape
    total = jnp.zeros((1, rank), F32)
    for i, (k, g, out) in enumerate(((ka, ga, ra), (kb, gb, rb))):
        value = dot_high(k[...] + g[...], x[...], NT)
        out[...] = value
        row = lax.broadcasted_iota(jnp.int32, (rows, rank), 0) + at[place + i]
        value = jnp.where(row < cols, value, 0.0)
        total = total + jnp.sum(value * value, axis=0, keepdims=True)
    squares[...] = jnp.broadcast_to(total, squares.shape)


def right_rows(at, place, cols, ka, ga, kb, gb, x):
    rows, rank = ka.shape
    vm = pl.BlockSpec(memory_space=pltpu.VMEM)
    return pl.pallas_call(
        functools.partial(right_kernel, place, cols),
        in_specs=[pl.BlockSpec(memory_space=pltpu.SMEM)] + [vm] * 5,
        out_specs=[vm] * 3,
        out_shape=[jax.ShapeDtypeStruct((rows, rank), F32)] * 2
        + [jax.ShapeDtypeStruct((GROUP, rank), F32)],
        compiler_params=params(8),
        cost_estimate=cost(24 * rows * rank * rank, 24 * rows * rank),
        name="right_rows",
    )(at, ka, ga, kb, gb, x)


def join_kernel(place, at, x, y, *rest):
    outs, both = rest[:-1], rest[-1]
    n, t = x.shape[0], at[place]
    both[pl.ds(pl.multiple_of(t * n, GROUP), n), :] = x[...]
    both[pl.ds(pl.multiple_of((1 - t) * n, GROUP), n), :] = y[...]
    top = 0
    for out in outs:
        out[...] = both[top : top + out.shape[0], :]
        top += out.shape[0]


def join(at, place, x, y, sizes):
    rows, rank = x.shape
    return pl.pallas_call(
        functools.partial(join_kernel, place),
        in_specs=[SMEM, VMEM, VMEM],
        out_specs=[VMEM] * len(sizes),
        out_shape=[jax.ShapeDtypeStruct((n, rank), F32) for n in sizes],
        scratch_shapes=[pltpu.VMEM((2 * rows, rank), F32)],
        compiler_params=params(6),
        cost_estimate=cost(rows * rank, 16 * rows * rank),
        name="join",
    )(at, x, y)


def halve_kernel(place, at, x, y, send, keep):
    n, t = send.shape[0], at[place]
    for part, out in ((1 - t, send), (t, keep)):
        rows = pl.ds(pl.multiple_of(part * n, GROUP), n)
        out[...] = x[rows, :] + y[rows, :]


def halve(at, place, x, y):
    rows, rank = x.shape
    return pl.pallas_call(
        functools.partial(halve_kernel, place),
        in_specs=[SMEM, VMEM, VMEM],
        out_specs=[VMEM, VMEM],
        out_shape=[jax.ShapeDtypeStruct((rows // 2, rank), F32)] * 2,
        compiler_params=params(6),
        cost_estimate=cost(rows * rank, 12 * rows * rank),
        name="halve",
    )(at, x, y)


def final_kernel(place, groups, unit, parts, total_cols, factor, at, *refs):
    refs = list(refs)
    take = lambda n: [refs.pop(0) for _ in range(n)]
    pieces = [take(4) for _ in groups]
    squares, oh, ol, own, other = take(5)
    del refs[: len(refs) - 3 - 6 * len(groups)]
    update, momentum, new_right = take(3)
    half = own.shape[0]
    blocks = update.shape[1] // LANES
    halves = [pl.ds(pl.multiple_of(at[h] * half, GROUP), half) for h in range(2)]

    def copies(group, k, stage_m, stage_u, stage_r, sems):
        start, count = group
        first = at[place + k] * (unit // LANES) + start
        for j in range(count):
            here = pl.ds(j * LANES, LANES)
            there = pl.ds(pl.multiple_of((first + j) * LANES, LANES), LANES)
            both = []
            if "m" in parts:
                both.append((stage_m.at[k, :, here], momentum.at[:, there]))
            if "u" in parts:
                both.append((stage_u.at[k, :, here], update.at[:, there]))
                both.append((stage_r.at[k, here, :], new_right.at[there, :]))
            yield first + j < blocks, [
                pltpu.make_async_copy(a, b, sems.at[i, k, j]) for i, (a, b) in enumerate(both)
            ]

    stages = []
    for group, data in zip(groups, pieces):
        stage_m, stage_u, stage_r, high, low, sems = take(6)
        stages.append((stage_m, stage_u, stage_r, sems))
        start, count = group
        n = count * LANES

        def body(k, _):
            def load(scaled):
                for i, piece in enumerate(data):

                    @pl.when(k == i)
                    def _(piece=piece):
                        x = piece[...]
                        if scaled:
                            x = x / jnp.sqrt(squares[0:1, :] / total_cols + 1e-06)
                            stage_r[k] = x
                        high[...], low[...] = split(x)

            if "m" in parts:
                load(False)
                value = 0.05 * dot3(oh[...], ol[...], high[...], low[...], NT)
                part = pl.ds(pl.multiple_of(at[place + k] * unit + start * LANES, LANES), n)
                stage_m[k, halves[0], :] = own[:, part] - value[:half]
                stage_m[k, halves[1], :] = other[:, part] - value[half:]
            if "u" in parts:
                load(True)
                value = factor * dot3(oh[...], ol[...], high[...], low[...], NT)
                stage_u[k, halves[0], :] = value[:half]
                stage_u[k, halves[1], :] = value[half:]
            for inside, some in copies(group, k, stage_m, stage_u, stage_r, sems):

                @pl.when(inside)
                def _(some=some):
                    for copy in some:
                        copy.start()

            return 0

        lax.fori_loop(0, 4, body, 0)

    for group, stage in zip(groups, stages):

        def finish(k, _):
            for inside, some in copies(group, k, *stage):

                @pl.when(inside)
                def _(some=some):
                    for copy in some:
                        copy.wait()

            return 0

        lax.fori_loop(0, 4, finish, 0)


def final(at, place, groups, unit, parts, pieces, squares, oh, ol, own, other, sizes, before):
    rows, rank = oh.shape
    cols, total_rows, total_cols = sizes
    factor = (total_rows / rank) ** 0.5
    m, u = "m" in parts, "u" in parts
    scratch = []
    for _, count in groups:
        n = count * LANES
        tiny = (4, GROUP, LANES)
        scratch += [
            pltpu.VMEM((4, rows, n) if m else tiny, F32),
            pltpu.VMEM((4, rows, n) if u else tiny, F32),
            pltpu.VMEM((4, n, rank) if u else tiny, F32),
            pltpu.VMEM((n, rank), BF16),
            pltpu.VMEM((n, rank), BF16),
            pltpu.SemaphoreType.DMA((3, 4, count)),
        ]
    width = 4 * sum(count for _, count in groups) * LANES
    return pl.pallas_call(
        functools.partial(final_kernel, place, groups, unit, parts, total_cols, factor),
        in_specs=[SMEM] + [VMEM] * (len(pieces) + 5) + [HBM] * len(before),
        out_specs=[HBM] * 3,
        out_shape=[
            jax.ShapeDtypeStruct((rows, cols), F32),
            jax.ShapeDtypeStruct((rows, cols), F32),
            jax.ShapeDtypeStruct((cols, rank), F32),
        ],
        scratch_shapes=scratch,
        input_output_aliases={len(pieces) + 6 + i: i for i in range(len(before))},
        compiler_params=params(20),
        cost_estimate=cost(6 * len(parts) * rows * width * rank, 4 * len(parts) * rows * width),
        name="final",
    )(at, *pieces, squares, oh, ol, own, other, *before)


def power_of_two(n):
    return n & (n - 1) == 0


def bits_of(n):
    return list(range(n.bit_length() - 1))


def swap(x, axis, *places):
    n = lax.axis_size(axis)
    mask = sum(1 << bit for bit in places)
    return lax.ppermute(x, axis, [(i, i ^ mask) for i in range(n)])


def spread_sum(x, bits):
    for b in bits[3:]:
        x = total(x, swap(x, "dp", b))
    b, c = bits[1:3]
    others = [swap(x, "dp", *m) for m in ((b,), (c,), (b, c))]
    return total(x, *others)


def on_device(gradient, momentum, right_factor):
    rows, cols = gradient.shape
    n_dp, n_tp = lax.axis_size("dp"), lax.axis_size("tensor")
    d, z = lax.axis_index("dp"), lax.axis_index("tensor")
    bits = bits_of(n_dp)

    unit = LANES * (-(-cols // (8 * LANES)))
    orders = [bits[1:], bits[1:][::-1]]
    table = []

    def put(*values):
        table.extend(values)
        return len(table) - len(values)

    bit_of = lambda b: (d >> b) & 1
    s, core = z & 1, d & 1
    put(s, 1 - s)
    core_at = put(core)
    send_at, keep_at, bit_at, near, far, first = [], [], [], [], [], []
    for h, order in enumerate(orders):
        t = bit_of(order[0])
        base, beside = 4 * h + 2 * core, 4 * h + 2 * (1 - core)
        send_at.append(put(beside, beside + 1))
        keep_at.append(put(base + 1 - t, base + t, 1 - t, t))
        bit_at.append({b: put(bit_of(b)) for b in order[1:]})
        near += [base + t, beside + t]
        far += [base + 1 - t, beside + 1 - t]
        at, n = (base + t) * unit, unit
        for b in order[1:]:
            n = n // 2
            at = at + bit_of(b) * n
        first.append(at)
    near_at, far_at, first_at = put(*near), put(*far), put(*first)
    at = jnp.stack([jnp.asarray(v, jnp.int32) for v in table])

    inputs = (gradient, momentum, right_factor, 8 * unit)
    buffer_other, away = left_half(at, 1, *inputs)
    if power_of_two(n_tp) and n_tp > 1:
        got = swap(away, "tensor", 0)
        buffer_own, mine = left_half(at, 0, *inputs)
        own = list(total(mine, got, parts=2))
        for bit in bits_of(n_tp)[1:]:
            for i in range(2):
                got = swap(own[i], "tensor", bit)
                own[i] = total(own[i], got)
        pieces = own[:]
        for i in range(2):
            pieces.append(swap(own[i], "tensor", 0))
    else:
        buffer_own, mine = left_half(at, 0, *inputs)
        both = lax.psum(jnp.where(s == 0, jnp.stack([mine, away]), jnp.stack([away, mine])), "tensor")
        pieces = [lax.dynamic_index_in_dim(both, i, 0, False) for i in (s, 1 - s)]

    left, lh, ll, send, gram = gram_of(at, core_at, pieces)
    got = swap(send, "dp", 0)
    gram = spread_sum(total(gram, got), bits)
    gram_beside = swap(gram, "dp", 0)

    held = (buffer_own, buffer_other)
    got = []
    for h in range(2):
        sent = w_send(at, send_at[h], *held, lh, ll, unit)
        got.append(swap(sent, "dp", 0))
    kept = []
    for h, order in enumerate(orders):
        send, keep = w_keep(at, keep_at[h], *held, lh, ll, got[h], unit)
        recv = swap(send, "dp", order[0])
        for b in order[1:]:
            send, keep = halve(at, bit_at[h][b], keep, recv)
            recv = swap(send, "dp", b)
        kept += [keep, recv]

    x_inv, oh, ol = chol_inverse(at, core_at, gram, gram_beside, left)
    *right, squares = right_rows(at, first_at, cols, *kept, x_inv)
    if power_of_two(n_tp):
        for b in bits_of(n_tp):
            squares = total(squares, swap(squares, "tensor", b))
    else:
        squares = lax.psum(squares, "tensor")
    got = swap(squares, "dp", 0)
    squares_part = total(squares, got)
    squares = spread_sum(squares_part, bits)

    blocks = unit // LANES
    groups = ((0, blocks - blocks // 2), (blocks - blocks // 2, blocks // 2))
    near, far = ([], []), ([], [])
    for h, (order, x) in enumerate(zip(orders, right)):
        for b in order[:0:-1]:
            y = swap(x, "dp", b)
            whole = 2 * x.shape[0]
            cut = [count * LANES for _, count in groups] if whole == unit else [whole]
            x, *rest = join(at, bit_at[h][b], x, y, cut)
        for g, part in enumerate([x] + rest):
            y = swap(part, "dp", order[0])
            beside = swap(part, "dp", 0)
            near[g].extend([part, beside])
            far[g].extend([y, swap(y, "dp", 0)])

    sizes = (cols, rows * n_dp, cols * n_tp)
    same = (oh, ol, *held, sizes)
    both = near[0] + near[1]
    outs = final(at, near_at, groups, unit, "m", both, squares_part, *same, ())
    outs = final(at, near_at, groups, unit, "u", both, squares, *same, outs)
    for g in range(2):
        outs = final(at, far_at, groups[g : g + 1], unit, "mu", far[g], squares, *same, outs)
    return tuple(outs)


def solution(mesh):
    return jax.shard_map(
        on_device,
        mesh=mesh,
        in_specs=(P("dp", "tensor"), P("dp", "tensor"), P("tensor", None)),
        out_specs=(P("dp", "tensor"), P("dp", "tensor"), P("tensor", None)),
        check_vma=False,
    )
```

```python
import functools

import jax
import jax.numpy as jnp
from jax import lax
from jax.experimental import pallas as pl
from jax.experimental.pallas import tpu as pltpu
from jax.sharding import PartitionSpec as P


F32 = jnp.float32
BF16 = jnp.bfloat16
HIGH = lax.Precision.HIGHEST
LANES = 128

NN = (((1,), (0,)), ((), ()))
NT = (((1,), (1,)), ((), ()))
TN = (((0,), (0,)), ((), ()))


HBM = pl.BlockSpec(memory_space=pltpu.HBM)
VMEM = pl.BlockSpec(memory_space=pltpu.VMEM)
SMEM = pl.BlockSpec(memory_space=pltpu.SMEM)


def params(mib):
    return pltpu.CompilerParams(vmem_limit_bytes=mib * 1024 * 1024)


def cost(flops, moved):
    return pl.CostEstimate(flops=int(flops), bytes_accessed=int(moved), transcendentals=0)


def split(x):
    hi = x.astype(BF16)
    lo = (x - hi.astype(F32)).astype(BF16)
    return hi, lo


def dot(a, b, dims):
    return lax.dot_general(a, b, dims, preferred_element_type=F32)


def dot3(ah, al, bh, bl, dims):
    return dot(ah, bh, dims) + (dot(ah, bl, dims) + dot(al, bh, dims))


def dot_high(a, b, dims):
    return lax.dot_general(a, b, dims, precision=HIGH, preferred_element_type=F32)


def column_block(cols):
    blocks = cols // LANES
    return LANES * max(k for k in range(1, 9) if blocks % k == 0)


def left_kernel(which, at, g, m, r, buffer, out, gs, ms, rs, sems):
    depth, half, wide = gs.shape
    steps = g.shape[1] // wide
    rows = pl.ds(pl.multiple_of(at[which] * half, GROUP), half)

    def copies(j, slot):
        part = pl.ds(pl.multiple_of(j * wide, LANES), wide)
        return (
            pltpu.make_async_copy(g.at[rows, part], gs.at[slot], sems.at[0, slot]),
            pltpu.make_async_copy(m.at[rows, part], ms.at[slot], sems.at[1, slot]),
            pltpu.make_async_copy(r.at[part, :], rs.at[slot], sems.at[2, slot]),
        )

    for j in range(min(depth, steps)):
        for copy in copies(j, j):
            copy.start()
    out[...] = jnp.zeros_like(out)

    def body(j, _):
        slot = lax.rem(j, depth)
        for copy in copies(j, slot):
            copy.wait()
        b = gs[slot] + ms[slot]
        buffer[:, pl.ds(pl.multiple_of(j * wide, LANES), wide)] = b
        bh, bl = split(b)
        rh, rl = split(rs[slot])
        out[...] += dot3(bh, bl, rh, rl, NN)

        @pl.when(j + depth < steps)
        def _():
            for copy in copies(j + depth, slot):
                copy.start()

        return 0

    lax.fori_loop(0, steps, body, 0)


def left_half(at, which, gradient, momentum, right_factor, padded):
    rows, cols = gradient.shape
    rank = right_factor.shape[1]
    half, wide, depth = rows // 2, column_block(cols), 4
    return pl.pallas_call(
        functools.partial(left_kernel, which),
        in_specs=[SMEM, HBM, HBM, HBM],
        out_specs=[VMEM, VMEM],
        out_shape=[pltpu.VMEM((half, padded), F32), jax.ShapeDtypeStruct((half, rank), F32)],
        scratch_shapes=[
            pltpu.VMEM((depth, half, wide), F32),
            pltpu.VMEM((depth, half, wide), F32),
            pltpu.VMEM((depth, wide, rank), F32),
            pltpu.SemaphoreType.DMA((3, depth)),
        ],
        compiler_params=params(40),
        cost_estimate=cost(6 * half * cols * rank, 4 * (2 * half * cols + cols * rank)),
        name="left_half",
    )(at, gradient, momentum, right_factor)


def total_kernel(count, *refs):
    ins, outs = refs[:count], refs[count:]
    n = outs[0].shape[0]
    for i, out in enumerate(outs):
        terms = [x[i * n : (i + 1) * n, :] for x in ins]
        while len(terms) > 1:
            terms = [terms[k] + terms[k + 1] for k in range(0, len(terms), 2)]
        out[...] = terms[0]


def total(*blocks, parts=1):
    rows, rank = blocks[0].shape
    outs = pl.pallas_call(
        functools.partial(total_kernel, len(blocks)),
        in_specs=[VMEM] * len(blocks),
        out_specs=[VMEM] * parts,
        out_shape=[jax.ShapeDtypeStruct((rows // parts, rank), F32)] * parts,
        compiler_params=params(6),
        cost_estimate=cost(rows * rank, 4 * (len(blocks) + 1) * rows * rank),
        name="total",
    )(*blocks)
    return outs[0] if parts == 1 else outs


def gram_kernel(place, at, *refs):
    pieces, (left, lh, ll, send, keep, gram) = refs[:-6], refs[-6:]
    n = pieces[0].shape[0]
    for i, piece in enumerate(pieces):
        x = piece[...]
        rows = pl.ds(i * n, n)
        left[rows, :] = x
        lh[rows, :], ll[rows, :] = split(x)
    half = left.shape[0] // 2
    own, other = left[:half, :], left[half:, :]
    gram[...] = dot_high(own, own, TN) + dot_high(other, other, TN)
    n, core = send.shape[0], at[place]
    send[...] = gram[pl.ds(pl.multiple_of((1 - core) * n, GROUP), n), :]
    keep[...] = gram[pl.ds(pl.multiple_of(core * n, GROUP), n), :]


def gram_of(at, place, pieces):
    rank = pieces[0].shape[1]
    rows = sum(p.shape[0] for p in pieces)
    return pl.pallas_call(
        functools.partial(gram_kernel, place),
        in_specs=[SMEM] + [VMEM] * len(pieces),
        out_specs=[VMEM] * 5,
        out_shape=[
            jax.ShapeDtypeStruct((rows, rank), F32),
            jax.ShapeDtypeStruct((rows, rank), BF16),
            jax.ShapeDtypeStruct((rows, rank), BF16),
            jax.ShapeDtypeStruct((rank // 2, rank), F32),
            jax.ShapeDtypeStruct((rank // 2, rank), F32),
        ],
        scratch_shapes=[pltpu.VMEM((rank, rank), F32)],
        compiler_params=params(8),
        cost_estimate=cost(12 * rows * rank * rank, 12 * rows * rank),
        name="gram_of",
    )(at, *pieces)


def w_term(unit, width, own, other, lh, ll):
    part = pl.ds(pl.multiple_of(unit * width, LANES), width)
    bh, bl = split(jnp.concatenate([own[:, part], other[:, part]], axis=0))
    return dot3(bh, bl, lh[...], ll[...], TN)


def w_send_kernel(place, at, own, other, lh, ll, out):
    out[...] = w_term(at[place + pl.program_id(0)], out.shape[0], own, other, lh, ll)


def w_keep_kernel(place, at, own, other, lh, ll, got, send, keep):
    i, width = pl.program_id(0), send.shape[0]
    total = w_term(at[place + i], width, own, other, lh, ll) + got[...]

    @pl.when(i == 0)
    def _():
        send[...] = total

    @pl.when(i == 1)
    def _():
        keep[...] = total


def w_cost(rows, rank, unit):
    return cost(2 * 6 * rows * unit * rank, 2 * 4 * unit * rank)


def w_send(at, place, own, other, lh, ll, unit):
    rows, rank = lh.shape
    return pl.pallas_call(
        functools.partial(w_send_kernel, place),
        grid_spec=pltpu.PrefetchScalarGridSpec(
            num_scalar_prefetch=1,
            grid=(2,),
            in_specs=[VMEM] * 4,
            out_specs=pl.BlockSpec((unit, rank), lambda i, at: (i, 0)),
        ),
        out_shape=jax.ShapeDtypeStruct((2 * unit, rank), F32),
        compiler_params=params(12),
        cost_estimate=w_cost(rows, rank, unit),
        name="w_send",
    )(at, own, other, lh, ll)


def w_keep(at, place, own, other, lh, ll, got, unit):
    rows, rank = lh.shape
    one = pl.BlockSpec((unit, rank), lambda i, at: (0, 0))
    return pl.pallas_call(
        functools.partial(w_keep_kernel, place),
        grid_spec=pltpu.PrefetchScalarGridSpec(
            num_scalar_prefetch=1,
            grid=(2,),
            in_specs=[VMEM] * 4 + [pl.BlockSpec((unit, rank), lambda i, at: (at[place + 2 + i], 0))],
            out_specs=[one, one],
        ),
        out_shape=[jax.ShapeDtypeStruct((unit, rank), F32)] * 2,
        compiler_params=params(14),
        cost_estimate=w_cost(rows, rank, unit),
        name="w_keep",
    )(at, own, other, lh, ll, got)


GROUP = 8


def factor_group(rows, at):
    full = (GROUP, LANES)
    columns = [jnp.broadcast_to(rows[:, at + j : at + j + 1], full) for j in range(GROUP)]
    a = {
        (i, j): jnp.broadcast_to(columns[j][i : i + 1, :], full)
        for j in range(GROUP)
        for i in range(j, GROUP)
    }
    low, c = {}, {}
    for k in range(GROUP):
        c[k, k] = lax.rsqrt(a[k, k])
        for i in range(k + 1, GROUP):
            low[i, k] = a[i, k] * c[k, k]
        for j in range(k + 1, GROUP):
            for i in range(j, GROUP):
                a[i, j] = a[i, j] - low[i, k] * low[j, k]
        for j in range(k):
            total = low[k, j] * c[j, j]
            for i in range(j + 1, k):
                total = total + low[k, i] * c[i, j]
            c[k, j] = -c[k, k] * total
    return c


def spread(x, width):
    return jnp.concatenate([x] * (width // LANES), axis=1)


def eliminate(block):
    size, width = block.shape
    sub = lax.broadcasted_iota(jnp.int32, (GROUP, LANES), 0)
    groups = [block[i : i + GROUP, :] for i in range(0, size, GROUP)]
    for p in range(len(groups)):
        at = p * GROUP
        rows = groups[p]
        c = factor_group(rows, at)
        done = None
        for j in range(GROUP):
            col = jnp.zeros((GROUP, LANES), F32)
            for i in range(j, GROUP):
                col = jnp.where(sub == i, c[i, j], col)
            term = spread(col, width) * jnp.broadcast_to(rows[j : j + 1, :], (GROUP, width))
            done = term if done is None else done + term
        groups[p] = done
        if p + 1 == len(groups):
            break
        solved = None
        for k in range(GROUP):
            col = jnp.zeros((GROUP, LANES), F32)
            for j in range(k + 1):
                col = jnp.where(sub == j, c[k, j], col)
            term = spread(col, width) * jnp.broadcast_to(done[k : k + 1, :], (GROUP, width))
            solved = term if solved is None else solved + term
        for q in range(p + 1, len(groups)):
            x = groups[q]
            total = None
            for j in range(GROUP):
                term = jnp.broadcast_to(x[:, at + j : at + j + 1], (GROUP, width)) * jnp.broadcast_to(
                    solved[j : j + 1, :], (GROUP, width)
                )
                total = term if total is None else total + term
            groups[q] = x - total
    return jnp.concatenate(groups, axis=0)


def chol_kernel(place, at, mine, beside, left, x_out, oh, ol, work):
    n, rank = mine.shape
    size = min(64, rank)
    core = at[place]
    work[pl.ds(pl.multiple_of(core * n, GROUP), n), :rank] = mine[...]
    work[pl.ds(pl.multiple_of((1 - core) * n, GROUP), n), :rank] = beside[...]
    r = lax.broadcasted_iota(jnp.int32, (rank, rank), 0)
    c = lax.broadcasted_iota(jnp.int32, (rank, rank), 1)
    work[:, rank:] = jnp.where(r == c, 1.0, 0.0).astype(F32)

    def step(b, _):
        top = pl.multiple_of(b * size, size)
        rows = pl.ds(top, size)
        width = 2 * rank
        block = pltpu.roll(work[rows, :], lax.rem(width - top, width), 1)
        block = pltpu.roll(eliminate(block), top, 1)
        x_out[rows, :] = block[:, rank:]

        @pl.when(b + 1 < rank // size)
        def _():
            work[...] -= dot_high(block[:, :rank], block, TN)

        return 0

    lax.fori_loop(0, rank // size, step, 0)
    h, l = split(dot_high(left[...], x_out[...], NT))
    oh[...] = h
    ol[...] = l


def chol_inverse(at, place, mine, beside, left):
    rows, rank = left.shape
    return pl.pallas_call(
        functools.partial(chol_kernel, place),
        in_specs=[SMEM] + [VMEM] * 3,
        out_specs=[VMEM] * 3,
        out_shape=[
            jax.ShapeDtypeStruct((rank, rank), F32),
            jax.ShapeDtypeStruct((rows, rank), BF16),
            jax.ShapeDtypeStruct((rows, rank), BF16),
        ],
        scratch_shapes=[pltpu.VMEM((rank, 2 * rank), F32)],
        compiler_params=params(8),
        cost_estimate=cost(4e9, 4 * rows * rank),
        name="chol_inverse",
    )(at, mine, beside, left)


def right_kernel(place, cols, at, ka, ga, kb, gb, x, ra, rb, squares):
    rows, rank = ka.shape
    total = jnp.zeros((1, rank), F32)
    for i, (k, g, out) in enumerate(((ka, ga, ra), (kb, gb, rb))):
        value = dot_high(k[...] + g[...], x[...], NT)
        out[...] = value
        row = lax.broadcasted_iota(jnp.int32, (rows, rank), 0) + at[place + i]
        value = jnp.where(row < cols, value, 0.0)
        total = total + jnp.sum(value * value, axis=0, keepdims=True)
    squares[...] = jnp.broadcast_to(total, squares.shape)


def right_rows(at, place, cols, ka, ga, kb, gb, x):
    rows, rank = ka.shape
    vm = pl.BlockSpec(memory_space=pltpu.VMEM)
    return pl.pallas_call(
        functools.partial(right_kernel, place, cols),
        in_specs=[pl.BlockSpec(memory_space=pltpu.SMEM)] + [vm] * 5,
        out_specs=[vm] * 3,
        out_shape=[jax.ShapeDtypeStruct((rows, rank), F32)] * 2
        + [jax.ShapeDtypeStruct((GROUP, rank), F32)],
        compiler_params=params(8),
        cost_estimate=cost(24 * rows * rank * rank, 24 * rows * rank),
        name="right_rows",
    )(at, ka, ga, kb, gb, x)


def join_kernel(place, at, x, y, both, *parts):
    n, t = x.shape[0], at[place]
    both[pl.ds(pl.multiple_of(t * n, GROUP), n), :] = x[...]
    both[pl.ds(pl.multiple_of((1 - t) * n, GROUP), n), :] = y[...]
    top = 0
    for out in parts:
        out[...] = both[top : top + out.shape[0], :]
        top += out.shape[0]


def join(at, place, x, y, sizes):
    rows, rank = x.shape
    return pl.pallas_call(
        functools.partial(join_kernel, place),
        in_specs=[SMEM, VMEM, VMEM],
        out_specs=[VMEM] * (1 + len(sizes)),
        out_shape=[jax.ShapeDtypeStruct((n, rank), F32) for n in [2 * rows, *sizes]],
        compiler_params=params(6),
        cost_estimate=cost(rows * rank, 16 * rows * rank),
        name="join",
    )(at, x, y)


def halve_kernel(place, at, x, y, send, keep):
    n, t = send.shape[0], at[place]
    for part, out in ((1 - t, send), (t, keep)):
        rows = pl.ds(pl.multiple_of(part * n, GROUP), n)
        out[...] = x[rows, :] + y[rows, :]


def halve(at, place, x, y):
    rows, rank = x.shape
    return pl.pallas_call(
        functools.partial(halve_kernel, place),
        in_specs=[SMEM, VMEM, VMEM],
        out_specs=[VMEM, VMEM],
        out_shape=[jax.ShapeDtypeStruct((rows // 2, rank), F32)] * 2,
        compiler_params=params(6),
        cost_estimate=cost(rows * rank, 12 * rows * rank),
        name="halve",
    )(at, x, y)


SLOTS = 2


def final_kernel(place, group, unit, total_cols, factor, at, *refs):
    pieces = refs[:4]
    squares, oh, ol, own, other = refs[4:9]
    update, momentum, new_right, stage_m, stage_u, stage_r, lh, ll, high, low, sems = refs[-11:]
    start, count = group
    n, rows, half = count * LANES, oh.shape[0], own.shape[0]
    blocks = update.shape[1] // LANES
    halves = [pl.ds(pl.multiple_of(at[h] * half, GROUP), half) for h in range(2)]
    scale = jnp.sqrt(squares[0:1, :] / total_cols + 1e-06)
    lh[:rows, :] = oh[...]
    ll[:rows, :] = ol[...]
    lh[rows:, :], ll[rows:, :] = split((oh[...].astype(F32) + ol[...].astype(F32)) * (factor / scale))

    def each_copy(k, act):
        slot = lax.rem(k, SLOTS)
        first = at[place + k] * (unit // LANES) + start
        for j in range(count):

            @pl.when(first + j < blocks)
            def _(j=j):
                here = pl.ds(j * LANES, LANES)
                there = pl.ds(pl.multiple_of((first + j) * LANES, LANES), LANES)
                for i, (a, b) in enumerate(
                    (
                        (stage_m.at[slot, :, here], momentum.at[:, there]),
                        (stage_u.at[slot, :, here], update.at[:, there]),
                        (stage_r.at[slot, here, :], new_right.at[there, :]),
                    )
                ):
                    act(pltpu.make_async_copy(a, b, sems.at[i, slot, j]))

    def body(k, _):
        slot = lax.rem(k, SLOTS)

        @pl.when(k >= SLOTS)
        def _():
            each_copy(k - SLOTS, lambda copy: copy.wait())

        for i, piece in enumerate(pieces):

            @pl.when(k == i)
            def _(piece=piece):
                right = piece[...]
                high[...], low[...] = split(right)
                stage_r[slot] = right / scale

        part = pl.ds(pl.multiple_of(at[place + k] * unit + start * LANES, LANES), n)
        value = dot(lh[...], high[...], NT) + dot(ll[...], high[...], NT)
        rest = dot(lh[rows:, :], low[...], NT)
        for h, buffer in enumerate((own, other)):
            top = h * half
            stage_m[slot, halves[h], :] = buffer[:, part] - 0.05 * value[top : top + half]
            stage_u[slot, halves[h], :] = value[rows + top : rows + top + half] + rest[top : top + half]
        each_copy(k, lambda copy: copy.start())
        return 0

    lax.fori_loop(0, 4, body, 0)
    for k in range(4 - SLOTS, 4):
        each_copy(k, lambda copy: copy.wait())


def final(at, place, group, unit, pieces, squares, oh, ol, own, other, sizes, before):
    rows, rank = oh.shape
    cols, total_rows, total_cols = sizes
    factor = (total_rows / rank) ** 0.5
    n = group[1] * LANES
    return pl.pallas_call(
        functools.partial(final_kernel, place, group, unit, total_cols, factor),
        in_specs=[SMEM] + [VMEM] * 9 + [HBM] * len(before),
        out_specs=[HBM] * 3,
        out_shape=[
            jax.ShapeDtypeStruct((rows, cols), F32),
            jax.ShapeDtypeStruct((rows, cols), F32),
            jax.ShapeDtypeStruct((cols, rank), F32),
        ],
        scratch_shapes=[
            pltpu.VMEM((SLOTS, rows, n), F32),
            pltpu.VMEM((SLOTS, rows, n), F32),
            pltpu.VMEM((SLOTS, n, rank), F32),
            pltpu.VMEM((2 * rows, rank), BF16),
            pltpu.VMEM((2 * rows, rank), BF16),
            pltpu.VMEM((n, rank), BF16),
            pltpu.VMEM((n, rank), BF16),
            pltpu.SemaphoreType.DMA((3, SLOTS, group[1])),
        ],
        input_output_aliases={10 + i: i for i in range(len(before))},
        compiler_params=params(28),
        cost_estimate=cost(48 * rows * n * rank, 32 * rows * n),
        name="final",
    )(at, *pieces, squares, oh, ol, own, other, *before)


def power_of_two(n):
    return n & (n - 1) == 0


def bits_of(n):
    return list(range(n.bit_length() - 1))


def swap(x, axis, *places):
    n = lax.axis_size(axis)
    mask = sum(1 << bit for bit in places)
    return lax.ppermute(x, axis, [(i, i ^ mask) for i in range(n)])


def spread_sum(x, bits):
    for b in bits[3:]:
        x = total(x, swap(x, "dp", b))
    b, c = bits[1:3]
    others = [swap(x, "dp", *m) for m in ((b,), (c,), (b, c))]
    return total(x, *others)


def on_device(gradient, momentum, right_factor):
    rows, cols = gradient.shape
    n_dp, n_tp = lax.axis_size("dp"), lax.axis_size("tensor")
    d, z = lax.axis_index("dp"), lax.axis_index("tensor")
    bits = bits_of(n_dp)

    unit = LANES * (-(-cols // (8 * LANES)))
    orders = [bits[1:], bits[1:][::-1]]
    table = []

    def put(*values):
        table.extend(values)
        return len(table) - len(values)

    bit_of = lambda b: (d >> b) & 1
    s, core = z & 1, d & 1
    put(s, 1 - s)
    core_at = put(core)
    send_at, keep_at, bit_at, near, far, first = [], [], [], [], [], []
    for h, order in enumerate(orders):
        t = bit_of(order[0])
        base, beside = 4 * h + 2 * core, 4 * h + 2 * (1 - core)
        send_at.append(put(beside, beside + 1))
        keep_at.append(put(base + 1 - t, base + t, 1 - t, t))
        bit_at.append({b: put(bit_of(b)) for b in order[1:]})
        near += [base + t, beside + t]
        far += [base + 1 - t, beside + 1 - t]
        at, n = (base + t) * unit, unit
        for b in order[1:]:
            n = n // 2
            at = at + bit_of(b) * n
        first.append(at)
    near_at, far_at, first_at = put(*near), put(*far), put(*first)
    at = jnp.stack([jnp.asarray(v, jnp.int32) for v in table])

    inputs = (gradient, momentum, right_factor, 8 * unit)
    buffer_other, away = left_half(at, 1, *inputs)
    if power_of_two(n_tp) and n_tp > 1:
        got = swap(away, "tensor", 0)
        buffer_own, mine = left_half(at, 0, *inputs)
        own = list(total(mine, got, parts=2))
        for bit in bits_of(n_tp)[1:]:
            for i in range(2):
                got = swap(own[i], "tensor", bit)
                own[i] = total(own[i], got)
        pieces = own[:]
        for i in range(2):
            pieces.append(swap(own[i], "tensor", 0))
    else:
        buffer_own, mine = left_half(at, 0, *inputs)
        both = lax.psum(jnp.where(s == 0, jnp.stack([mine, away]), jnp.stack([away, mine])), "tensor")
        pieces = [lax.dynamic_index_in_dim(both, i, 0, False) for i in (s, 1 - s)]

    left, lh, ll, send, gram = gram_of(at, core_at, pieces)
    got = swap(send, "dp", 0)
    gram = spread_sum(total(gram, got), bits)
    gram_beside = swap(gram, "dp", 0)

    held = (buffer_own, buffer_other)
    got = []
    for h in range(2):
        sent = w_send(at, send_at[h], *held, lh, ll, unit)
        got.append(swap(sent, "dp", 0))
    kept = []
    for h, order in enumerate(orders):
        send, keep = w_keep(at, keep_at[h], *held, lh, ll, got[h], unit)
        recv = swap(send, "dp", order[0])
        for b in order[1:]:
            send, keep = halve(at, bit_at[h][b], keep, recv)
            recv = swap(send, "dp", b)
        kept += [keep, recv]

    x_inv, oh, ol = chol_inverse(at, core_at, gram, gram_beside, left)
    *right, squares = right_rows(at, first_at, cols, *kept, x_inv)
    if power_of_two(n_tp):
        for b in bits_of(n_tp):
            squares = total(squares, swap(squares, "tensor", b))
    else:
        squares = lax.psum(squares, "tensor")
    got = swap(squares, "dp", 0)
    squares = total(squares, got)
    squares = spread_sum(squares, bits)

    blocks = unit // LANES
    groups = ((0, blocks - blocks // 2), (blocks - blocks // 2, blocks // 2))
    near, far = [], ([], [])
    for h, (order, x) in enumerate(zip(orders, right)):
        parts = [x]
        for b in order[:0:-1]:
            y = swap(x, "dp", b)
            last = 2 * x.shape[0] == unit
            x, *parts = join(
                at, bit_at[h][b], x, y, [count * LANES for _, count in groups] if last else []
            )
        for g, part in enumerate(parts):
            y = swap(part, "dp", order[0])
            far[g].extend([y, swap(y, "dp", 0)])
        near.extend([x, swap(x, "dp", 0)])

    same = (squares, oh, ol, *held, (cols, rows * n_dp, cols * n_tp))
    outs = final(at, near_at, (0, blocks), unit, near, *same, ())
    for g in range(2):
        outs = final(at, far_at, groups[g], unit, far[g], *same, outs)
    return tuple(outs)


def solution(mesh):
    return jax.shard_map(
        on_device,
        mesh=mesh,
        in_specs=(P("dp", "tensor"), P("dp", "tensor"), P("tensor", None)),
        out_specs=(P("dp", "tensor"), P("dp", "tensor"), P("tensor", None)),
        check_vma=False,
    )
```

```python
import functools

import jax
import jax.numpy as jnp
from jax import lax
from jax.experimental import pallas as pl
from jax.experimental.pallas import tpu as pltpu
from jax.sharding import PartitionSpec as P


F32 = jnp.float32
BF16 = jnp.bfloat16
HIGH = lax.Precision.HIGHEST
LANES = 128

NN = (((1,), (0,)), ((), ()))
NT = (((1,), (1,)), ((), ()))
TN = (((0,), (0,)), ((), ()))


HBM = pl.BlockSpec(memory_space=pltpu.HBM)
VMEM = pl.BlockSpec(memory_space=pltpu.VMEM)
SMEM = pl.BlockSpec(memory_space=pltpu.SMEM)


def params(mib):
    return pltpu.CompilerParams(vmem_limit_bytes=mib * 1024 * 1024)


def cost(flops, moved):
    return pl.CostEstimate(flops=int(flops), bytes_accessed=int(moved), transcendentals=0)


def split(x):
    hi = x.astype(BF16)
    lo = (x - hi.astype(F32)).astype(BF16)
    return hi, lo


def dot(a, b, dims):
    return lax.dot_general(a, b, dims, preferred_element_type=F32)


def dot3(ah, al, bh, bl, dims):
    return dot(ah, bh, dims) + (dot(ah, bl, dims) + dot(al, bh, dims))


def dot_high(a, b, dims):
    return lax.dot_general(a, b, dims, precision=HIGH, preferred_element_type=F32)


def column_block(cols):
    blocks = cols // LANES
    return LANES * max(k for k in range(1, 9) if blocks % k == 0)


def left_kernel(which, at, g, m, r, buffer, out, gs, ms, rs, sems):
    depth, half, wide = gs.shape
    steps = g.shape[1] // wide
    rows = pl.ds(pl.multiple_of(at[which] * half, GROUP), half)

    def copies(j, slot):
        part = pl.ds(pl.multiple_of(j * wide, LANES), wide)
        return (
            pltpu.make_async_copy(g.at[rows, part], gs.at[slot], sems.at[0, slot]),
            pltpu.make_async_copy(m.at[rows, part], ms.at[slot], sems.at[1, slot]),
            pltpu.make_async_copy(r.at[part, :], rs.at[slot], sems.at[2, slot]),
        )

    for j in range(min(depth, steps)):
        for copy in copies(j, j):
            copy.start()
    out[...] = jnp.zeros_like(out)

    def body(j, _):
        slot = lax.rem(j, depth)
        for copy in copies(j, slot):
            copy.wait()
        b = gs[slot] + ms[slot]
        buffer[:, pl.ds(pl.multiple_of(j * wide, LANES), wide)] = b
        bh, bl = split(b)
        rh, rl = split(rs[slot])
        out[...] += dot3(bh, bl, rh, rl, NN)

        @pl.when(j + depth < steps)
        def _():
            for copy in copies(j + depth, slot):
                copy.start()

        return 0

    lax.fori_loop(0, steps, body, 0)


def left_half(at, which, gradient, momentum, right_factor, padded):
    rows, cols = gradient.shape
    rank = right_factor.shape[1]
    half, wide, depth = rows // 2, column_block(cols), 4
    return pl.pallas_call(
        functools.partial(left_kernel, which),
        in_specs=[SMEM, HBM, HBM, HBM],
        out_specs=[VMEM, VMEM],
        out_shape=[pltpu.VMEM((half, padded), F32), jax.ShapeDtypeStruct((half, rank), F32)],
        scratch_shapes=[
            pltpu.VMEM((depth, half, wide), F32),
            pltpu.VMEM((depth, half, wide), F32),
            pltpu.VMEM((depth, wide, rank), F32),
            pltpu.SemaphoreType.DMA((3, depth)),
        ],
        compiler_params=params(40),
        cost_estimate=cost(6 * half * cols * rank, 4 * (2 * half * cols + cols * rank)),
        name="left_half",
    )(at, gradient, momentum, right_factor)


def total_kernel(count, *refs):
    ins, outs = refs[:count], refs[count:]
    n = outs[0].shape[0]
    for i, out in enumerate(outs):
        terms = [x[i * n : (i + 1) * n, :] for x in ins]
        while len(terms) > 1:
            terms = [terms[k] + terms[k + 1] for k in range(0, len(terms), 2)]
        out[...] = terms[0]


def total(*blocks, parts=1):
    rows, rank = blocks[0].shape
    outs = pl.pallas_call(
        functools.partial(total_kernel, len(blocks)),
        in_specs=[VMEM] * len(blocks),
        out_specs=[VMEM] * parts,
        out_shape=[jax.ShapeDtypeStruct((rows // parts, rank), F32)] * parts,
        compiler_params=params(6),
        cost_estimate=cost(rows * rank, 4 * (len(blocks) + 1) * rows * rank),
        name="total",
    )(*blocks)
    return outs[0] if parts == 1 else outs


def gram_kernel(place, at, *refs):
    pieces, (left, lh, ll, send, keep, gram) = refs[:-6], refs[-6:]
    n = pieces[0].shape[0]
    for i, piece in enumerate(pieces):
        x = piece[...]
        rows = pl.ds(i * n, n)
        left[rows, :] = x
        lh[rows, :], ll[rows, :] = split(x)
    half = left.shape[0] // 2
    own, other = left[:half, :], left[half:, :]
    gram[...] = dot_high(own, own, TN) + dot_high(other, other, TN)
    n, core = send.shape[0], at[place]
    send[...] = gram[pl.ds(pl.multiple_of((1 - core) * n, GROUP), n), :]
    keep[...] = gram[pl.ds(pl.multiple_of(core * n, GROUP), n), :]


def gram_of(at, place, pieces):
    rank = pieces[0].shape[1]
    rows = sum(p.shape[0] for p in pieces)
    return pl.pallas_call(
        functools.partial(gram_kernel, place),
        in_specs=[SMEM] + [VMEM] * len(pieces),
        out_specs=[VMEM] * 5,
        out_shape=[
            jax.ShapeDtypeStruct((rows, rank), F32),
            jax.ShapeDtypeStruct((rows, rank), BF16),
            jax.ShapeDtypeStruct((rows, rank), BF16),
            jax.ShapeDtypeStruct((rank // 2, rank), F32),
            jax.ShapeDtypeStruct((rank // 2, rank), F32),
        ],
        scratch_shapes=[pltpu.VMEM((rank, rank), F32)],
        compiler_params=params(8),
        cost_estimate=cost(12 * rows * rank * rank, 12 * rows * rank),
        name="gram_of",
    )(at, *pieces)


def w_term(unit, width, own, other, lh, ll):
    part = pl.ds(pl.multiple_of(unit * width, LANES), width)
    bh, bl = split(jnp.concatenate([own[:, part], other[:, part]], axis=0))
    return dot3(bh, bl, lh[...], ll[...], TN)


def w_send_kernel(place, at, own, other, lh, ll, out):
    out[...] = w_term(at[place + pl.program_id(0)], out.shape[0], own, other, lh, ll)


def w_keep_kernel(place, at, own, other, lh, ll, got, send, keep):
    i, width = pl.program_id(0), send.shape[0]
    total = w_term(at[place + i], width, own, other, lh, ll) + got[...]

    @pl.when(i == 0)
    def _():
        send[...] = total

    @pl.when(i == 1)
    def _():
        keep[...] = total


def w_cost(rows, rank, unit):
    return cost(2 * 6 * rows * unit * rank, 2 * 4 * unit * rank)


def w_send(at, place, own, other, lh, ll, unit):
    rows, rank = lh.shape
    return pl.pallas_call(
        functools.partial(w_send_kernel, place),
        grid_spec=pltpu.PrefetchScalarGridSpec(
            num_scalar_prefetch=1,
            grid=(2,),
            in_specs=[VMEM] * 4,
            out_specs=pl.BlockSpec((unit, rank), lambda i, at: (i, 0)),
        ),
        out_shape=jax.ShapeDtypeStruct((2 * unit, rank), F32),
        compiler_params=params(12),
        cost_estimate=w_cost(rows, rank, unit),
        name="w_send",
    )(at, own, other, lh, ll)


def w_keep(at, place, own, other, lh, ll, got, unit):
    rows, rank = lh.shape
    one = pl.BlockSpec((unit, rank), lambda i, at: (0, 0))
    return pl.pallas_call(
        functools.partial(w_keep_kernel, place),
        grid_spec=pltpu.PrefetchScalarGridSpec(
            num_scalar_prefetch=1,
            grid=(2,),
            in_specs=[VMEM] * 4 + [pl.BlockSpec((unit, rank), lambda i, at: (at[place + 2 + i], 0))],
            out_specs=[one, one],
        ),
        out_shape=[jax.ShapeDtypeStruct((unit, rank), F32)] * 2,
        compiler_params=params(14),
        cost_estimate=w_cost(rows, rank, unit),
        name="w_keep",
    )(at, own, other, lh, ll, got)


GROUP = 8


def factor_group(rows, at):
    full = (GROUP, LANES)
    columns = [jnp.broadcast_to(rows[:, at + j : at + j + 1], full) for j in range(GROUP)]
    a = {
        (i, j): jnp.broadcast_to(columns[j][i : i + 1, :], full)
        for j in range(GROUP)
        for i in range(j, GROUP)
    }
    low, c = {}, {}
    for k in range(GROUP):
        c[k, k] = lax.rsqrt(a[k, k])
        for i in range(k + 1, GROUP):
            low[i, k] = a[i, k] * c[k, k]
        for j in range(k + 1, GROUP):
            for i in range(j, GROUP):
                a[i, j] = a[i, j] - low[i, k] * low[j, k]
        for j in range(k):
            total = low[k, j] * c[j, j]
            for i in range(j + 1, k):
                total = total + low[k, i] * c[i, j]
            c[k, j] = -c[k, k] * total
    return c


def spread(x, width):
    return jnp.concatenate([x] * (width // LANES), axis=1)


def eliminate(block):
    size, width = block.shape
    sub = lax.broadcasted_iota(jnp.int32, (GROUP, LANES), 0)
    groups = [block[i : i + GROUP, :] for i in range(0, size, GROUP)]
    for p in range(len(groups)):
        at = p * GROUP
        rows = groups[p]
        c = factor_group(rows, at)
        done = None
        for j in range(GROUP):
            col = jnp.zeros((GROUP, LANES), F32)
            for i in range(j, GROUP):
                col = jnp.where(sub == i, c[i, j], col)
            term = spread(col, width) * jnp.broadcast_to(rows[j : j + 1, :], (GROUP, width))
            done = term if done is None else done + term
        groups[p] = done
        if p + 1 == len(groups):
            break
        solved = None
        for k in range(GROUP):
            col = jnp.zeros((GROUP, LANES), F32)
            for j in range(k + 1):
                col = jnp.where(sub == j, c[k, j], col)
            term = spread(col, width) * jnp.broadcast_to(done[k : k + 1, :], (GROUP, width))
            solved = term if solved is None else solved + term
        for q in range(p + 1, len(groups)):
            x = groups[q]
            total = None
            for j in range(GROUP):
                term = jnp.broadcast_to(x[:, at + j : at + j + 1], (GROUP, width)) * jnp.broadcast_to(
                    solved[j : j + 1, :], (GROUP, width)
                )
                total = term if total is None else total + term
            groups[q] = x - total
    return jnp.concatenate(groups, axis=0)


def chol_kernel(place, at, mine, beside, left, x_out, oh, ol, work):
    n, rank = mine.shape
    size = min(64, rank)
    core = at[place]
    work[pl.ds(pl.multiple_of(core * n, GROUP), n), :rank] = mine[...]
    work[pl.ds(pl.multiple_of((1 - core) * n, GROUP), n), :rank] = beside[...]
    r = lax.broadcasted_iota(jnp.int32, (rank, rank), 0)
    c = lax.broadcasted_iota(jnp.int32, (rank, rank), 1)
    work[:, rank:] = jnp.where(r == c, 1.0, 0.0).astype(F32)

    def step(b, _):
        top = pl.multiple_of(b * size, size)
        rows = pl.ds(top, size)
        width = 2 * rank
        block = pltpu.roll(work[rows, :], lax.rem(width - top, width), 1)
        block = pltpu.roll(eliminate(block), top, 1)
        x_out[rows, :] = block[:, rank:]

        @pl.when(b + 1 < rank // size)
        def _():
            work[...] -= dot_high(block[:, :rank], block, TN)

        return 0

    lax.fori_loop(0, rank // size, step, 0)
    h, l = split(dot_high(left[...], x_out[...], NT))
    oh[...] = h
    ol[...] = l


def chol_inverse(at, place, mine, beside, left):
    rows, rank = left.shape
    return pl.pallas_call(
        functools.partial(chol_kernel, place),
        in_specs=[SMEM] + [VMEM] * 3,
        out_specs=[VMEM] * 3,
        out_shape=[
            jax.ShapeDtypeStruct((rank, rank), F32),
            jax.ShapeDtypeStruct((rows, rank), BF16),
            jax.ShapeDtypeStruct((rows, rank), BF16),
        ],
        scratch_shapes=[pltpu.VMEM((rank, 2 * rank), F32)],
        compiler_params=params(8),
        cost_estimate=cost(4e9, 4 * rows * rank),
        name="chol_inverse",
    )(at, mine, beside, left)


def right_kernel(place, cols, at, ka, ga, kb, gb, x, ra, rb, squares):
    rows, rank = ka.shape
    total = jnp.zeros((1, rank), F32)
    for i, (k, g, out) in enumerate(((ka, ga, ra), (kb, gb, rb))):
        value = dot_high(k[...] + g[...], x[...], NT)
        out[...] = value
        row = lax.broadcasted_iota(jnp.int32, (rows, rank), 0) + at[place + i]
        value = jnp.where(row < cols, value, 0.0)
        total = total + jnp.sum(value * value, axis=0, keepdims=True)
    squares[...] = jnp.broadcast_to(total, squares.shape)


def right_rows(at, place, cols, ka, ga, kb, gb, x):
    rows, rank = ka.shape
    vm = pl.BlockSpec(memory_space=pltpu.VMEM)
    return pl.pallas_call(
        functools.partial(right_kernel, place, cols),
        in_specs=[pl.BlockSpec(memory_space=pltpu.SMEM)] + [vm] * 5,
        out_specs=[vm] * 3,
        out_shape=[jax.ShapeDtypeStruct((rows, rank), F32)] * 2
        + [jax.ShapeDtypeStruct((GROUP, rank), F32)],
        compiler_params=params(8),
        cost_estimate=cost(24 * rows * rank * rank, 24 * rows * rank),
        name="right_rows",
    )(at, ka, ga, kb, gb, x)


def join_kernel(place, at, x, y, both, *parts):
    n, t = x.shape[0], at[place]
    both[pl.ds(pl.multiple_of(t * n, GROUP), n), :] = x[...]
    both[pl.ds(pl.multiple_of((1 - t) * n, GROUP), n), :] = y[...]
    top = 0
    for out in parts:
        out[...] = both[top : top + out.shape[0], :]
        top += out.shape[0]


def join(at, place, x, y, sizes):
    rows, rank = x.shape
    return pl.pallas_call(
        functools.partial(join_kernel, place),
        in_specs=[SMEM, VMEM, VMEM],
        out_specs=[VMEM] * (1 + len(sizes)),
        out_shape=[jax.ShapeDtypeStruct((n, rank), F32) for n in [2 * rows, *sizes]],
        compiler_params=params(6),
        cost_estimate=cost(rows * rank, 16 * rows * rank),
        name="join",
    )(at, x, y)


def halve_kernel(place, at, x, y, send, keep):
    n, t = send.shape[0], at[place]
    for part, out in ((1 - t, send), (t, keep)):
        rows = pl.ds(pl.multiple_of(part * n, GROUP), n)
        out[...] = x[rows, :] + y[rows, :]


def halve(at, place, x, y):
    rows, rank = x.shape
    return pl.pallas_call(
        functools.partial(halve_kernel, place),
        in_specs=[SMEM, VMEM, VMEM],
        out_specs=[VMEM, VMEM],
        out_shape=[jax.ShapeDtypeStruct((rows // 2, rank), F32)] * 2,
        compiler_params=params(6),
        cost_estimate=cost(rows * rank, 12 * rows * rank),
        name="halve",
    )(at, x, y)


SLOTS = 2


def final_kernel(units, place, group, unit, total_cols, factor, at, *refs):
    pieces = refs[:units]
    squares, oh, ol, own, other = refs[units : units + 5]
    update, momentum, new_right, stage_m, stage_u, stage_r, lh, ll, high, low, sems = refs[-11:]
    start, count = group
    n, rows, half = count * LANES, oh.shape[0], own.shape[0]
    blocks = update.shape[1] // LANES
    halves = [pl.ds(pl.multiple_of(at[h] * half, GROUP), half) for h in range(2)]
    scale = jnp.sqrt(squares[0:1, :] / total_cols + 1e-06)
    lh[:rows, :] = oh[...]
    ll[:rows, :] = ol[...]
    lh[rows:, :], ll[rows:, :] = split((oh[...].astype(F32) + ol[...].astype(F32)) * (factor / scale))

    def each_copy(k, act):
        slot = lax.rem(k, SLOTS)
        first = at[place + k] * (unit // LANES) + start
        for j in range(count):

            @pl.when(first + j < blocks)
            def _(j=j):
                here = pl.ds(j * LANES, LANES)
                there = pl.ds(pl.multiple_of((first + j) * LANES, LANES), LANES)
                for i, (a, b) in enumerate(
                    (
                        (stage_m.at[slot, :, here], momentum.at[:, there]),
                        (stage_u.at[slot, :, here], update.at[:, there]),
                        (stage_r.at[slot, here, :], new_right.at[there, :]),
                    )
                ):
                    act(pltpu.make_async_copy(a, b, sems.at[i, slot, j]))

    def body(k, _):
        slot = lax.rem(k, SLOTS)

        @pl.when(k >= SLOTS)
        def _():
            each_copy(k - SLOTS, lambda copy: copy.wait())

        for i, piece in enumerate(pieces):

            @pl.when(k == i)
            def _(piece=piece):
                right = piece[...]
                high[...], low[...] = split(right)
                stage_r[slot] = right / scale

        part = pl.ds(pl.multiple_of(at[place + k] * unit + start * LANES, LANES), n)
        value = dot(lh[...], high[...], NT) + dot(ll[...], high[...], NT)
        rest = dot(lh[rows:, :], low[...], NT)
        for h, buffer in enumerate((own, other)):
            top = h * half
            stage_m[slot, halves[h], :] = buffer[:, part] - 0.05 * value[top : top + half]
            stage_u[slot, halves[h], :] = value[rows + top : rows + top + half] + rest[top : top + half]
        each_copy(k, lambda copy: copy.start())
        return 0

    lax.fori_loop(0, units, body, 0)
    for k in range(units - SLOTS, units):
        each_copy(k, lambda copy: copy.wait())


def final(at, place, group, unit, pieces, squares, oh, ol, own, other, sizes, before):
    rows, rank = oh.shape
    cols, total_rows, total_cols = sizes
    factor = (total_rows / rank) ** 0.5
    n = group[1] * LANES
    return pl.pallas_call(
        functools.partial(final_kernel, len(pieces), place, group, unit, total_cols, factor),
        in_specs=[SMEM] + [VMEM] * (len(pieces) + 5) + [HBM] * len(before),
        out_specs=[HBM] * 3,
        out_shape=[
            jax.ShapeDtypeStruct((rows, cols), F32),
            jax.ShapeDtypeStruct((rows, cols), F32),
            jax.ShapeDtypeStruct((cols, rank), F32),
        ],
        scratch_shapes=[
            pltpu.VMEM((SLOTS, rows, n), F32),
            pltpu.VMEM((SLOTS, rows, n), F32),
            pltpu.VMEM((SLOTS, n, rank), F32),
            pltpu.VMEM((2 * rows, rank), BF16),
            pltpu.VMEM((2 * rows, rank), BF16),
            pltpu.VMEM((n, rank), BF16),
            pltpu.VMEM((n, rank), BF16),
            pltpu.SemaphoreType.DMA((3, SLOTS, group[1])),
        ],
        input_output_aliases={len(pieces) + 6 + i: i for i in range(len(before))},
        compiler_params=params(28),
        cost_estimate=cost(12 * len(pieces) * rows * n * rank, 8 * len(pieces) * rows * n),
        name="final",
    )(at, *pieces, squares, oh, ol, own, other, *before)


def power_of_two(n):
    return n & (n - 1) == 0


def bits_of(n):
    return list(range(n.bit_length() - 1))


def swap(x, axis, *places):
    n = lax.axis_size(axis)
    mask = sum(1 << bit for bit in places)
    return lax.ppermute(x, axis, [(i, i ^ mask) for i in range(n)])


def spread_sum(x, bits):
    for b in bits[3:]:
        x = total(x, swap(x, "dp", b))
    b, c = bits[1:3]
    others = [swap(x, "dp", *m) for m in ((b,), (c,), (b, c))]
    return total(x, *others)


def on_device(gradient, momentum, right_factor):
    rows, cols = gradient.shape
    n_dp, n_tp = lax.axis_size("dp"), lax.axis_size("tensor")
    d, z = lax.axis_index("dp"), lax.axis_index("tensor")
    bits = bits_of(n_dp)

    unit = LANES * (-(-cols // (8 * LANES)))
    orders = [bits[1:], bits[1:][::-1]]
    table = []

    def put(*values):
        table.extend(values)
        return len(table) - len(values)

    bit_of = lambda b: (d >> b) & 1
    s, core = z & 1, d & 1
    put(s, 1 - s)
    core_at = put(core)
    send_at, keep_at, bit_at, first = [], [], [], []
    near, near_beside, far, far_beside = [], [], [], []
    for h, order in enumerate(orders):
        t = bit_of(order[0])
        base, beside = 4 * h + 2 * core, 4 * h + 2 * (1 - core)
        send_at.append(put(beside, beside + 1))
        keep_at.append(put(base + 1 - t, base + t, 1 - t, t))
        bit_at.append({b: put(bit_of(b)) for b in order[1:]})
        near.append(base + t)
        near_beside.append(beside + t)
        far.append(base + 1 - t)
        far_beside.append(beside + 1 - t)
        at, n = (base + t) * unit, unit
        for b in order[1:]:
            n = n // 2
            at = at + bit_of(b) * n
        first.append(at)
    near_at, beside_at = put(*near), put(*near_beside)
    far_at, first_at = put(*far, *far_beside), put(*first)
    at = jnp.stack([jnp.asarray(v, jnp.int32) for v in table])

    inputs = (gradient, momentum, right_factor, 8 * unit)
    buffer_other, away = left_half(at, 1, *inputs)
    if power_of_two(n_tp) and n_tp > 1:
        got = swap(away, "tensor", 0)
        buffer_own, mine = left_half(at, 0, *inputs)
        own = list(total(mine, got, parts=2))
        for bit in bits_of(n_tp)[1:]:
            for i in range(2):
                got = swap(own[i], "tensor", bit)
                own[i] = total(own[i], got)
        pieces = own[:]
        for i in range(2):
            pieces.append(swap(own[i], "tensor", 0))
    else:
        buffer_own, mine = left_half(at, 0, *inputs)
        both = lax.psum(jnp.where(s == 0, jnp.stack([mine, away]), jnp.stack([away, mine])), "tensor")
        pieces = [lax.dynamic_index_in_dim(both, i, 0, False) for i in (s, 1 - s)]

    left, lh, ll, send, gram = gram_of(at, core_at, pieces)
    got = swap(send, "dp", 0)
    gram = spread_sum(total(gram, got), bits)
    gram_beside = swap(gram, "dp", 0)

    held = (buffer_own, buffer_other)
    got = []
    for h in range(2):
        sent = w_send(at, send_at[h], *held, lh, ll, unit)
        got.append(swap(sent, "dp", 0))
    kept = []
    for h, order in enumerate(orders):
        send, keep = w_keep(at, keep_at[h], *held, lh, ll, got[h], unit)
        recv = swap(send, "dp", order[0])
        for b in order[1:]:
            send, keep = halve(at, bit_at[h][b], keep, recv)
            recv = swap(send, "dp", b)
        kept += [keep, recv]

    x_inv, oh, ol = chol_inverse(at, core_at, gram, gram_beside, left)
    *right, squares = right_rows(at, first_at, cols, *kept, x_inv)
    if n_tp == 4:
        squares = total(squares, *(swap(squares, "tensor", *m) for m in ((0,), (1,), (0, 1))))
    else:
        squares = lax.psum(squares, "tensor")
    got = swap(squares, "dp", 0)
    squares = total(squares, got)
    squares = spread_sum(squares, bits)

    blocks = unit // LANES
    groups = ((0, blocks - blocks // 2), (blocks - blocks // 2, blocks // 2))
    near, near_beside, far, far_beside = [], [], ([], []), ([], [])
    for h, (order, x) in enumerate(zip(orders, right)):
        parts = [x]
        for b in order[:0:-1]:
            y = swap(x, "dp", b)
            last = 2 * x.shape[0] == unit
            x, *parts = join(
                at, bit_at[h][b], x, y, [count * LANES for _, count in groups] if last else []
            )
        for g, part in enumerate(parts):
            y = swap(part, "dp", order[0])
            far_beside[g].append(swap(y, "dp", 0))
            far[g].append(y)
        near.append(x)
        near_beside.append(swap(x, "dp", 0))

    same = (squares, oh, ol, *held, (cols, rows * n_dp, cols * n_tp))
    outs = final(at, near_at, (0, blocks), unit, near, *same, ())
    outs = final(at, beside_at, (0, blocks), unit, near_beside, *same, outs)
    for g in range(2):
        outs = final(at, far_at, groups[g], unit, far[g] + far_beside[g], *same, outs)
    return tuple(outs)


def solution(mesh):
    return jax.shard_map(
        on_device,
        mesh=mesh,
        in_specs=(P("dp", "tensor"), P("dp", "tensor"), P("tensor", None)),
        out_specs=(P("dp", "tensor"), P("dp", "tensor"), P("tensor", None)),
        check_vma=False,
    )
```

```python
import functools

import jax
import jax.numpy as jnp
from jax import lax
from jax.experimental import pallas as pl
from jax.experimental.pallas import tpu as pltpu
from jax.sharding import PartitionSpec as P


F32 = jnp.float32
BF16 = jnp.bfloat16
HIGH = lax.Precision.HIGHEST
LANES = 128

NN = (((1,), (0,)), ((), ()))
NT = (((1,), (1,)), ((), ()))
TN = (((0,), (0,)), ((), ()))


HBM = pl.BlockSpec(memory_space=pltpu.HBM)
VMEM = pl.BlockSpec(memory_space=pltpu.VMEM)
SMEM = pl.BlockSpec(memory_space=pltpu.SMEM)


def params(mib):
    return pltpu.CompilerParams(vmem_limit_bytes=mib * 1024 * 1024)


def cost(flops, moved):
    return pl.CostEstimate(flops=int(flops), bytes_accessed=int(moved), transcendentals=0)


def split(x):
    hi = x.astype(BF16)
    lo = (x - hi.astype(F32)).astype(BF16)
    return hi, lo


def dot(a, b, dims):
    return lax.dot_general(a, b, dims, preferred_element_type=F32)


def dot3(ah, al, bh, bl, dims):
    return dot(ah, bh, dims) + (dot(ah, bl, dims) + dot(al, bh, dims))


def dot_high(a, b, dims):
    return lax.dot_general(a, b, dims, precision=HIGH, preferred_element_type=F32)


def column_block(cols):
    blocks = cols // LANES
    return LANES * max(k for k in range(1, 9) if blocks % k == 0)


DEPTH = 4


def left_kernel(first, which, part, at, g, m, *refs):
    if first:
        r, buffer, rh, rl, *outs, gs, ms, rs, sems = refs
    else:
        rh, rl, buffer, *outs, gs, ms, sems = refs
    depth, n, wide = gs.shape
    steps = g.shape[1] // wide
    top = at[which] * (g.shape[0] // 2) + part * n
    rows = pl.ds(pl.multiple_of(top, GROUP), n)

    def copies(j, slot):
        part = pl.ds(pl.multiple_of(j * wide, LANES), wide)
        some = [
            pltpu.make_async_copy(g.at[rows, part], gs.at[slot], sems.at[0, slot]),
            pltpu.make_async_copy(m.at[rows, part], ms.at[slot], sems.at[1, slot]),
        ]
        if first:
            some.append(pltpu.make_async_copy(r.at[part, :], rs.at[slot], sems.at[2, slot]))
        return some

    for j in range(min(depth, steps)):
        for copy in copies(j, j):
            copy.start()
    for out in outs:
        out[...] = jnp.zeros_like(out)

    def body(j, _):
        slot = lax.rem(j, depth)
        part = pl.ds(pl.multiple_of(j * wide, LANES), wide)
        for copy in copies(j, slot):
            copy.wait()
        b = gs[slot] + ms[slot]
        buffer[:, part] = b
        bh, bl = split(b)
        if first:
            rh[part, :], rl[part, :] = split(rs[slot])
        term = dot3(bh, bl, rh[part, :], rl[part, :], NN)
        size = n // len(outs)
        for i, out in enumerate(outs):
            out[...] += term[i * size : (i + 1) * size]

        @pl.when(j + depth < steps)
        def _():
            for copy in copies(j + depth, slot):
                copy.start()

        return 0

    lax.fori_loop(0, steps, body, 0)


def left_rows(at, which, part, parts, gradient, momentum, right, padded):
    first = not isinstance(right, tuple)
    right = (right,) if first else right
    rows, cols = gradient.shape
    rank = right[0].shape[1]
    wide = column_block(cols)
    n = rows // 2 if first else rows // (2 * parts)
    outs = parts if first else 1
    terms = [pltpu.VMEM((cols, rank), BF16)] * 2 if first else []
    return pl.pallas_call(
        functools.partial(left_kernel, first, which, part),
        in_specs=[SMEM, HBM, HBM] + ([HBM] if first else [VMEM, VMEM]),
        out_specs=[VMEM] * (1 + len(terms) + outs),
        out_shape=[pltpu.VMEM((n, padded), F32)]
        + terms
        + [jax.ShapeDtypeStruct((rows // (2 * parts), rank), F32)] * outs,
        scratch_shapes=[pltpu.VMEM((DEPTH, n, wide), F32)] * 2
        + ([pltpu.VMEM((DEPTH, wide, rank), F32)] if first else [])
        + [pltpu.SemaphoreType.DMA((3 if first else 2, DEPTH))],
        compiler_params=params(34 if first else 30),
        cost_estimate=cost(6 * n * cols * rank, 4 * (2 * n * cols + cols * rank)),
        name="left_rows",
    )(at, gradient, momentum, *right)


def total_kernel(count, *refs):
    ins, outs = refs[:count], refs[count:]
    n = outs[0].shape[0]
    for i, out in enumerate(outs):
        terms = [x[i * n : (i + 1) * n, :] for x in ins]
        while len(terms) > 1:
            terms = [terms[k] + terms[k + 1] for k in range(0, len(terms), 2)]
        out[...] = terms[0]


def total(*blocks, parts=1):
    rows, rank = blocks[0].shape
    outs = pl.pallas_call(
        functools.partial(total_kernel, len(blocks)),
        in_specs=[VMEM] * len(blocks),
        out_specs=[VMEM] * parts,
        out_shape=[jax.ShapeDtypeStruct((rows // parts, rank), F32)] * parts,
        compiler_params=params(6),
        cost_estimate=cost(rows * rank, 4 * (len(blocks) + 1) * rows * rank),
        name="total",
    )(*blocks)
    return outs[0] if parts == 1 else outs


def gram_kernel(place, at, *refs):
    pieces, (left, lh, ll, send, keep, gram) = refs[:-6], refs[-6:]
    n = pieces[0].shape[0]
    for i, piece in enumerate(pieces):
        x = piece[...]
        rows = pl.ds(i * n, n)
        left[rows, :] = x
        lh[rows, :], ll[rows, :] = split(x)
    half = left.shape[0] // 2
    own, other = left[:half, :], left[half:, :]
    gram[...] = dot_high(own, own, TN) + dot_high(other, other, TN)
    n, core = send.shape[0], at[place]
    send[...] = gram[pl.ds(pl.multiple_of((1 - core) * n, GROUP), n), :]
    keep[...] = gram[pl.ds(pl.multiple_of(core * n, GROUP), n), :]


def gram_of(at, place, pieces):
    rank = pieces[0].shape[1]
    rows = sum(p.shape[0] for p in pieces)
    return pl.pallas_call(
        functools.partial(gram_kernel, place),
        in_specs=[SMEM] + [VMEM] * len(pieces),
        out_specs=[VMEM] * 5,
        out_shape=[
            jax.ShapeDtypeStruct((rows, rank), F32),
            jax.ShapeDtypeStruct((rows, rank), BF16),
            jax.ShapeDtypeStruct((rows, rank), BF16),
            jax.ShapeDtypeStruct((rank // 2, rank), F32),
            jax.ShapeDtypeStruct((rank // 2, rank), F32),
        ],
        scratch_shapes=[pltpu.VMEM((rank, rank), F32)],
        compiler_params=params(8),
        cost_estimate=cost(12 * rows * rank * rank, 12 * rows * rank),
        name="gram_of",
    )(at, *pieces)


def w_term(unit, width, lh, ll, buffers):
    part = pl.ds(pl.multiple_of(unit * width, LANES), width)
    bh, bl = split(jnp.concatenate([x[:, part] for x in buffers], axis=0))
    return dot3(bh, bl, lh[...], ll[...], TN)


def w_send_kernel(place, at, lh, ll, *refs):
    *buffers, out = refs
    out[...] = w_term(at[place + pl.program_id(0)], out.shape[0], lh, ll, buffers)


def w_keep_kernel(place, at, got, lh, ll, *refs):
    *buffers, send, keep = refs
    i, width = pl.program_id(0), send.shape[0]
    value = w_term(at[place + i], width, lh, ll, buffers) + got[...]

    @pl.when(i == 0)
    def _():
        send[...] = value

    @pl.when(i == 1)
    def _():
        keep[...] = value


def w_cost(rows, rank, unit):
    return cost(2 * 6 * rows * unit * rank, 2 * 4 * unit * rank)


def w_send(at, place, lh, ll, unit, *buffers):
    rows, rank = lh.shape
    return pl.pallas_call(
        functools.partial(w_send_kernel, place),
        grid_spec=pltpu.PrefetchScalarGridSpec(
            num_scalar_prefetch=1,
            grid=(2,),
            in_specs=[VMEM] * (2 + len(buffers)),
            out_specs=pl.BlockSpec((unit, rank), lambda i, at: (i, 0)),
        ),
        out_shape=jax.ShapeDtypeStruct((2 * unit, rank), F32),
        compiler_params=params(12),
        cost_estimate=w_cost(rows, rank, unit),
        name="w_send",
    )(at, lh, ll, *buffers)


def w_keep(at, place, got, lh, ll, unit, *buffers):
    rows, rank = lh.shape
    one = pl.BlockSpec((unit, rank), lambda i, at: (0, 0))
    return pl.pallas_call(
        functools.partial(w_keep_kernel, place),
        grid_spec=pltpu.PrefetchScalarGridSpec(
            num_scalar_prefetch=1,
            grid=(2,),
            in_specs=[pl.BlockSpec((unit, rank), lambda i, at: (at[place + 2 + i], 0))]
            + [VMEM] * (2 + len(buffers)),
            out_specs=[one, one],
        ),
        out_shape=[jax.ShapeDtypeStruct((unit, rank), F32)] * 2,
        compiler_params=params(14),
        cost_estimate=w_cost(rows, rank, unit),
        name="w_keep",
    )(at, got, lh, ll, *buffers)


GROUP = 8


def factor_group(rows, at):
    full = (GROUP, LANES)
    columns = [jnp.broadcast_to(rows[:, at + j : at + j + 1], full) for j in range(GROUP)]
    a = {
        (i, j): jnp.broadcast_to(columns[j][i : i + 1, :], full)
        for j in range(GROUP)
        for i in range(j, GROUP)
    }
    low, c = {}, {}
    for k in range(GROUP):
        c[k, k] = lax.rsqrt(a[k, k])
        for i in range(k + 1, GROUP):
            low[i, k] = a[i, k] * c[k, k]
        for j in range(k + 1, GROUP):
            for i in range(j, GROUP):
                a[i, j] = a[i, j] - low[i, k] * low[j, k]
        for j in range(k):
            total = low[k, j] * c[j, j]
            for i in range(j + 1, k):
                total = total + low[k, i] * c[i, j]
            c[k, j] = -c[k, k] * total
    return c


def spread(x, width):
    return jnp.concatenate([x] * (width // LANES), axis=1)


def eliminate(block):
    size, width = block.shape
    sub = lax.broadcasted_iota(jnp.int32, (GROUP, LANES), 0)
    groups = [block[i : i + GROUP, :] for i in range(0, size, GROUP)]
    for p in range(len(groups)):
        at = p * GROUP
        rows = groups[p]
        c = factor_group(rows, at)
        done = None
        for j in range(GROUP):
            col = jnp.zeros((GROUP, LANES), F32)
            for i in range(j, GROUP):
                col = jnp.where(sub == i, c[i, j], col)
            term = spread(col, width) * jnp.broadcast_to(rows[j : j + 1, :], (GROUP, width))
            done = term if done is None else done + term
        groups[p] = done
        if p + 1 == len(groups):
            break
        solved = None
        for k in range(GROUP):
            col = jnp.zeros((GROUP, LANES), F32)
            for j in range(k + 1):
                col = jnp.where(sub == j, c[k, j], col)
            term = spread(col, width) * jnp.broadcast_to(done[k : k + 1, :], (GROUP, width))
            solved = term if solved is None else solved + term
        for q in range(p + 1, len(groups)):
            x = groups[q]
            total = None
            for j in range(GROUP):
                term = jnp.broadcast_to(x[:, at + j : at + j + 1], (GROUP, width)) * jnp.broadcast_to(
                    solved[j : j + 1, :], (GROUP, width)
                )
                total = term if total is None else total + term
            groups[q] = x - total
    return jnp.concatenate(groups, axis=0)


def chol_kernel(place, at, mine, beside, left, x_out, oh, ol, work):
    n, rank = mine.shape
    size = min(64, rank)
    core = at[place]
    work[pl.ds(pl.multiple_of(core * n, GROUP), n), :rank] = mine[...]
    work[pl.ds(pl.multiple_of((1 - core) * n, GROUP), n), :rank] = beside[...]
    r = lax.broadcasted_iota(jnp.int32, (rank, rank), 0)
    c = lax.broadcasted_iota(jnp.int32, (rank, rank), 1)
    work[:, rank:] = jnp.where(r == c, 1.0, 0.0).astype(F32)

    def step(b, _):
        top = pl.multiple_of(b * size, size)
        rows = pl.ds(top, size)
        width = 2 * rank
        block = pltpu.roll(work[rows, :], lax.rem(width - top, width), 1)
        block = pltpu.roll(eliminate(block), top, 1)
        x_out[rows, :] = block[:, rank:]

        @pl.when(b + 1 < rank // size)
        def _():
            work[...] -= dot_high(block[:, :rank], block, TN)

        return 0

    lax.fori_loop(0, rank // size, step, 0)
    h, l = split(dot_high(left[...], x_out[...], NT))
    oh[...] = h
    ol[...] = l


def chol_inverse(at, place, mine, beside, left):
    rows, rank = left.shape
    return pl.pallas_call(
        functools.partial(chol_kernel, place),
        in_specs=[SMEM] + [VMEM] * 3,
        out_specs=[VMEM] * 3,
        out_shape=[
            jax.ShapeDtypeStruct((rank, rank), F32),
            jax.ShapeDtypeStruct((rows, rank), BF16),
            jax.ShapeDtypeStruct((rows, rank), BF16),
        ],
        scratch_shapes=[pltpu.VMEM((rank, 2 * rank), F32)],
        compiler_params=params(8),
        cost_estimate=cost(4e9, 4 * rows * rank),
        name="chol_inverse",
    )(at, mine, beside, left)


def right_kernel(place, cols, at, ka, ga, kb, gb, x, ra, rb, squares):
    rows, rank = ka.shape
    total = jnp.zeros((1, rank), F32)
    for i, (k, g, out) in enumerate(((ka, ga, ra), (kb, gb, rb))):
        value = dot_high(k[...] + g[...], x[...], NT)
        out[...] = value
        row = lax.broadcasted_iota(jnp.int32, (rows, rank), 0) + at[place + i]
        value = jnp.where(row < cols, value, 0.0)
        total = total + jnp.sum(value * value, axis=0, keepdims=True)
    squares[...] = jnp.broadcast_to(total, squares.shape)


def right_rows(at, place, cols, ka, ga, kb, gb, x):
    rows, rank = ka.shape
    vm = pl.BlockSpec(memory_space=pltpu.VMEM)
    return pl.pallas_call(
        functools.partial(right_kernel, place, cols),
        in_specs=[pl.BlockSpec(memory_space=pltpu.SMEM)] + [vm] * 5,
        out_specs=[vm] * 3,
        out_shape=[jax.ShapeDtypeStruct((rows, rank), F32)] * 2
        + [jax.ShapeDtypeStruct((GROUP, rank), F32)],
        compiler_params=params(8),
        cost_estimate=cost(24 * rows * rank * rank, 24 * rows * rank),
        name="right_rows",
    )(at, ka, ga, kb, gb, x)


def join_kernel(place, at, x, y, both, *parts):
    n, t = x.shape[0], at[place]
    both[pl.ds(pl.multiple_of(t * n, GROUP), n), :] = x[...]
    both[pl.ds(pl.multiple_of((1 - t) * n, GROUP), n), :] = y[...]
    top = 0
    for out in parts:
        out[...] = both[top : top + out.shape[0], :]
        top += out.shape[0]


def join(at, place, x, y, sizes):
    rows, rank = x.shape
    return pl.pallas_call(
        functools.partial(join_kernel, place),
        in_specs=[SMEM, VMEM, VMEM],
        out_specs=[VMEM] * (1 + len(sizes)),
        out_shape=[jax.ShapeDtypeStruct((n, rank), F32) for n in [2 * rows, *sizes]],
        compiler_params=params(6),
        cost_estimate=cost(rows * rank, 16 * rows * rank),
        name="join",
    )(at, x, y)


def halve_kernel(place, at, x, y, send, keep):
    n, t = send.shape[0], at[place]
    for part, out in ((1 - t, send), (t, keep)):
        rows = pl.ds(pl.multiple_of(part * n, GROUP), n)
        out[...] = x[rows, :] + y[rows, :]


def halve(at, place, x, y):
    rows, rank = x.shape
    return pl.pallas_call(
        functools.partial(halve_kernel, place),
        in_specs=[SMEM, VMEM, VMEM],
        out_specs=[VMEM, VMEM],
        out_shape=[jax.ShapeDtypeStruct((rows // 2, rank), F32)] * 2,
        compiler_params=params(6),
        cost_estimate=cost(rows * rank, 12 * rows * rank),
        name="halve",
    )(at, x, y)


SLOTS = 2


def final_kernel(held, place, group, unit, total_cols, factor, at, *refs):
    pieces, (squares, oh, ol), buffers = refs[:4], refs[4:7], refs[7 : 7 + held]
    update, momentum, new_right, stage_m, stage_u, stage_r, lh, ll, high, low, sems = refs[-11:]
    start, count = group
    n, rows = count * LANES, oh.shape[0]
    half = rows // 2
    blocks = update.shape[1] // LANES
    *own, other = buffers
    ranges = [(x, 0, i * x.shape[0]) for i, x in enumerate(own)] + [(other, 1, 0)]
    scale = jnp.sqrt(squares[0:1, :] / total_cols + 1e-06)
    lh[:rows, :] = oh[...]
    ll[:rows, :] = ol[...]
    lh[rows:, :], ll[rows:, :] = split((oh[...].astype(F32) + ol[...].astype(F32)) * (factor / scale))

    def each_copy(k, act):
        slot = lax.rem(k, SLOTS)
        first = at[place + k] * (unit // LANES) + start
        for j in range(count):

            @pl.when(first + j < blocks)
            def _(j=j):
                here = pl.ds(j * LANES, LANES)
                there = pl.ds(pl.multiple_of((first + j) * LANES, LANES), LANES)
                for i, (a, b) in enumerate(
                    (
                        (stage_m.at[slot, :, here], momentum.at[:, there]),
                        (stage_u.at[slot, :, here], update.at[:, there]),
                        (stage_r.at[slot, here, :], new_right.at[there, :]),
                    )
                ):
                    act(pltpu.make_async_copy(a, b, sems.at[i, slot, j]))

    def body(k, _):
        slot = lax.rem(k, SLOTS)

        @pl.when(k >= SLOTS)
        def _():
            each_copy(k - SLOTS, lambda copy: copy.wait())

        for i, piece in enumerate(pieces):

            @pl.when(k == i)
            def _(piece=piece):
                right = piece[...]
                high[...], low[...] = split(right)
                stage_r[slot] = right / scale

        part = pl.ds(pl.multiple_of(at[place + k] * unit + start * LANES, LANES), n)
        value = dot(lh[...], high[...], NT) + dot(ll[...], high[...], NT)
        rest = dot(lh[rows:, :], low[...], NT)
        for buffer, h, past in ranges:
            size, top = buffer.shape[0], h * half + past
            here = pl.ds(pl.multiple_of(at[h] * half + past, GROUP), size)
            stage_m[slot, here, :] = buffer[:, part] - 0.05 * value[top : top + size]
            stage_u[slot, here, :] = value[rows + top : rows + top + size] + rest[top : top + size]
        each_copy(k, lambda copy: copy.start())
        return 0

    lax.fori_loop(0, 4, body, 0)
    for k in range(4 - SLOTS, 4):
        each_copy(k, lambda copy: copy.wait())


def final(at, place, group, unit, pieces, squares, oh, ol, buffers, sizes, before):
    rows, rank = oh.shape
    cols, total_rows, total_cols = sizes
    factor = (total_rows / rank) ** 0.5
    n = group[1] * LANES
    return pl.pallas_call(
        functools.partial(final_kernel, len(buffers), place, group, unit, total_cols, factor),
        in_specs=[SMEM] + [VMEM] * (7 + len(buffers)) + [HBM] * len(before),
        out_specs=[HBM] * 3,
        out_shape=[
            jax.ShapeDtypeStruct((rows, cols), F32),
            jax.ShapeDtypeStruct((rows, cols), F32),
            jax.ShapeDtypeStruct((cols, rank), F32),
        ],
        scratch_shapes=[
            pltpu.VMEM((SLOTS, rows, n), F32),
            pltpu.VMEM((SLOTS, rows, n), F32),
            pltpu.VMEM((SLOTS, n, rank), F32),
            pltpu.VMEM((2 * rows, rank), BF16),
            pltpu.VMEM((2 * rows, rank), BF16),
            pltpu.VMEM((n, rank), BF16),
            pltpu.VMEM((n, rank), BF16),
            pltpu.SemaphoreType.DMA((3, SLOTS, group[1])),
        ],
        input_output_aliases={len(buffers) + 8 + i: i for i in range(len(before))},
        compiler_params=params(28),
        cost_estimate=cost(48 * rows * n * rank, 32 * rows * n),
        name="final",
    )(at, *pieces, squares, oh, ol, *buffers, *before)


def power_of_two(n):
    return n & (n - 1) == 0


def bits_of(n):
    return list(range(n.bit_length() - 1))


def swap(x, axis, *places):
    n = lax.axis_size(axis)
    mask = sum(1 << bit for bit in places)
    return lax.ppermute(x, axis, [(i, i ^ mask) for i in range(n)])


def spread_sum(x, bits):
    for b in bits[3:]:
        x = total(x, swap(x, "dp", b))
    b, c = bits[1:3]
    others = [swap(x, "dp", *m) for m in ((b,), (c,), (b, c))]
    return total(x, *others)


def on_device(gradient, momentum, right_factor):
    rows, cols = gradient.shape
    n_dp, n_tp = lax.axis_size("dp"), lax.axis_size("tensor")
    d, z = lax.axis_index("dp"), lax.axis_index("tensor")
    bits = bits_of(n_dp)

    unit = LANES * (-(-cols // (8 * LANES)))
    orders = [bits[1:], bits[1:][::-1]]
    table = []

    def put(*values):
        table.extend(values)
        return len(table) - len(values)

    bit_of = lambda b: (d >> b) & 1
    s, core = z & 1, d & 1
    put(s, 1 - s)
    core_at = put(core)
    send_at, keep_at, bit_at, near, far, first = [], [], [], [], [], []
    for h, order in enumerate(orders):
        t = bit_of(order[0])
        base, beside = 4 * h + 2 * core, 4 * h + 2 * (1 - core)
        send_at.append(put(beside, beside + 1))
        keep_at.append(put(base + 1 - t, base + t, 1 - t, t))
        bit_at.append({b: put(bit_of(b)) for b in order[1:]})
        near += [base + t, beside + t]
        far += [base + 1 - t, beside + 1 - t]
        at, n = (base + t) * unit, unit
        for b in order[1:]:
            n = n // 2
            at = at + bit_of(b) * n
        first.append(at)
    near_at, far_at, first_at = put(*near), put(*far), put(*first)
    at = jnp.stack([jnp.asarray(v, jnp.int32) for v in table])

    parts = 2 if rows % (4 * GROUP) == 0 else 1
    other, rh, rl, *away = left_rows(at, 1, 0, parts, gradient, momentum, right_factor, 8 * unit)
    own, mine = [], []
    for i in range(parts):
        x, y = left_rows(at, 0, i, parts, gradient, momentum, (rh, rl), 8 * unit)
        own.append(x)
        mine.append(y)
    held = (*own, other)
    if power_of_two(n_tp) and n_tp > 1:
        pieces = []
        for i in range(parts):
            got = swap(away[i], "tensor", 0)
            pieces.append(total(mine[i], got))
        for bit in bits_of(n_tp)[1:]:
            for i in range(parts):
                got = swap(pieces[i], "tensor", bit)
                pieces[i] = total(pieces[i], got)
        for i in range(parts):
            pieces.append(swap(pieces[i], "tensor", 0))
    else:
        mine, away = jnp.concatenate(mine), jnp.concatenate(away)
        both = lax.psum(jnp.where(s == 0, jnp.stack([mine, away]), jnp.stack([away, mine])), "tensor")
        pieces = [lax.dynamic_index_in_dim(both, i, 0, False) for i in (s, 1 - s)]

    left, lh, ll, send, gram = gram_of(at, core_at, pieces)
    got = swap(send, "dp", 0)
    gram = spread_sum(total(gram, got), bits)
    gram_beside = swap(gram, "dp", 0)

    got = []
    for h in range(2):
        sent = w_send(at, send_at[h], lh, ll, unit, *held)
        got.append(swap(sent, "dp", 0))
    kept = []
    for h, order in enumerate(orders):
        send, keep = w_keep(at, keep_at[h], got[h], lh, ll, unit, *held)
        recv = swap(send, "dp", order[0])
        for b in order[1:]:
            send, keep = halve(at, bit_at[h][b], keep, recv)
            recv = swap(send, "dp", b)
        kept += [keep, recv]

    x_inv, oh, ol = chol_inverse(at, core_at, gram, gram_beside, left)
    *right, squares = right_rows(at, first_at, cols, *kept, x_inv)
    if power_of_two(n_tp):
        for b in bits_of(n_tp):
            squares = total(squares, swap(squares, "tensor", b))
    else:
        squares = lax.psum(squares, "tensor")
    got = swap(squares, "dp", 0)
    squares = total(squares, got)
    squares = spread_sum(squares, bits)

    blocks = unit // LANES
    groups = ((0, blocks - blocks // 2), (blocks - blocks // 2, blocks // 2))
    near, far = [], ([], [])
    for h, (order, x) in enumerate(zip(orders, right)):
        parts = [x]
        for b in order[:0:-1]:
            y = swap(x, "dp", b)
            last = 2 * x.shape[0] == unit
            x, *parts = join(
                at, bit_at[h][b], x, y, [count * LANES for _, count in groups] if last else []
            )
        for g, part in enumerate(parts):
            y = swap(part, "dp", order[0])
            far[g].extend([y, swap(y, "dp", 0)])
        near.extend([x, swap(x, "dp", 0)])

    same = (squares, oh, ol, held, (cols, rows * n_dp, cols * n_tp))
    outs = final(at, near_at, (0, blocks), unit, near, *same, ())
    for g in range(2):
        outs = final(at, far_at, groups[g], unit, far[g], *same, outs)
    return tuple(outs)


def solution(mesh):
    return jax.shard_map(
        on_device,
        mesh=mesh,
        in_specs=(P("dp", "tensor"), P("dp", "tensor"), P("tensor", None)),
        out_specs=(P("dp", "tensor"), P("dp", "tensor"), P("tensor", None)),
        check_vma=False,
    )
```

```python
import functools

import jax
import jax.numpy as jnp
from jax import lax
from jax.experimental import pallas as pl
from jax.experimental.pallas import tpu as pltpu
from jax.sharding import PartitionSpec as P


F32 = jnp.float32
BF16 = jnp.bfloat16
HIGH = lax.Precision.HIGHEST
LANES = 128

NN = (((1,), (0,)), ((), ()))
NT = (((1,), (1,)), ((), ()))
TN = (((0,), (0,)), ((), ()))


HBM = pl.BlockSpec(memory_space=pltpu.HBM)
VMEM = pl.BlockSpec(memory_space=pltpu.VMEM)
SMEM = pl.BlockSpec(memory_space=pltpu.SMEM)


def params(mib):
    return pltpu.CompilerParams(vmem_limit_bytes=mib * 1024 * 1024)


def cost(flops, moved):
    return pl.CostEstimate(flops=int(flops), bytes_accessed=int(moved), transcendentals=0)


def split(x):
    hi = x.astype(BF16)
    lo = (x - hi.astype(F32)).astype(BF16)
    return hi, lo


def dot(a, b, dims):
    return lax.dot_general(a, b, dims, preferred_element_type=F32)


def dot3(ah, al, bh, bl, dims):
    return dot(ah, bh, dims) + (dot(ah, bl, dims) + dot(al, bh, dims))


def dot_high(a, b, dims):
    return lax.dot_general(a, b, dims, precision=HIGH, preferred_element_type=F32)


def column_block(cols):
    blocks = cols // LANES
    return LANES * max(k for k in range(1, 9) if blocks % k == 0)


FIRST_DEPTH, LATER_DEPTH = 6, 9


def left_kernel(first, which, part, at, g, m, *refs):
    if first:
        r, buffer, rh, rl, *outs, gs, ms, rs, sems = refs
    else:
        rh, rl, buffer, *outs, gs, ms, sems = refs
    depth, n, wide = gs.shape
    steps = g.shape[1] // wide
    top = at[which] * (g.shape[0] // 2) + part * n
    rows = pl.ds(pl.multiple_of(top, GROUP), n)

    def copies(j, slot):
        part = pl.ds(pl.multiple_of(j * wide, LANES), wide)
        some = [
            pltpu.make_async_copy(g.at[rows, part], gs.at[slot], sems.at[0, slot]),
            pltpu.make_async_copy(m.at[rows, part], ms.at[slot], sems.at[1, slot]),
        ]
        if first:
            some.append(pltpu.make_async_copy(r.at[part, :], rs.at[slot], sems.at[2, slot]))
        return some

    for j in range(min(depth, steps)):
        for copy in copies(j, j):
            copy.start()
    for out in outs:
        out[...] = jnp.zeros_like(out)

    def body(j, _):
        slot = lax.rem(j, depth)
        part = pl.ds(pl.multiple_of(j * wide, LANES), wide)
        for copy in copies(j, slot):
            copy.wait()
        b = gs[slot] + ms[slot]
        buffer[:, part] = b
        bh, bl = split(b)
        if first:
            rh[part, :], rl[part, :] = split(rs[slot])
        term = dot3(bh, bl, rh[part, :], rl[part, :], NN)
        size = n // len(outs)
        for i, out in enumerate(outs):
            out[...] += term[i * size : (i + 1) * size]

        @pl.when(j + depth < steps)
        def _():
            for copy in copies(j + depth, slot):
                copy.start()

        return 0

    lax.fori_loop(0, steps, body, 0)


def left_rows(at, which, part, parts, gradient, momentum, right, padded):
    first = not isinstance(right, tuple)
    right = (right,) if first else right
    rows, cols = gradient.shape
    rank = right[0].shape[1]
    wide = column_block(cols)
    n = rows // 2 if first else rows // (2 * parts)
    outs = parts if first else 1
    depth = FIRST_DEPTH if first else LATER_DEPTH
    terms = [pltpu.VMEM((cols, rank), BF16)] * 2 if first else []
    return pl.pallas_call(
        functools.partial(left_kernel, first, which, part),
        in_specs=[SMEM, HBM, HBM] + ([HBM] if first else [VMEM, VMEM]),
        out_specs=[VMEM] * (1 + len(terms) + outs),
        out_shape=[pltpu.VMEM((n, padded), F32)]
        + terms
        + [jax.ShapeDtypeStruct((rows // (2 * parts), rank), F32)] * outs,
        scratch_shapes=[pltpu.VMEM((depth, n, wide), F32)] * 2
        + ([pltpu.VMEM((depth, wide, rank), F32)] if first else [])
        + [pltpu.SemaphoreType.DMA((3 if first else 2, depth))],
        compiler_params=params(34 if first else 30),
        cost_estimate=cost(6 * n * cols * rank, 4 * (2 * n * cols + cols * rank)),
        name="left_rows",
    )(at, gradient, momentum, *right)


def total_kernel(count, *refs):
    ins, outs = refs[:count], refs[count:]
    n = outs[0].shape[0]
    for i, out in enumerate(outs):
        terms = [x[i * n : (i + 1) * n, :] for x in ins]
        while len(terms) > 1:
            terms = [terms[k] + terms[k + 1] for k in range(0, len(terms), 2)]
        out[...] = terms[0]


def total(*blocks, parts=1):
    rows, rank = blocks[0].shape
    outs = pl.pallas_call(
        functools.partial(total_kernel, len(blocks)),
        in_specs=[VMEM] * len(blocks),
        out_specs=[VMEM] * parts,
        out_shape=[jax.ShapeDtypeStruct((rows // parts, rank), F32)] * parts,
        compiler_params=params(6),
        cost_estimate=cost(rows * rank, 4 * (len(blocks) + 1) * rows * rank),
        name="total",
    )(*blocks)
    return outs[0] if parts == 1 else outs


def gram_kernel(place, at, *refs):
    pieces, (left, lh, ll, send, keep, gram) = refs[:-6], refs[-6:]
    n = pieces[0].shape[0]
    for i, piece in enumerate(pieces):
        x = piece[...]
        rows = pl.ds(i * n, n)
        left[rows, :] = x
        lh[rows, :], ll[rows, :] = split(x)
    half = left.shape[0] // 2
    own, other = left[:half, :], left[half:, :]
    gram[...] = dot_high(own, own, TN) + dot_high(other, other, TN)
    n, core = send.shape[0], at[place]
    send[...] = gram[pl.ds(pl.multiple_of((1 - core) * n, GROUP), n), :]
    keep[...] = gram[pl.ds(pl.multiple_of(core * n, GROUP), n), :]


def gram_of(at, place, pieces):
    rank = pieces[0].shape[1]
    rows = sum(p.shape[0] for p in pieces)
    return pl.pallas_call(
        functools.partial(gram_kernel, place),
        in_specs=[SMEM] + [VMEM] * len(pieces),
        out_specs=[VMEM] * 5,
        out_shape=[
            jax.ShapeDtypeStruct((rows, rank), F32),
            jax.ShapeDtypeStruct((rows, rank), BF16),
            jax.ShapeDtypeStruct((rows, rank), BF16),
            jax.ShapeDtypeStruct((rank // 2, rank), F32),
            jax.ShapeDtypeStruct((rank // 2, rank), F32),
        ],
        scratch_shapes=[pltpu.VMEM((rank, rank), F32)],
        compiler_params=params(8),
        cost_estimate=cost(12 * rows * rank * rank, 12 * rows * rank),
        name="gram_of",
    )(at, *pieces)


def w_term(unit, width, lh, ll, buffers):
    part = pl.ds(pl.multiple_of(unit * width, LANES), width)
    bh, bl = split(jnp.concatenate([x[:, part] for x in buffers], axis=0))
    return dot3(bh, bl, lh[...], ll[...], TN)


def w_send_kernel(place, at, lh, ll, *refs):
    *buffers, out = refs
    out[...] = w_term(at[place + pl.program_id(0)], out.shape[0], lh, ll, buffers)


def w_keep_kernel(place, at, got, lh, ll, *refs):
    *buffers, send, keep = refs
    i, width = pl.program_id(0), send.shape[0]
    value = w_term(at[place + i], width, lh, ll, buffers) + got[...]

    @pl.when(i == 0)
    def _():
        send[...] = value

    @pl.when(i == 1)
    def _():
        keep[...] = value


def w_cost(rows, rank, unit):
    return cost(2 * 6 * rows * unit * rank, 2 * 4 * unit * rank)


def w_send(at, place, lh, ll, unit, *buffers):
    rows, rank = lh.shape
    return pl.pallas_call(
        functools.partial(w_send_kernel, place),
        grid_spec=pltpu.PrefetchScalarGridSpec(
            num_scalar_prefetch=1,
            grid=(2,),
            in_specs=[VMEM] * (2 + len(buffers)),
            out_specs=pl.BlockSpec((unit, rank), lambda i, at: (i, 0)),
        ),
        out_shape=jax.ShapeDtypeStruct((2 * unit, rank), F32),
        compiler_params=params(12),
        cost_estimate=w_cost(rows, rank, unit),
        name="w_send",
    )(at, lh, ll, *buffers)


def w_keep(at, place, got, lh, ll, unit, *buffers):
    rows, rank = lh.shape
    one = pl.BlockSpec((unit, rank), lambda i, at: (0, 0))
    return pl.pallas_call(
        functools.partial(w_keep_kernel, place),
        grid_spec=pltpu.PrefetchScalarGridSpec(
            num_scalar_prefetch=1,
            grid=(2,),
            in_specs=[pl.BlockSpec((unit, rank), lambda i, at: (at[place + 2 + i], 0))]
            + [VMEM] * (2 + len(buffers)),
            out_specs=[one, one],
        ),
        out_shape=[jax.ShapeDtypeStruct((unit, rank), F32)] * 2,
        compiler_params=params(14),
        cost_estimate=w_cost(rows, rank, unit),
        name="w_keep",
    )(at, got, lh, ll, *buffers)


GROUP = 8


def factor_group(rows, at):
    full = (GROUP, LANES)
    columns = [jnp.broadcast_to(rows[:, at + j : at + j + 1], full) for j in range(GROUP)]
    a = {
        (i, j): jnp.broadcast_to(columns[j][i : i + 1, :], full)
        for j in range(GROUP)
        for i in range(j, GROUP)
    }
    low, c = {}, {}
    for k in range(GROUP):
        c[k, k] = lax.rsqrt(a[k, k])
        for i in range(k + 1, GROUP):
            low[i, k] = a[i, k] * c[k, k]
        for j in range(k + 1, GROUP):
            for i in range(j, GROUP):
                a[i, j] = a[i, j] - low[i, k] * low[j, k]
        for j in range(k):
            total = low[k, j] * c[j, j]
            for i in range(j + 1, k):
                total = total + low[k, i] * c[i, j]
            c[k, j] = -c[k, k] * total
    return c


def spread(x, width):
    return jnp.concatenate([x] * (width // LANES), axis=1)


def eliminate(block):
    size, width = block.shape
    sub = lax.broadcasted_iota(jnp.int32, (GROUP, LANES), 0)
    groups = [block[i : i + GROUP, :] for i in range(0, size, GROUP)]
    for p in range(len(groups)):
        at = p * GROUP
        rows = groups[p]
        c = factor_group(rows, at)
        done = None
        for j in range(GROUP):
            col = jnp.zeros((GROUP, LANES), F32)
            for i in range(j, GROUP):
                col = jnp.where(sub == i, c[i, j], col)
            term = spread(col, width) * jnp.broadcast_to(rows[j : j + 1, :], (GROUP, width))
            done = term if done is None else done + term
        groups[p] = done
        if p + 1 == len(groups):
            break
        solved = None
        for k in range(GROUP):
            col = jnp.zeros((GROUP, LANES), F32)
            for j in range(k + 1):
                col = jnp.where(sub == j, c[k, j], col)
            term = spread(col, width) * jnp.broadcast_to(done[k : k + 1, :], (GROUP, width))
            solved = term if solved is None else solved + term
        for q in range(p + 1, len(groups)):
            x = groups[q]
            total = None
            for j in range(GROUP):
                term = jnp.broadcast_to(x[:, at + j : at + j + 1], (GROUP, width)) * jnp.broadcast_to(
                    solved[j : j + 1, :], (GROUP, width)
                )
                total = term if total is None else total + term
            groups[q] = x - total
    return jnp.concatenate(groups, axis=0)


def chol_kernel(place, at, mine, beside, left, x_out, oh, ol, work):
    n, rank = mine.shape
    size = min(64, rank)
    core = at[place]
    work[pl.ds(pl.multiple_of(core * n, GROUP), n), :rank] = mine[...]
    work[pl.ds(pl.multiple_of((1 - core) * n, GROUP), n), :rank] = beside[...]
    r = lax.broadcasted_iota(jnp.int32, (rank, rank), 0)
    c = lax.broadcasted_iota(jnp.int32, (rank, rank), 1)
    work[:, rank:] = jnp.where(r == c, 1.0, 0.0).astype(F32)

    def step(b, _):
        top = pl.multiple_of(b * size, size)
        rows = pl.ds(top, size)
        width = 2 * rank
        block = pltpu.roll(work[rows, :], lax.rem(width - top, width), 1)
        block = pltpu.roll(eliminate(block), top, 1)
        x_out[rows, :] = block[:, rank:]

        @pl.when(b + 1 < rank // size)
        def _():
            work[...] -= dot_high(block[:, :rank], block, TN)

        return 0

    lax.fori_loop(0, rank // size, step, 0)
    h, l = split(dot_high(left[...], x_out[...], NT))
    oh[...] = h
    ol[...] = l


def chol_inverse(at, place, mine, beside, left):
    rows, rank = left.shape
    return pl.pallas_call(
        functools.partial(chol_kernel, place),
        in_specs=[SMEM] + [VMEM] * 3,
        out_specs=[VMEM] * 3,
        out_shape=[
            jax.ShapeDtypeStruct((rank, rank), F32),
            jax.ShapeDtypeStruct((rows, rank), BF16),
            jax.ShapeDtypeStruct((rows, rank), BF16),
        ],
        scratch_shapes=[pltpu.VMEM((rank, 2 * rank), F32)],
        compiler_params=params(8),
        cost_estimate=cost(4e9, 4 * rows * rank),
        name="chol_inverse",
    )(at, mine, beside, left)


def right_kernel(place, cols, at, ka, ga, kb, gb, x, ra, rb, squares):
    rows, rank = ka.shape
    total = jnp.zeros((1, rank), F32)
    for i, (k, g, out) in enumerate(((ka, ga, ra), (kb, gb, rb))):
        value = dot_high(k[...] + g[...], x[...], NT)
        out[...] = value
        row = lax.broadcasted_iota(jnp.int32, (rows, rank), 0) + at[place + i]
        value = jnp.where(row < cols, value, 0.0)
        total = total + jnp.sum(value * value, axis=0, keepdims=True)
    squares[...] = jnp.broadcast_to(total, squares.shape)


def right_rows(at, place, cols, ka, ga, kb, gb, x):
    rows, rank = ka.shape
    vm = pl.BlockSpec(memory_space=pltpu.VMEM)
    return pl.pallas_call(
        functools.partial(right_kernel, place, cols),
        in_specs=[pl.BlockSpec(memory_space=pltpu.SMEM)] + [vm] * 5,
        out_specs=[vm] * 3,
        out_shape=[jax.ShapeDtypeStruct((rows, rank), F32)] * 2
        + [jax.ShapeDtypeStruct((GROUP, rank), F32)],
        compiler_params=params(8),
        cost_estimate=cost(24 * rows * rank * rank, 24 * rows * rank),
        name="right_rows",
    )(at, ka, ga, kb, gb, x)


def join_kernel(place, at, x, y, both, *parts):
    n, t = x.shape[0], at[place]
    both[pl.ds(pl.multiple_of(t * n, GROUP), n), :] = x[...]
    both[pl.ds(pl.multiple_of((1 - t) * n, GROUP), n), :] = y[...]
    top = 0
    for out in parts:
        out[...] = both[top : top + out.shape[0], :]
        top += out.shape[0]


def join(at, place, x, y, sizes):
    rows, rank = x.shape
    return pl.pallas_call(
        functools.partial(join_kernel, place),
        in_specs=[SMEM, VMEM, VMEM],
        out_specs=[VMEM] * (1 + len(sizes)),
        out_shape=[jax.ShapeDtypeStruct((n, rank), F32) for n in [2 * rows, *sizes]],
        compiler_params=params(6),
        cost_estimate=cost(rows * rank, 16 * rows * rank),
        name="join",
    )(at, x, y)


def halve_kernel(place, at, x, y, send, keep):
    n, t = send.shape[0], at[place]
    for part, out in ((1 - t, send), (t, keep)):
        rows = pl.ds(pl.multiple_of(part * n, GROUP), n)
        out[...] = x[rows, :] + y[rows, :]


def halve(at, place, x, y):
    rows, rank = x.shape
    return pl.pallas_call(
        functools.partial(halve_kernel, place),
        in_specs=[SMEM, VMEM, VMEM],
        out_specs=[VMEM, VMEM],
        out_shape=[jax.ShapeDtypeStruct((rows // 2, rank), F32)] * 2,
        compiler_params=params(6),
        cost_estimate=cost(rows * rank, 12 * rows * rank),
        name="halve",
    )(at, x, y)


SLOTS = 2


def final_kernel(held, place, group, unit, total_cols, factor, at, *refs):
    pieces, (squares, oh, ol), buffers = refs[:4], refs[4:7], refs[7 : 7 + held]
    update, momentum, new_right, stage_m, stage_u, stage_r, lh, ll, high, low, sems = refs[-11:]
    start, count = group
    n, rows = count * LANES, oh.shape[0]
    half = rows // 2
    blocks = update.shape[1] // LANES
    *own, other = buffers
    ranges = [(x, 0, i * x.shape[0]) for i, x in enumerate(own)] + [(other, 1, 0)]
    scale = jnp.sqrt(squares[0:1, :] / total_cols + 1e-06)
    lh[:rows, :] = oh[...]
    ll[:rows, :] = ol[...]
    lh[rows:, :], ll[rows:, :] = split((oh[...].astype(F32) + ol[...].astype(F32)) * (factor / scale))

    def each_copy(k, act):
        slot = lax.rem(k, SLOTS)
        first = at[place + k] * (unit // LANES) + start
        for j in range(count):

            @pl.when(first + j < blocks)
            def _(j=j):
                here = pl.ds(j * LANES, LANES)
                there = pl.ds(pl.multiple_of((first + j) * LANES, LANES), LANES)
                for i, (a, b) in enumerate(
                    (
                        (stage_m.at[slot, :, here], momentum.at[:, there]),
                        (stage_u.at[slot, :, here], update.at[:, there]),
                        (stage_r.at[slot, here, :], new_right.at[there, :]),
                    )
                ):
                    act(pltpu.make_async_copy(a, b, sems.at[i, slot, j]))

    def body(k, _):
        slot = lax.rem(k, SLOTS)

        @pl.when(k >= SLOTS)
        def _():
            each_copy(k - SLOTS, lambda copy: copy.wait())

        for i, piece in enumerate(pieces):

            @pl.when(k == i)
            def _(piece=piece):
                right = piece[...]
                high[...], low[...] = split(right)
                stage_r[slot] = right / scale

        part = pl.ds(pl.multiple_of(at[place + k] * unit + start * LANES, LANES), n)
        value = dot(lh[...], high[...], NT) + dot(ll[...], high[...], NT)
        rest = dot(lh[rows:, :], low[...], NT)
        for buffer, h, past in ranges:
            size, top = buffer.shape[0], h * half + past
            here = pl.ds(pl.multiple_of(at[h] * half + past, GROUP), size)
            stage_m[slot, here, :] = buffer[:, part] - 0.05 * value[top : top + size]
            stage_u[slot, here, :] = value[rows + top : rows + top + size] + rest[top : top + size]
        each_copy(k, lambda copy: copy.start())
        return 0

    lax.fori_loop(0, 4, body, 0)
    for k in range(4 - SLOTS, 4):
        each_copy(k, lambda copy: copy.wait())


def final(at, place, group, unit, pieces, squares, oh, ol, buffers, sizes, before):
    rows, rank = oh.shape
    cols, total_rows, total_cols = sizes
    factor = (total_rows / rank) ** 0.5
    n = group[1] * LANES
    return pl.pallas_call(
        functools.partial(final_kernel, len(buffers), place, group, unit, total_cols, factor),
        in_specs=[SMEM] + [VMEM] * (7 + len(buffers)) + [HBM] * len(before),
        out_specs=[HBM] * 3,
        out_shape=[
            jax.ShapeDtypeStruct((rows, cols), F32),
            jax.ShapeDtypeStruct((rows, cols), F32),
            jax.ShapeDtypeStruct((cols, rank), F32),
        ],
        scratch_shapes=[
            pltpu.VMEM((SLOTS, rows, n), F32),
            pltpu.VMEM((SLOTS, rows, n), F32),
            pltpu.VMEM((SLOTS, n, rank), F32),
            pltpu.VMEM((2 * rows, rank), BF16),
            pltpu.VMEM((2 * rows, rank), BF16),
            pltpu.VMEM((n, rank), BF16),
            pltpu.VMEM((n, rank), BF16),
            pltpu.SemaphoreType.DMA((3, SLOTS, group[1])),
        ],
        input_output_aliases={len(buffers) + 8 + i: i for i in range(len(before))},
        compiler_params=params(28),
        cost_estimate=cost(48 * rows * n * rank, 32 * rows * n),
        name="final",
    )(at, *pieces, squares, oh, ol, *buffers, *before)


def power_of_two(n):
    return n & (n - 1) == 0


def bits_of(n):
    return list(range(n.bit_length() - 1))


def swap(x, axis, *places):
    n = lax.axis_size(axis)
    mask = sum(1 << bit for bit in places)
    return lax.ppermute(x, axis, [(i, i ^ mask) for i in range(n)])


def spread_sum(x, bits):
    for b in bits[3:]:
        x = total(x, swap(x, "dp", b))
    b, c = bits[1:3]
    others = [swap(x, "dp", *m) for m in ((b,), (c,), (b, c))]
    return total(x, *others)


def on_device(gradient, momentum, right_factor):
    rows, cols = gradient.shape
    n_dp, n_tp = lax.axis_size("dp"), lax.axis_size("tensor")
    d, z = lax.axis_index("dp"), lax.axis_index("tensor")
    bits = bits_of(n_dp)

    unit = LANES * (-(-cols // (8 * LANES)))
    orders = [bits[1:], bits[1:][::-1]]
    table = []

    def put(*values):
        table.extend(values)
        return len(table) - len(values)

    bit_of = lambda b: (d >> b) & 1
    s, core = z & 1, d & 1
    put(s, 1 - s)
    core_at = put(core)
    send_at, keep_at, bit_at, near, far, first = [], [], [], [], [], []
    for h, order in enumerate(orders):
        t = bit_of(order[0])
        base, beside = 4 * h + 2 * core, 4 * h + 2 * (1 - core)
        send_at.append(put(beside, beside + 1))
        keep_at.append(put(base + 1 - t, base + t, 1 - t, t))
        bit_at.append({b: put(bit_of(b)) for b in order[1:]})
        near += [base + t, beside + t]
        far += [base + 1 - t, beside + 1 - t]
        at, n = (base + t) * unit, unit
        for b in order[1:]:
            n = n // 2
            at = at + bit_of(b) * n
        first.append(at)
    near_at, far_at, first_at = put(*near), put(*far), put(*first)
    at = jnp.stack([jnp.asarray(v, jnp.int32) for v in table])

    parts = 2 if rows % (4 * GROUP) == 0 else 1
    other, rh, rl, *away = left_rows(at, 1, 0, parts, gradient, momentum, right_factor, 8 * unit)
    own, mine = [], []
    for i in range(parts):
        x, y = left_rows(at, 0, i, parts, gradient, momentum, (rh, rl), 8 * unit)
        own.append(x)
        mine.append(y)
    held = (*own, other)
    if power_of_two(n_tp) and n_tp > 1:
        pieces = []
        for i in range(parts):
            got = swap(away[i], "tensor", 0)
            pieces.append(total(mine[i], got))
        for bit in bits_of(n_tp)[1:]:
            for i in range(parts):
                got = swap(pieces[i], "tensor", bit)
                pieces[i] = total(pieces[i], got)
        for i in range(parts):
            pieces.append(swap(pieces[i], "tensor", 0))
    else:
        mine, away = jnp.concatenate(mine), jnp.concatenate(away)
        both = lax.psum(jnp.where(s == 0, jnp.stack([mine, away]), jnp.stack([away, mine])), "tensor")
        pieces = [lax.dynamic_index_in_dim(both, i, 0, False) for i in (s, 1 - s)]

    left, lh, ll, send, gram = gram_of(at, core_at, pieces)
    got = swap(send, "dp", 0)
    gram = spread_sum(total(gram, got), bits)
    gram_beside = swap(gram, "dp", 0)

    got = []
    for h in range(2):
        sent = w_send(at, send_at[h], lh, ll, unit, *held)
        got.append(swap(sent, "dp", 0))
    kept = []
    for h, order in enumerate(orders):
        send, keep = w_keep(at, keep_at[h], got[h], lh, ll, unit, *held)
        recv = swap(send, "dp", order[0])
        for b in order[1:]:
            send, keep = halve(at, bit_at[h][b], keep, recv)
            recv = swap(send, "dp", b)
        kept += [keep, recv]

    x_inv, oh, ol = chol_inverse(at, core_at, gram, gram_beside, left)
    *right, squares = right_rows(at, first_at, cols, *kept, x_inv)
    if power_of_two(n_tp):
        for b in bits_of(n_tp):
            squares = total(squares, swap(squares, "tensor", b))
    else:
        squares = lax.psum(squares, "tensor")
    got = swap(squares, "dp", 0)
    squares = total(squares, got)
    squares = spread_sum(squares, bits)

    blocks = unit // LANES
    groups = ((0, blocks - blocks // 2), (blocks - blocks // 2, blocks // 2))
    near, far = [], ([], [])
    for h, (order, x) in enumerate(zip(orders, right)):
        parts = [x]
        for b in order[:0:-1]:
            y = swap(x, "dp", b)
            last = 2 * x.shape[0] == unit
            x, *parts = join(
                at, bit_at[h][b], x, y, [count * LANES for _, count in groups] if last else []
            )
        for g, part in enumerate(parts):
            y = swap(part, "dp", order[0])
            far[g].extend([y, swap(y, "dp", 0)])
        near.extend([x, swap(x, "dp", 0)])

    same = (squares, oh, ol, held, (cols, rows * n_dp, cols * n_tp))
    outs = final(at, near_at, (0, blocks), unit, near, *same, ())
    for g in range(2):
        outs = final(at, far_at, groups[g], unit, far[g], *same, outs)
    return tuple(outs)


def solution(mesh):
    return jax.shard_map(
        on_device,
        mesh=mesh,
        in_specs=(P("dp", "tensor"), P("dp", "tensor"), P("tensor", None)),
        out_specs=(P("dp", "tensor"), P("dp", "tensor"), P("tensor", None)),
        check_vma=False,
    )
```
